32 devices in a mesh: dp: 8 (over y, x, core), fsdp: 4 (over z).
Axes of the slice: x: 2, y: 2, z: 4, core: 2. Of those that a mesh axis runs over, the one named last changes fastest.
Arguments:
- tokens: bfloat16 [19200, 1024], P(('dp', 'fsdp')), may hold values from -6 to 6
- cotangent: bfloat16 [19200, 1024], P(('dp', 'fsdp')), may hold values from -6 to 6
- crop_group: int32 [8], P('dp'), may hold values from 0 to 1, as said below
- group_tokens: int32 [2], replicated, may hold values from 1000 to 7999
- qkv_weight: float32 [1024, 3072], P('fsdp'), may hold values from -0.1875 to 0.1875
- query_bias: float32 [1024], P('fsdp'), may hold values from -2 to 2
- value_bias: float32 [1024], P('fsdp'), may hold values from -2 to 2
- out_weight: float32 [1024, 1024], P('fsdp'), may hold values from -0.375 to 0.375
- out_bias: float32 [1024], P('fsdp'), may hold values from -2 to 2
- attn_gain: float32 [1024], P('fsdp'), may hold values from 0.5 to 1.5
- attn_shift: float32 [1024], P('fsdp'), may hold values from -2 to 2
- mlp_gain: float32 [1024], P('fsdp'), may hold values from 0.5 to 1.5
- mlp_shift: float32 [1024], P('fsdp'), may hold values from -2 to 2
- up_weight: float32 [1024, 4096], P('fsdp'), may hold values from -0.1875 to 0.1875
- up_bias: float32 [4096], P('fsdp'), may hold values from -2 to 2
- down_weight: float32 [4096, 1024], P('fsdp'), may hold values from -0.09375 to 0.09375
- down_bias: float32 [1024], P('fsdp'), may hold values from -2 to 2
Outputs:
- mixed_out: bfloat16 [19200, 1024], P(('dp', 'fsdp'))
- grad_tokens: bfloat16 [19200, 1024], P(('dp', 'fsdp'))
- grad_qkv_weight: float32 [1024, 3072], P('fsdp')
- grad_query_bias: float32 [1024], P('fsdp')
- grad_value_bias: float32 [1024], P('fsdp')
- grad_out_weight: float32 [1024, 1024], P('fsdp')
- grad_out_bias: float32 [1024], P('fsdp')
- grad_attn_gain: float32 [1024], P('fsdp')
- grad_attn_shift: float32 [1024], P('fsdp')
- grad_mlp_gain: float32 [1024], P('fsdp')
- grad_mlp_shift: float32 [1024], P('fsdp')
- grad_up_weight: float32 [1024, 4096], P('fsdp')
- grad_up_bias: float32 [4096], P('fsdp')
- grad_down_weight: float32 [4096, 1024], P('fsdp')
- grad_down_bias: float32 [1024], P('fsdp')
The draws below stay inside these ranges and needn't reach their ends.
Inputs may be any that keep to these rules, and one draw needn't show every extreme that they name: `crop_group`: exactly 5 entries are 1 and the others 0.
All inputs are finite; a program needn't handle non-finite values.
Results may differ from the reference program's by a relative error of at most 0.02.
Values may be sent and summed in bfloat16 or wider, within the bound.
A program may use at most 192 MiB of HBM per device.

```python
import jax
import jax.numpy as jnp
from jax import lax

D = 1024
HEADS = 16
HEAD_DIM = 64
FF = 4096
GLEN = 50
LLEN = 10
TOK_DEV = 600
N_GLOBAL = 5
TOKENS = 19200
N_DP = 8
N_FSDP = 4


def draw_crop_group(key, part):
    order = jax.random.permutation(key, N_DP)
    return (order < N_GLOBAL).astype(jnp.int32)


def block_scale(key, dims, shards, low, top_value):
    loudness = 1.0
    for dim, parts in shards:
        heights = jax.random.uniform(jax.random.fold_in(jax.random.fold_in(key, 6), dim), (parts,), jnp.float32, low / len(shards), top_value / len(shards))
        loudness = loudness * jnp.repeat(jnp.exp(heights), dims[dim] // parts).reshape((-1,) + (1,) * (len(dims) - 1 - dim))
    return loudness


def normal_values(key, extent, width, bound, shards=(), kind=jnp.bfloat16):
    values = jax.random.normal(key, extent, jnp.float32) * width
    if len(shards) > 0:
        values = block_scale(key, extent, shards, -0.22, 0.18) * values
    return jnp.clip(values, min=-bound, max=bound).astype(kind)


def setup_inputs(seed: int = 0) -> dict:
    arg_keys = jax.random.split(jax.random.key(seed), 18)
    tokens = normal_values(arg_keys[0], (TOKENS, D), 1.0, 6.0, ((0, 32),))
    cotangent = normal_values(arg_keys[1], (TOKENS, D), 1.0, 6.0, ((0, 32),))
    crop_group = draw_crop_group(jax.random.fold_in(arg_keys[17], 71), 0)
    group_tokens = jax.random.randint(arg_keys[3], (2,), 1000, 8000).astype(jnp.int32)
    qkv_weight = normal_values(arg_keys[4], (D, 3 * D), D ** -0.5, 0.1875, ((0, 4),), jnp.float32)
    query_bias = normal_values(arg_keys[5], (D,), 0.3, 2.0, ((0, 4),), jnp.float32)
    value_bias = normal_values(arg_keys[6], (D,), 0.3, 2.0, ((0, 4),), jnp.float32)
    out_weight = normal_values(arg_keys[7], (D, D), (D // 4) ** -0.5, 0.375, ((0, 4),), jnp.float32)
    out_bias = normal_values(arg_keys[8], (D,), 0.3, 2.0, ((0, 4),), jnp.float32)
    attn_gain = jnp.clip(1.0 + 0.1 * jax.random.normal(arg_keys[9], (D,), jnp.float32), 0.5, 1.5)
    attn_shift = normal_values(arg_keys[10], (D,), 0.3, 2.0, ((0, 4),), jnp.float32)
    mlp_gain = jnp.clip(1.0 + 0.1 * jax.random.normal(arg_keys[11], (D,), jnp.float32), 0.5, 1.5)
    mlp_shift = normal_values(arg_keys[12], (D,), 0.3, 2.0, ((0, 4),), jnp.float32)
    up_weight = normal_values(arg_keys[13], (D, FF), D ** -0.5, 0.1875, ((0, 4),), jnp.float32)
    up_bias = normal_values(arg_keys[14], (FF,), 0.3, 2.0, ((0, 4),), jnp.float32)
    down_weight = normal_values(arg_keys[15], (FF, D), FF ** -0.5, 0.09375, ((0, 4),), jnp.float32)
    down_bias = normal_values(arg_keys[16], (D,), 0.3, 2.0, ((0, 4),), jnp.float32)
    return dict(tokens=tokens, cotangent=cotangent, crop_group=crop_group, group_tokens=group_tokens, qkv_weight=qkv_weight, query_bias=query_bias, value_bias=value_bias, out_weight=out_weight, out_bias=out_bias, attn_gain=attn_gain, attn_shift=attn_shift, mlp_gain=mlp_gain, mlp_shift=mlp_shift, up_weight=up_weight, up_bias=up_bias, down_weight=down_weight, down_bias=down_bias)


HIGH = lax.Precision.HIGHEST
EPSILON = 1e-06
BIG_NEGATIVE = -1000000000.0
ROOT_HALF = 0.7071067811865476

@jax.custom_vjp
def low(v):
    return lax.optimization_barrier(v.astype(jnp.bfloat16)).astype(jnp.float32)

@jax.custom_vjp
def low_back(v):
    return v

def low_keep(v):
    return (low(v), None)

def low_pass(kept, grad):
    return (grad,)

def back_keep(v):
    return (v, None)

def back_low(kept, grad):
    return (low(grad),)
low.defvjp(low_keep, low_pass)
low_back.defvjp(back_keep, back_low)

def normalize(values, gain, shift):
    middle = lax.optimization_barrier(jnp.mean(values, axis=-1, keepdims=True))
    centered = values - middle
    inverse = lax.rsqrt(lax.optimization_barrier(jnp.mean(centered * centered, axis=-1, keepdims=True)) + EPSILON)
    return centered * inverse * gain + shift

def gelu(values):
    return 0.5 * values * (1.0 + jax.scipy.special.erf(values * ROOT_HALF))

def block_forward(params, inputs, seg_length):
    qkv_weight, query_bias, value_bias, out_weight, out_bias, attn_gain, attn_shift, mlp_gain, mlp_shift, up_weight, up_bias, down_weight, down_bias = params
    length = inputs.shape[0]
    factor = HEAD_DIM ** (-0.5)
    normed = low(normalize(inputs, attn_gain, attn_shift))
    projected = jnp.dot(normed, qkv_weight, precision=HIGH)
    projected = projected + jnp.concatenate([query_bias, jnp.zeros_like(query_bias), value_bias])
    projected = low(low_back(projected))
    queries = projected[:, :D].reshape(length, HEADS, HEAD_DIM)
    key_rows = projected[:, D:2 * D].reshape(length, HEADS, HEAD_DIM)
    value_rows = projected[:, 2 * D:].reshape(length, HEADS, HEAD_DIM)
    scores = jnp.einsum('qhd,khd->hqk', queries, key_rows, precision=HIGH) * factor
    scores = low_back(scores)
    segment = lax.iota(jnp.int32, length) // seg_length
    allowed = segment[:, None] == segment[None, :]
    scores = jnp.where(allowed[None], scores, BIG_NEGATIVE)
    highest = lax.optimization_barrier(jnp.max(scores, axis=-1, keepdims=True))
    exponent = jnp.exp(scores - highest)
    attention = low(exponent / lax.optimization_barrier(jnp.sum(exponent, axis=-1, keepdims=True)))
    context = jnp.einsum('hqk,khd->qhd', attention, value_rows, precision=HIGH).reshape(length, D)
    context = low(low_back(context))
    branch = jnp.dot(context, out_weight, precision=HIGH) + out_bias
    middle = inputs + low_back(branch)
    normed_two = low(normalize(middle, mlp_gain, mlp_shift))
    preacts = low_back(jnp.dot(normed_two, up_weight, precision=HIGH) + up_bias)
    activated = low(gelu(preacts))
    branch_two = jnp.dot(activated, down_weight, precision=HIGH) + down_bias
    return middle + low_back(branch_two)

def reference(tokens, cotangent, crop_group, group_tokens, qkv_weight, query_bias, value_bias, out_weight, out_bias, attn_gain, attn_shift, mlp_gain, mlp_shift, up_weight, up_bias, down_weight, down_bias):
    masters = (qkv_weight, query_bias, value_bias, out_weight, out_bias, attn_gain, attn_shift, mlp_gain, mlp_shift, up_weight, up_bias, down_weight, down_bias)
    seg_lengths = jnp.where(crop_group == 1, GLEN, LLEN).astype(jnp.int32)
    totals = (group_tokens[0] + group_tokens[1]).astype(jnp.float32)
    shares = jnp.where(crop_group == 1, group_tokens[1], group_tokens[0]).astype(jnp.float32) / totals
    lengths = jnp.repeat(seg_lengths, N_FSDP)
    loss_share = jnp.repeat(shares, N_FSDP)
    inputs = tokens.astype(jnp.float32).reshape(N_DP * N_FSDP, TOK_DEV, D)
    upstream = cotangent.astype(jnp.float32).reshape(N_DP * N_FSDP, TOK_DEV, D) * loss_share[:, None, None]
    checked = jax.checkpoint(block_forward)
    rounded = tuple((low(member) for member in masters))

    def scan_step(carry, trio):
        block_in, block_up, seg_length = trio

        def local(values, params):
            return checked(params, values, seg_length)
        outputs, pullback = jax.vjp(local, block_in, rounded)
        grad_in, grad_params = pullback(block_up)
        carry = tuple((total + low(share) for total, share in zip(carry, grad_params)))
        return (carry, (outputs, grad_in))
    start = tuple((jnp.zeros_like(member) for member in masters))
    grads, (outputs, grad_inputs) = lax.scan(scan_step, start, (inputs, upstream, lengths))
    return (outputs.reshape(TOKENS, D).astype(jnp.bfloat16), grad_inputs.reshape(TOKENS, D).astype(jnp.bfloat16), grads[0], grads[1], grads[2], grads[3], grads[4], grads[5], grads[6], grads[7], grads[8], grads[9], grads[10], grads[11], grads[12])
```

```python
import functools

import jax
import jax.numpy as jnp
from jax import lax
from jax.sharding import PartitionSpec as P

D = 1024
HEADS = 16
HEAD_DIM = 64
GLEN = 50
LLEN = 10


EPSILON = 1e-06
ROOT_HALF = 0.7071067811865476
INV_ROOT_TAU = 0.3989422804014327


def normalize(values):
    middle = jnp.mean(values, axis=-1, keepdims=True)
    centered = values - middle
    inverse = lax.rsqrt(jnp.mean(centered * centered, axis=-1, keepdims=True) + EPSILON)
    return (centered * inverse, inverse)


def norm_back(grad_out, gain, scaled, inverse):
    grad_scaled = grad_out * gain
    return inverse * (
        grad_scaled
        - jnp.mean(grad_scaled, axis=-1, keepdims=True)
        - scaled * jnp.mean(grad_scaled * scaled, axis=-1, keepdims=True)
    )


def by_crops(values, crop):
    return values.reshape(values.shape[0] // crop, crop, HEADS, HEAD_DIM)


def crop_scores(queries, key_rows):
    factor = HEAD_DIM ** (-0.5)
    return (
        jnp.einsum("cqhd,ckhd->chqk", queries, key_rows, preferred_element_type=jnp.float32)
        * factor
    )


def attend_crops(queries, key_rows, value_rows, crop):
    length = queries.shape[0]
    crop_q, crop_k, crop_v = (
        by_crops(queries, crop),
        by_crops(key_rows, crop),
        by_crops(value_rows, crop),
    )
    scores = crop_scores(crop_q, crop_k)
    highest = jnp.max(scores, axis=-1, keepdims=True)
    exponent = jnp.exp(scores - highest)
    summed = jnp.sum(exponent, axis=-1, keepdims=True)
    attention = (exponent / summed).astype(jnp.bfloat16)
    context = jnp.einsum("chqk,ckhd->cqhd", attention, crop_v, preferred_element_type=jnp.float32)
    logsum = (highest + jnp.log(summed))[..., 0]
    return (
        context.reshape(length, HEADS * HEAD_DIM),
        jnp.transpose(logsum, (0, 2, 1)).reshape(length, HEADS),
    )


def attend_crops_back(queries, key_rows, value_rows, logsum, grad_context, crop):
    length = queries.shape[0]
    factor = HEAD_DIM ** (-0.5)
    crop_q, crop_k, crop_v = (
        by_crops(queries, crop),
        by_crops(key_rows, crop),
        by_crops(value_rows, crop),
    )
    crop_g = by_crops(grad_context, crop)
    crop_l = jnp.transpose(logsum.reshape(length // crop, crop, HEADS), (0, 2, 1))
    scores = crop_scores(crop_q, crop_k)
    probs = jnp.exp(scores - crop_l[..., None])
    probs_low = probs.astype(jnp.bfloat16)
    grad_values = jnp.einsum(
        "chqk,cqhd->ckhd", probs_low, crop_g, preferred_element_type=jnp.float32
    )
    grad_probs = jnp.einsum("cqhd,ckhd->chqk", crop_g, crop_v, preferred_element_type=jnp.float32)
    delta = jnp.sum(probs * grad_probs, axis=-1, keepdims=True)
    grad_scores = (probs * (grad_probs - delta)).astype(jnp.bfloat16)
    grad_queries = (
        jnp.einsum("chqk,ckhd->cqhd", grad_scores, crop_k, preferred_element_type=jnp.float32)
        * factor
    )
    grad_keys = (
        jnp.einsum("chqk,cqhd->ckhd", grad_scores, crop_q, preferred_element_type=jnp.float32)
        * factor
    )
    width = HEADS * HEAD_DIM
    return jnp.concatenate(
        [
            grad_queries.reshape(length, width),
            grad_keys.reshape(length, width),
            grad_values.reshape(length, width),
        ],
        axis=1,
    ).astype(jnp.bfloat16)


VECTOR_ORDER = (1, 2, 4, 5, 6, 7, 8, 10, 12)


def xor_pairs(n, mask):
    return [(i, i ^ mask) for i in range(n)]


def ring_pairs(n):
    return [(i, (i + 1) % n) for i in range(n)]


def chip_masks(n_dp):
    masks = []
    mask = 2
    while mask < n_dp:
        masks.append(mask)
        mask *= 2
    return masks


def spread_in_plane(items, n_dp, order):
    held = list(items)
    batches = [list(items)]
    for mask in order:
        got = lax.ppermute([it[2] for it in held], "dp", xor_pairs(n_dp, mask))
        new = [(it[0] ^ mask, it[1], piece) for it, piece in zip(held, got)]
        held = held + new
        batches.append(new)
    partner = []
    for batch in batches:
        got = lax.ppermute([it[2] for it in batch], "dp", xor_pairs(n_dp, 1))
        partner += [(it[0] ^ 1, it[1], piece) for it, piece in zip(batch, got)]
    return held + partner


def gather_weights(shards, n_dp, n_fsdp):
    d = lax.axis_index("dp")
    f = lax.axis_index("fsdp")
    rows = [s.shape[0] // (2 * n_dp) for s in shards]
    full = [
        lax.dynamic_update_slice(
            jnp.zeros((n_fsdp, n_dp, 2, r, s.shape[1]), s.dtype),
            s.reshape(1, n_dp, 2, r, s.shape[1]),
            (f, 0, 0, 0, 0),
        )
        for s, r in zip(shards, rows)
    ]
    own = [
        [lax.dynamic_slice_in_dim(s, (2 * d + h) * r, r, 0) for s, r in zip(shards, rows)]
        for h in range(2)
    ]
    z_items = ([], [])
    buf = own
    for step in range(1, n_fsdp):
        buf = lax.ppermute(buf, "fsdp", ring_pairs(n_fsdp))
        source = (f - step) % n_fsdp
        for h in range(2):
            z_items[h].append((0, source, buf[h]))
    masks = chip_masks(n_dp)
    for h in range(2):
        order = masks if h == 0 else masks[::-1]
        for x, source, pieces in spread_in_plane(z_items[h], n_dp, order):
            full = [
                lax.dynamic_update_slice(w, p[None, None, None], (source, d ^ x, h, 0, 0))
                for w, p in zip(full, pieces)
            ]
    return [w.reshape(-1, w.shape[-1]) for w in full]


def reduce_weights(grads, n_dp, n_fsdp):
    d = lax.axis_index("dp")
    f = lax.axis_index("fsdp")
    bits = n_dp.bit_length() - 1
    rows = [g.shape[0] // (n_fsdp * 2 * n_dp) for g in grads]
    masks = chip_masks(n_dp)
    finals = []
    for h in range(2):
        acc = [
            g.reshape((n_fsdp,) + (2,) * bits + (2, r, g.shape[1]))[(slice(None),) * (bits + 1) + (h,)]
            for g, r in zip(grads, rows)
        ]
        live = list(range(bits - 1, -1, -1))
        seq = [1] + (masks[::-1] if h == 0 else masks)
        for mask in seq:
            bit = mask.bit_length() - 1
            axis = 1 + live.index(bit)
            mine = (d >> bit) & 1
            send = [lax.dynamic_index_in_dim(a, 1 - mine, axis, keepdims=False) for a in acc]
            keep = [lax.dynamic_index_in_dim(a, mine, axis, keepdims=False) for a in acc]
            got = lax.ppermute([s.astype(jnp.bfloat16) for s in send], "dp", xor_pairs(n_dp, mask))
            acc = [k.astype(jnp.float32) + g.astype(jnp.float32) for k, g in zip(keep, got)]
            live.remove(bit)
        if n_fsdp == 1:
            finals.append([a[0].astype(jnp.bfloat16) for a in acc])
            continue
        send = [lax.dynamic_index_in_dim(a, (f - 1) % n_fsdp, 0, keepdims=False).astype(jnp.bfloat16) for a in acc]
        for step in range(1, n_fsdp):
            got = lax.ppermute(send, "fsdp", ring_pairs(n_fsdp))
            chunk = (f - 1 - step) % n_fsdp
            send = [
                (g.astype(jnp.float32) + lax.dynamic_index_in_dim(a, chunk, 0, keepdims=False)).astype(jnp.bfloat16)
                for g, a in zip(got, acc)
            ]
        finals.append(send)
    outs = [jnp.zeros((n_dp, 2, r, g.shape[1]), jnp.bfloat16) for g, r in zip(grads, rows)]
    for h in range(2):
        order = masks if h == 0 else masks[::-1]
        for x, _, pieces in spread_in_plane([(0, None, finals[h])], n_dp, order):
            outs = [lax.dynamic_update_slice(o, p[None, None], (d ^ x, h, 0, 0)) for o, p in zip(outs, pieces)]
    return [o.reshape(-1, o.shape[-1]).astype(jnp.float32) for o in outs]


def gather_weights_native(shards, n_dp, n_fsdp):
    return [lax.all_gather(s, "fsdp", axis=0, tiled=True) for s in shards]


def reduce_weights_native(grads, n_dp, n_fsdp):
    return [
        lax.psum(lax.psum_scatter(g, "fsdp", scatter_dimension=0, tiled=True), "dp").astype(jnp.float32)
        for g in grads
    ]


def pack_vectors(vectors, n_dp, n_fsdp):
    rows = jnp.concatenate([v.reshape(n_fsdp, -1) for v in vectors], axis=1)
    return rows.reshape(n_fsdp * 2 * n_dp, -1)


def unpack_vectors(packed, sizes, n_fsdp):
    rows = packed.reshape(n_fsdp, -1)
    out = []
    offset = 0
    for size in sizes:
        width = size // n_fsdp
        out.append(rows[:, offset : offset + width].reshape(size))
        offset += width
    return out


def column_sums(values):
    return jnp.sum(values.astype(jnp.float32), axis=0)

def local(
    tokens,
    cotangent,
    crop_group,
    group_tokens,
    qkv_weight,
    query_bias,
    value_bias,
    out_weight,
    out_bias,
    attn_gain,
    attn_shift,
    mlp_gain,
    mlp_shift,
    up_weight,
    up_bias,
    down_weight,
    down_bias,
    n_dp,
    n_fsdp,
):
    small = n_dp * n_fsdp <= 64
    gather = gather_weights if small else gather_weights_native
    reduce = reduce_weights if small else reduce_weights_native
    vectors = (query_bias, value_bias, out_bias, attn_gain, attn_shift, mlp_gain, mlp_shift, up_bias, down_bias)
    sizes = [v.shape[0] * n_fsdp for v in vectors]
    vec_shard = jnp.concatenate([v.astype(jnp.bfloat16) for v in vectors]).reshape(2 * n_dp, -1)
    qkv_low, vec_full = gather([qkv_weight.astype(jnp.bfloat16), vec_shard], n_dp, n_fsdp)
    (out_low,) = gather([out_weight.astype(jnp.bfloat16)], n_dp, n_fsdp)
    (up_low,) = gather([up_weight.astype(jnp.bfloat16)], n_dp, n_fsdp)
    (down_low,) = gather([down_weight.astype(jnp.bfloat16)], n_dp, n_fsdp)
    (
        query_add,
        value_add,
        out_add,
        gain_one,
        shift_one,
        gain_two,
        shift_two,
        up_add,
        down_add,
    ) = [v.astype(jnp.float32) for v in unpack_vectors(vec_full, sizes, n_fsdp)]
    is_global = crop_group[0] == 1
    totals = (group_tokens[0] + group_tokens[1]).astype(jnp.float32)
    loss_share = jnp.where(is_global, group_tokens[1], group_tokens[0]).astype(jnp.float32) / totals
    inputs = tokens.astype(jnp.float32)
    scaled_one, inverse_one = normalize(inputs)
    normed_one = (scaled_one * gain_one + shift_one).astype(jnp.bfloat16)
    projected = jnp.dot(normed_one, qkv_low, preferred_element_type=jnp.float32)
    projected = projected + jnp.concatenate([query_add, jnp.zeros_like(query_add), value_add])
    projected_low = projected.astype(jnp.bfloat16)
    queries = projected_low[:, :D]
    key_rows = projected_low[:, D : 2 * D]
    value_rows = projected_low[:, 2 * D :]
    context, logsum = lax.cond(
        is_global,
        lambda parts: attend_crops(parts[0], parts[1], parts[2], GLEN),
        lambda parts: attend_crops(parts[0], parts[1], parts[2], LLEN),
        (queries, key_rows, value_rows),
    )
    context_low = context.astype(jnp.bfloat16)
    middle = inputs + (jnp.dot(context_low, out_low, preferred_element_type=jnp.float32) + out_add)
    scaled_two, inverse_two = normalize(middle)
    normed_two = (scaled_two * gain_two + shift_two).astype(jnp.bfloat16)
    preacts = jnp.dot(normed_two, up_low, preferred_element_type=jnp.float32) + up_add
    error_part = 1.0 + jax.scipy.special.erf(preacts * ROOT_HALF)
    activated = (0.5 * preacts * error_part).astype(jnp.bfloat16)
    mixed_out = (
        middle + (jnp.dot(activated, down_low, preferred_element_type=jnp.float32) + down_add)
    ).astype(jnp.bfloat16)
    upstream = cotangent.astype(jnp.float32) * loss_share
    upstream_low = upstream.astype(jnp.bfloat16)
    grad_down_weight = jnp.dot(activated.T, upstream_low, preferred_element_type=jnp.float32)
    grad_down_bias = column_sums(upstream_low)
    grad_activated = jnp.dot(upstream_low, down_low.T, preferred_element_type=jnp.float32)
    slope = 0.5 * error_part + preacts * jnp.exp(-0.5 * preacts * preacts) * INV_ROOT_TAU
    grad_preacts = (grad_activated * slope).astype(jnp.bfloat16)
    grad_up_weight = jnp.dot(normed_two.T, grad_preacts, preferred_element_type=jnp.float32)
    grad_up_bias = column_sums(grad_preacts)
    grad_normed_two = jnp.dot(grad_preacts, up_low.T, preferred_element_type=jnp.float32)
    grad_mlp_gain = jnp.sum(grad_normed_two * scaled_two, axis=0)
    grad_mlp_shift = jnp.sum(grad_normed_two, axis=0)
    grad_middle = upstream + norm_back(grad_normed_two, gain_two, scaled_two, inverse_two)
    grad_branch = grad_middle.astype(jnp.bfloat16)
    grad_out_weight = jnp.dot(context_low.T, grad_branch, preferred_element_type=jnp.float32)
    grad_out_bias = column_sums(grad_branch)
    grad_context = jnp.dot(grad_branch, out_low.T, preferred_element_type=jnp.float32).astype(
        jnp.bfloat16
    )
    grad_projected = lax.cond(
        is_global,
        lambda parts: attend_crops_back(parts[0], parts[1], parts[2], parts[3], parts[4], GLEN),
        lambda parts: attend_crops_back(parts[0], parts[1], parts[2], parts[3], parts[4], LLEN),
        (queries, key_rows, value_rows, logsum, grad_context),
    )
    grad_qkv_weight = jnp.dot(normed_one.T, grad_projected, preferred_element_type=jnp.float32)
    grad_query_bias = column_sums(grad_projected[:, :D])
    grad_value_bias = column_sums(grad_projected[:, 2 * D :])
    grad_normed_one = jnp.dot(grad_projected, qkv_low.T, preferred_element_type=jnp.float32)
    grad_attn_gain = jnp.sum(grad_normed_one * scaled_one, axis=0)
    grad_attn_shift = jnp.sum(grad_normed_one, axis=0)
    grad_tokens = (
        grad_middle + norm_back(grad_normed_one, gain_one, scaled_one, inverse_one)
    ).astype(jnp.bfloat16)
    grad_vectors = (
        grad_query_bias,
        grad_value_bias,
        grad_out_bias,
        grad_attn_gain,
        grad_attn_shift,
        grad_mlp_gain,
        grad_mlp_shift,
        grad_up_bias,
        grad_down_bias,
    )
    vec_grads = pack_vectors([g.astype(jnp.bfloat16) for g in grad_vectors], n_dp, n_fsdp)
    (grad_down_shard,) = reduce([grad_down_weight.astype(jnp.bfloat16)], n_dp, n_fsdp)
    (grad_up_shard,) = reduce([grad_up_weight.astype(jnp.bfloat16)], n_dp, n_fsdp)
    (grad_out_shard,) = reduce([grad_out_weight.astype(jnp.bfloat16)], n_dp, n_fsdp)
    grad_qkv_shard, vec_shard_grads = reduce(
        [grad_qkv_weight.astype(jnp.bfloat16), vec_grads], n_dp, n_fsdp
    )
    vec_out = unpack_vectors(vec_shard_grads.reshape(1, -1), [s // n_fsdp for s in sizes], 1)
    return (
        mixed_out,
        grad_tokens,
        grad_qkv_shard,
        vec_out[0],
        vec_out[1],
        grad_out_shard,
        vec_out[2],
        vec_out[3],
        vec_out[4],
        vec_out[5],
        vec_out[6],
        grad_up_shard,
        vec_out[7],
        grad_down_shard,
        vec_out[8],
    )


def solution(mesh):
    placed = (
        P(("dp", "fsdp"), None),
        P(("dp", "fsdp"), None),
        P("dp"),
        P(),
        P("fsdp", None),
        P("fsdp"),
        P("fsdp"),
        P("fsdp", None),
        P("fsdp"),
        P("fsdp"),
        P("fsdp"),
        P("fsdp"),
        P("fsdp"),
        P("fsdp", None),
        P("fsdp"),
        P("fsdp", None),
        P("fsdp"),
    )
    n_dp = mesh.shape["dp"]
    n_fsdp = mesh.shape["fsdp"]
    return jax.shard_map(
        functools.partial(local, n_dp=n_dp, n_fsdp=n_fsdp),
        mesh=mesh,
        in_specs=placed,
        out_specs=(
            P(("dp", "fsdp"), None),
            P(("dp", "fsdp"), None),
            P("fsdp", None),
            P("fsdp"),
            P("fsdp"),
            P("fsdp", None),
            P("fsdp"),
            P("fsdp"),
            P("fsdp"),
            P("fsdp"),
            P("fsdp"),
            P("fsdp", None),
            P("fsdp"),
            P("fsdp", None),
            P("fsdp"),
        ),
        check_vma=False,
    )
```

```python
import functools

import jax
import jax.numpy as jnp
from jax import lax
from jax.sharding import PartitionSpec as P

D = 1024
HEADS = 16
HEAD_DIM = 64
GLEN = 50
LLEN = 10


EPSILON = 1e-06
ROOT_HALF = 0.7071067811865476
INV_ROOT_TAU = 0.3989422804014327


def normalize(values):
    middle = jnp.mean(values, axis=-1, keepdims=True)
    centered = values - middle
    inverse = lax.rsqrt(jnp.mean(centered * centered, axis=-1, keepdims=True) + EPSILON)
    return (centered * inverse, inverse)


def norm_back(grad_out, gain, scaled, inverse):
    grad_scaled = grad_out * gain
    return inverse * (
        grad_scaled
        - jnp.mean(grad_scaled, axis=-1, keepdims=True)
        - scaled * jnp.mean(grad_scaled * scaled, axis=-1, keepdims=True)
    )


def by_crops(values, crop):
    return values.reshape(values.shape[0] // crop, crop, HEADS, HEAD_DIM)


def crop_scores(queries, key_rows):
    factor = HEAD_DIM ** (-0.5)
    return (
        jnp.einsum("cqhd,ckhd->chqk", queries, key_rows, preferred_element_type=jnp.float32)
        * factor
    )


def attend_crops(queries, key_rows, value_rows, crop):
    length = queries.shape[0]
    crop_q, crop_k, crop_v = (
        by_crops(queries, crop),
        by_crops(key_rows, crop),
        by_crops(value_rows, crop),
    )
    scores = crop_scores(crop_q, crop_k)
    highest = jnp.max(scores, axis=-1, keepdims=True)
    exponent = jnp.exp(scores - highest)
    summed = jnp.sum(exponent, axis=-1, keepdims=True)
    attention = (exponent / summed).astype(jnp.bfloat16)
    context = jnp.einsum("chqk,ckhd->cqhd", attention, crop_v, preferred_element_type=jnp.float32)
    logsum = (highest + jnp.log(summed))[..., 0]
    return (
        context.reshape(length, HEADS * HEAD_DIM),
        jnp.transpose(logsum, (0, 2, 1)).reshape(length, HEADS),
    )


def attend_crops_back(queries, key_rows, value_rows, logsum, grad_context, crop):
    length = queries.shape[0]
    factor = HEAD_DIM ** (-0.5)
    crop_q, crop_k, crop_v = (
        by_crops(queries, crop),
        by_crops(key_rows, crop),
        by_crops(value_rows, crop),
    )
    crop_g = by_crops(grad_context, crop)
    crop_l = jnp.transpose(logsum.reshape(length // crop, crop, HEADS), (0, 2, 1))
    scores = crop_scores(crop_q, crop_k)
    probs = jnp.exp(scores - crop_l[..., None])
    probs_low = probs.astype(jnp.bfloat16)
    grad_values = jnp.einsum(
        "chqk,cqhd->ckhd", probs_low, crop_g, preferred_element_type=jnp.float32
    )
    grad_probs = jnp.einsum("cqhd,ckhd->chqk", crop_g, crop_v, preferred_element_type=jnp.float32)
    delta = jnp.sum(probs * grad_probs, axis=-1, keepdims=True)
    grad_scores = (probs * (grad_probs - delta)).astype(jnp.bfloat16)
    grad_queries = (
        jnp.einsum("chqk,ckhd->cqhd", grad_scores, crop_k, preferred_element_type=jnp.float32)
        * factor
    )
    grad_keys = (
        jnp.einsum("chqk,cqhd->ckhd", grad_scores, crop_q, preferred_element_type=jnp.float32)
        * factor
    )
    width = HEADS * HEAD_DIM
    return jnp.concatenate(
        [
            grad_queries.reshape(length, width),
            grad_keys.reshape(length, width),
            grad_values.reshape(length, width),
        ],
        axis=1,
    ).astype(jnp.bfloat16)


VECTOR_ORDER = (1, 2, 4, 5, 6, 7, 8, 10, 12)


def xor_pairs(n, mask):
    return [(i, i ^ mask) for i in range(n)]


def exchange(leaves, held, bit, d, n_dp):
    got = lax.ppermute(leaves, "dp", xor_pairs(n_dp, 1 << bit))
    pos = sum(1 for b in held if b > bit)
    mine = ((d >> bit) & 1) == 0
    out = [
        jnp.where(mine, jnp.stack([a, g], axis=pos), jnp.stack([g, a], axis=pos))
        for a, g in zip(leaves, got)
    ]
    return out, sorted(held + [bit], reverse=True)


def split_bit(leaves, held, bit, d, n_dp, lead):
    axis = lead + held.index(bit)
    mine = (d >> bit) & 1
    send = [lax.dynamic_index_in_dim(a, 1 - mine, axis, keepdims=False) for a in leaves]
    keep = [lax.dynamic_index_in_dim(a, mine, axis, keepdims=False) for a in leaves]
    got = lax.ppermute([v.astype(jnp.bfloat16) for v in send], "dp", xor_pairs(n_dp, 1 << bit))
    return [k.astype(jnp.float32) + g.astype(jnp.float32) for k, g in zip(keep, got)], [b for b in held if b != bit]


def chip_bits(n_dp):
    return list(range(1, n_dp.bit_length() - 1))


def view_rows(matrix, n_fsdp, n_dp):
    return matrix.reshape(n_fsdp, n_dp, 2, -1, 1024)


def gather_group(shards, vec, n_dp, n_fsdp):
    d = lax.axis_index("dp")
    f = lax.axis_index("fsdp")
    widths = [s.shape[0] * s.shape[1] // (1024 * 2 * n_dp) for s in shards]
    pack = jnp.concatenate([s.reshape(n_dp, 2, -1, 1024) for s in shards], axis=2)
    own = lax.dynamic_index_in_dim(pack, d, 0, keepdims=False)
    down = [(i, (i - 1) % n_fsdp) for i in range(n_fsdp)]
    ring = []
    vring = []
    buf = [own] + ([vec] if vec is not None else [])
    for _ in range(1, n_fsdp):
        buf = lax.ppermute(buf, "fsdp", down)
        ring.append(buf[0])
        if vec is not None:
            vring.append(buf[1])
    if n_fsdp > 1:
        zrel = jnp.stack(ring, axis=0)
        halves = []
        for h in range(2):
            order = chip_bits(n_dp)
            order = order if h == 0 else order[::-1]
            leaves, held = [zrel[:, h]], []
            for bit in order:
                leaves, held = exchange(leaves, held, bit, d, n_dp)
            halves.append(leaves[0])
        both = jnp.stack(halves, axis=-3)
        held = chip_bits(n_dp)[::-1]
        if n_dp > 1:
            (both,), held = exchange([both], held, 0, d, n_dp)
        plane = both.reshape((n_dp, n_fsdp - 1) + both.shape[-3:])
        rel = jnp.concatenate([pack[None], jnp.swapaxes(plane, 0, 1)], axis=0)
    else:
        rel = pack[None]
    full = jnp.roll(rel, f, axis=0)
    out = []
    offset = 0
    for s, w in zip(shards, widths):
        out.append(full[:, :, :, offset : offset + w].reshape(n_fsdp * s.shape[0], s.shape[1]))
        offset += w
    vecs = None
    if vec is not None:
        vecs = jnp.roll(jnp.stack([vec] + vring, axis=0), f, axis=0)
    return out, vecs


def reduce_group(grads, vec_grads, n_dp, n_fsdp):
    d = lax.axis_index("dp")
    f = lax.axis_index("fsdp")
    bits = n_dp.bit_length() - 1
    widths = [g.shape[0] * g.shape[1] // (1024 * 2 * n_dp * n_fsdp) for g in grads]
    pack = jnp.concatenate([view_rows(g.astype(jnp.bfloat16), n_fsdp, n_dp) for g in grads], axis=3)
    leaves = [pack.reshape((n_fsdp,) + (2,) * bits + pack.shape[2:])]
    if vec_grads is not None:
        leaves.append(vec_grads.reshape((n_fsdp,) + (2,) * bits + vec_grads.shape[2:]))
    held = list(range(bits - 1, -1, -1))
    if bits > 0:
        leaves, held = split_bit(leaves, held, 0, d, n_dp, 1)
    finals = []
    for h in range(2):
        order = chip_bits(n_dp)
        order = order[::-1] if h == 0 else order
        part = [lax.index_in_dim(a, h, 1 + len(held), keepdims=False) for a in leaves]
        hb = list(held)
        for bit in order:
            part, hb = split_bit(part, hb, bit, d, n_dp, 1)
        finals.append(part)
    acc = [jnp.stack([finals[0][i], finals[1][i]], axis=1) for i in range(len(leaves))]
    down = [(i, (i - 1) % n_fsdp) for i in range(n_fsdp)]
    send = [lax.dynamic_index_in_dim(a, (f + 1) % n_fsdp, 0, keepdims=False).astype(jnp.bfloat16) for a in acc]
    if n_fsdp == 1:
        send = [a[0].astype(jnp.bfloat16) for a in acc]
    for step in range(1, n_fsdp):
        got = lax.ppermute(send, "fsdp", down)
        chunk = (f + 1 + step) % n_fsdp
        send = [
            (g.astype(jnp.float32) + lax.dynamic_index_in_dim(a, chunk, 0, keepdims=False)).astype(jnp.bfloat16)
            for g, a in zip(got, acc)
        ]
    halves = []
    for h in range(2):
        order = chip_bits(n_dp)
        order = order if h == 0 else order[::-1]
        part, hb = [v[h] for v in send], []
        for bit in order:
            part, hb = exchange(part, hb, bit, d, n_dp)
        halves.append(part)
    both = [jnp.stack([halves[0][i], halves[1][i]], axis=len(hb)) for i in range(len(send))]
    if n_dp > 1:
        both, hb = exchange(both, hb, 0, d, n_dp)
    shard_pack = both[0].reshape((n_dp, 2) + both[0].shape[-2:]).astype(jnp.float32)
    out = []
    offset = 0
    for g, w in zip(grads, widths):
        rows = g.shape[0] // n_fsdp
        out.append(shard_pack[:, :, offset : offset + w].reshape(rows, g.shape[1]))
        offset += w
    vec_out = None
    if vec_grads is not None:
        vec_out = both[1].reshape(-1).astype(jnp.float32)
    return out, vec_out


def gather_weights_native(shards, n_dp, n_fsdp):
    return [lax.all_gather(s, "fsdp", axis=0, tiled=True) for s in shards]


def reduce_weights_native(grads, n_dp, n_fsdp):
    return [
        lax.psum(lax.psum_scatter(g, "fsdp", scatter_dimension=0, tiled=True), "dp").astype(jnp.float32)
        for g in grads
    ]


def unpack_vectors(packed, sizes, n_fsdp):
    rows = packed.reshape(n_fsdp, -1)
    out = []
    offset = 0
    for size in sizes:
        width = size // n_fsdp
        out.append(rows[:, offset : offset + width].reshape(size))
        offset += width
    return out


def column_sums(values):
    return jnp.sum(values.astype(jnp.float32), axis=0)

def local(
    tokens,
    cotangent,
    crop_group,
    group_tokens,
    qkv_weight,
    query_bias,
    value_bias,
    out_weight,
    out_bias,
    attn_gain,
    attn_shift,
    mlp_gain,
    mlp_shift,
    up_weight,
    up_bias,
    down_weight,
    down_bias,
    n_dp,
    n_fsdp,
):
    small = n_dp * n_fsdp <= 64
    vectors = (query_bias, value_bias, out_bias, attn_gain, attn_shift, mlp_gain, mlp_shift, up_bias, down_bias)
    sizes = [v.shape[0] * n_fsdp for v in vectors]
    vec_local = jnp.concatenate([v.astype(jnp.bfloat16) for v in vectors])
    low = [w.astype(jnp.bfloat16) for w in (qkv_weight, out_weight, up_weight, down_weight)]
    if small:
        (qkv_low, out_low), vec_rows = gather_group(low[:2], vec_local, n_dp, n_fsdp)
        (up_low, down_low), _ = gather_group(low[2:], None, n_dp, n_fsdp)
    else:
        qkv_low, out_low, up_low, down_low = gather_weights_native(low, n_dp, n_fsdp)
        vec_rows = lax.all_gather(vec_local, "fsdp", axis=0, tiled=False)
    (
        query_add,
        value_add,
        out_add,
        gain_one,
        shift_one,
        gain_two,
        shift_two,
        up_add,
        down_add,
    ) = [v.astype(jnp.float32) for v in unpack_vectors(vec_rows, sizes, n_fsdp)]
    is_global = crop_group[0] == 1
    totals = (group_tokens[0] + group_tokens[1]).astype(jnp.float32)
    loss_share = jnp.where(is_global, group_tokens[1], group_tokens[0]).astype(jnp.float32) / totals
    inputs = tokens.astype(jnp.float32)
    scaled_one, inverse_one = normalize(inputs)
    normed_one = (scaled_one * gain_one + shift_one).astype(jnp.bfloat16)
    projected = jnp.dot(normed_one, qkv_low, preferred_element_type=jnp.float32)
    projected = projected + jnp.concatenate([query_add, jnp.zeros_like(query_add), value_add])
    projected_low = projected.astype(jnp.bfloat16)
    queries = projected_low[:, :D]
    key_rows = projected_low[:, D : 2 * D]
    value_rows = projected_low[:, 2 * D :]
    context, logsum = lax.cond(
        is_global,
        lambda parts: attend_crops(parts[0], parts[1], parts[2], GLEN),
        lambda parts: attend_crops(parts[0], parts[1], parts[2], LLEN),
        (queries, key_rows, value_rows),
    )
    context_low = context.astype(jnp.bfloat16)
    middle = inputs + (jnp.dot(context_low, out_low, preferred_element_type=jnp.float32) + out_add)
    scaled_two, inverse_two = normalize(middle)
    normed_two = (scaled_two * gain_two + shift_two).astype(jnp.bfloat16)
    preacts = jnp.dot(normed_two, up_low, preferred_element_type=jnp.float32) + up_add
    error_part = 1.0 + jax.scipy.special.erf(preacts * ROOT_HALF)
    activated = (0.5 * preacts * error_part).astype(jnp.bfloat16)
    mixed_out = (
        middle + (jnp.dot(activated, down_low, preferred_element_type=jnp.float32) + down_add)
    ).astype(jnp.bfloat16)
    upstream = cotangent.astype(jnp.float32) * loss_share
    upstream_low = upstream.astype(jnp.bfloat16)
    grad_down_weight = jnp.dot(activated.T, upstream_low, preferred_element_type=jnp.float32)
    grad_down_bias = column_sums(upstream_low)
    grad_activated = jnp.dot(upstream_low, down_low.T, preferred_element_type=jnp.float32)
    slope = 0.5 * error_part + preacts * jnp.exp(-0.5 * preacts * preacts) * INV_ROOT_TAU
    grad_preacts = (grad_activated * slope).astype(jnp.bfloat16)
    grad_up_weight = jnp.dot(normed_two.T, grad_preacts, preferred_element_type=jnp.float32)
    grad_up_bias = column_sums(grad_preacts)
    grad_normed_two = jnp.dot(grad_preacts, up_low.T, preferred_element_type=jnp.float32)
    grad_mlp_gain = jnp.sum(grad_normed_two * scaled_two, axis=0)
    grad_mlp_shift = jnp.sum(grad_normed_two, axis=0)
    grad_middle = upstream + norm_back(grad_normed_two, gain_two, scaled_two, inverse_two)
    grad_branch = grad_middle.astype(jnp.bfloat16)
    grad_out_weight = jnp.dot(context_low.T, grad_branch, preferred_element_type=jnp.float32)
    grad_out_bias = column_sums(grad_branch)
    grad_context = jnp.dot(grad_branch, out_low.T, preferred_element_type=jnp.float32).astype(
        jnp.bfloat16
    )
    grad_projected = lax.cond(
        is_global,
        lambda parts: attend_crops_back(parts[0], parts[1], parts[2], parts[3], parts[4], GLEN),
        lambda parts: attend_crops_back(parts[0], parts[1], parts[2], parts[3], parts[4], LLEN),
        (queries, key_rows, value_rows, logsum, grad_context),
    )
    grad_qkv_weight = jnp.dot(normed_one.T, grad_projected, preferred_element_type=jnp.float32)
    grad_query_bias = column_sums(grad_projected[:, :D])
    grad_value_bias = column_sums(grad_projected[:, 2 * D :])
    grad_normed_one = jnp.dot(grad_projected, qkv_low.T, preferred_element_type=jnp.float32)
    grad_attn_gain = jnp.sum(grad_normed_one * scaled_one, axis=0)
    grad_attn_shift = jnp.sum(grad_normed_one, axis=0)
    grad_tokens = (
        grad_middle + norm_back(grad_normed_one, gain_one, scaled_one, inverse_one)
    ).astype(jnp.bfloat16)
    grad_vectors = (
        grad_query_bias,
        grad_value_bias,
        grad_out_bias,
        grad_attn_gain,
        grad_attn_shift,
        grad_mlp_gain,
        grad_mlp_shift,
        grad_up_bias,
        grad_down_bias,
    )
    vec_grads = jnp.concatenate(
        [g.astype(jnp.bfloat16).reshape(n_fsdp, -1) for g in grad_vectors], axis=1
    )
    if small:
        (grad_up_shard, grad_down_shard), _ = reduce_group([grad_up_weight, grad_down_weight], None, n_dp, n_fsdp)
        (grad_out_shard, grad_qkv_shard), vec_flat = reduce_group(
            [grad_out_weight, grad_qkv_weight], vec_grads.reshape(n_fsdp, n_dp, 2, -1), n_dp, n_fsdp
        )
    else:
        grad_qkv_shard, grad_out_shard, grad_up_shard, grad_down_shard = reduce_weights_native(
            [w.astype(jnp.bfloat16) for w in (grad_qkv_weight, grad_out_weight, grad_up_weight, grad_down_weight)],
            n_dp,
            n_fsdp,
        )
        (vec_flat,) = reduce_weights_native([vec_grads], n_dp, n_fsdp)
    vec_out = unpack_vectors(vec_flat.reshape(1, -1), [s // n_fsdp for s in sizes], 1)
    return (
        mixed_out,
        grad_tokens,
        grad_qkv_shard,
        vec_out[0],
        vec_out[1],
        grad_out_shard,
        vec_out[2],
        vec_out[3],
        vec_out[4],
        vec_out[5],
        vec_out[6],
        grad_up_shard,
        vec_out[7],
        grad_down_shard,
        vec_out[8],
    )


def solution(mesh):
    placed = (
        P(("dp", "fsdp"), None),
        P(("dp", "fsdp"), None),
        P("dp"),
        P(),
        P("fsdp", None),
        P("fsdp"),
        P("fsdp"),
        P("fsdp", None),
        P("fsdp"),
        P("fsdp"),
        P("fsdp"),
        P("fsdp"),
        P("fsdp"),
        P("fsdp", None),
        P("fsdp"),
        P("fsdp", None),
        P("fsdp"),
    )
    n_dp = mesh.shape["dp"]
    n_fsdp = mesh.shape["fsdp"]
    return jax.shard_map(
        functools.partial(local, n_dp=n_dp, n_fsdp=n_fsdp),
        mesh=mesh,
        in_specs=placed,
        out_specs=(
            P(("dp", "fsdp"), None),
            P(("dp", "fsdp"), None),
            P("fsdp", None),
            P("fsdp"),
            P("fsdp"),
            P("fsdp", None),
            P("fsdp"),
            P("fsdp"),
            P("fsdp"),
            P("fsdp"),
            P("fsdp"),
            P("fsdp", None),
            P("fsdp"),
            P("fsdp", None),
            P("fsdp"),
        ),
        check_vma=False,
    )
```

```python
import functools

import jax
import jax.numpy as jnp
from jax import lax
from jax.sharding import PartitionSpec as P

D = 1024
HEADS = 16
HEAD_DIM = 64
GLEN = 50
LLEN = 10


EPSILON = 1e-06
ROOT_HALF = 0.7071067811865476
INV_ROOT_TAU = 0.3989422804014327


def normalize(values):
    middle = jnp.mean(values, axis=-1, keepdims=True)
    centered = values - middle
    inverse = lax.rsqrt(jnp.mean(centered * centered, axis=-1, keepdims=True) + EPSILON)
    return (centered * inverse, inverse)


def norm_back(grad_out, gain, scaled, inverse):
    grad_scaled = grad_out * gain
    return inverse * (
        grad_scaled
        - jnp.mean(grad_scaled, axis=-1, keepdims=True)
        - scaled * jnp.mean(grad_scaled * scaled, axis=-1, keepdims=True)
    )


def by_crops(values, crop):
    return values.reshape(values.shape[0] // crop, crop, HEADS, HEAD_DIM)


def crop_scores(queries, key_rows):
    factor = HEAD_DIM ** (-0.5)
    return (
        jnp.einsum("cqhd,ckhd->chqk", queries, key_rows, preferred_element_type=jnp.float32)
        * factor
    )


def attend_crops(queries, key_rows, value_rows, crop):
    length = queries.shape[0]
    crop_q, crop_k, crop_v = (
        by_crops(queries, crop),
        by_crops(key_rows, crop),
        by_crops(value_rows, crop),
    )
    scores = crop_scores(crop_q, crop_k)
    highest = jnp.max(scores, axis=-1, keepdims=True)
    exponent = jnp.exp(scores - highest)
    summed = jnp.sum(exponent, axis=-1, keepdims=True)
    attention = (exponent / summed).astype(jnp.bfloat16)
    context = jnp.einsum("chqk,ckhd->cqhd", attention, crop_v, preferred_element_type=jnp.float32)
    logsum = (highest + jnp.log(summed))[..., 0]
    return (
        context.reshape(length, HEADS * HEAD_DIM),
        jnp.transpose(logsum, (0, 2, 1)).reshape(length, HEADS),
    )


def attend_crops_back(queries, key_rows, value_rows, logsum, grad_context, crop):
    length = queries.shape[0]
    factor = HEAD_DIM ** (-0.5)
    crop_q, crop_k, crop_v = (
        by_crops(queries, crop),
        by_crops(key_rows, crop),
        by_crops(value_rows, crop),
    )
    crop_g = by_crops(grad_context, crop)
    crop_l = jnp.transpose(logsum.reshape(length // crop, crop, HEADS), (0, 2, 1))
    scores = crop_scores(crop_q, crop_k)
    probs = jnp.exp(scores - crop_l[..., None])
    probs_low = probs.astype(jnp.bfloat16)
    grad_values = jnp.einsum(
        "chqk,cqhd->ckhd", probs_low, crop_g, preferred_element_type=jnp.float32
    )
    grad_probs = jnp.einsum("cqhd,ckhd->chqk", crop_g, crop_v, preferred_element_type=jnp.float32)
    delta = jnp.sum(probs * grad_probs, axis=-1, keepdims=True)
    grad_scores = (probs * (grad_probs - delta)).astype(jnp.bfloat16)
    grad_queries = (
        jnp.einsum("chqk,ckhd->cqhd", grad_scores, crop_k, preferred_element_type=jnp.float32)
        * factor
    )
    grad_keys = (
        jnp.einsum("chqk,cqhd->ckhd", grad_scores, crop_q, preferred_element_type=jnp.float32)
        * factor
    )
    width = HEADS * HEAD_DIM
    return jnp.concatenate(
        [
            grad_queries.reshape(length, width),
            grad_keys.reshape(length, width),
            grad_values.reshape(length, width),
        ],
        axis=1,
    ).astype(jnp.bfloat16)


VECTOR_ORDER = (1, 2, 4, 5, 6, 7, 8, 10, 12)


def xor_pairs(n, mask):
    return [(i, i ^ mask) for i in range(n)]


def exchange(leaves, held, bit, d, n_dp):
    got = lax.ppermute(leaves, "dp", xor_pairs(n_dp, 1 << bit))
    pos = sum(1 for b in held if b > bit)
    mine = ((d >> bit) & 1) == 0
    out = [
        jnp.where(mine, jnp.stack([a, g], axis=pos), jnp.stack([g, a], axis=pos))
        for a, g in zip(leaves, got)
    ]
    return out, sorted(held + [bit], reverse=True)


def split_bit(leaves, held, bit, d, n_dp, lead):
    axis = lead + held.index(bit)
    mine = (d >> bit) & 1
    send = [lax.dynamic_index_in_dim(a, 1 - mine, axis, keepdims=False) for a in leaves]
    keep = [lax.dynamic_index_in_dim(a, mine, axis, keepdims=False) for a in leaves]
    got = lax.ppermute([v.astype(jnp.bfloat16) for v in send], "dp", xor_pairs(n_dp, 1 << bit))
    return [k.astype(jnp.float32) + g.astype(jnp.float32) for k, g in zip(keep, got)], [b for b in held if b != bit]


def chip_bits(n_dp):
    return list(range(1, n_dp.bit_length() - 1))


def gather_chain(shard, vec, n_dp, n_fsdp):
    d = lax.axis_index("dp")
    f = lax.axis_index("fsdp")
    rows, cols = shard.shape
    pieces = shard.reshape(n_dp, 2, rows // (2 * n_dp), cols)
    own = lax.dynamic_index_in_dim(pieces, d, 0, keepdims=False)
    down = [(i, (i - 1) % n_fsdp) for i in range(n_fsdp)]
    ring, vring = [], []
    buf = [own] + ([vec] if vec is not None else [])
    for _ in range(1, n_fsdp):
        buf = lax.ppermute(buf, "fsdp", down)
        ring.append(buf[0])
        if vec is not None:
            vring.append(buf[1])
    vecs = None
    if vec is not None:
        vecs = jnp.roll(jnp.stack([vec] + vring, axis=0), f, axis=0)
    if n_fsdp == 1:
        return shard, vecs
    zrel = jnp.stack(ring, axis=0)
    halves = []
    for h in range(2):
        order = chip_bits(n_dp)
        order = order if h == 0 else order[::-1]
        leaves, held = [zrel[:, h]], []
        for bit in order:
            leaves, held = exchange(leaves, held, bit, d, n_dp)
        halves.append(leaves[0])
    both = jnp.stack(halves, axis=-3)
    held = chip_bits(n_dp)[::-1]
    if n_dp > 1:
        (both,), held = exchange([both], held, 0, d, n_dp)
    plane = both.reshape((n_dp, n_fsdp - 1) + both.shape[-3:])
    rel = jnp.concatenate([pieces[None], jnp.swapaxes(plane, 0, 1)], axis=0)
    return jnp.roll(rel, f, axis=0).reshape(n_fsdp * rows, cols), vecs


def reduce_chain(grad, n_dp, n_fsdp):
    d = lax.axis_index("dp")
    f = lax.axis_index("fsdp")
    bits = n_dp.bit_length() - 1
    rows, cols = grad.shape
    w = rows // (n_fsdp * 2 * n_dp)
    leaves = [grad.astype(jnp.bfloat16).reshape((n_fsdp,) + (2,) * bits + (2, w, cols))]
    held = list(range(bits - 1, -1, -1))
    if bits > 0:
        leaves, held = split_bit(leaves, held, 0, d, n_dp, 1)
    finals = []
    for h in range(2):
        order = chip_bits(n_dp)
        order = order[::-1] if h == 0 else order
        part = [lax.index_in_dim(leaves[0], h, 1 + len(held), keepdims=False)]
        hb = list(held)
        for bit in order:
            part, hb = split_bit(part, hb, bit, d, n_dp, 1)
        finals.append(part[0])
    acc = jnp.stack(finals, axis=1)
    down = [(i, (i - 1) % n_fsdp) for i in range(n_fsdp)]
    if n_fsdp == 1:
        send = acc[0].astype(jnp.bfloat16)
    else:
        send = lax.dynamic_index_in_dim(acc, (f + 1) % n_fsdp, 0, keepdims=False).astype(jnp.bfloat16)
    for step in range(1, n_fsdp):
        got = lax.ppermute(send, "fsdp", down)
        chunk = (f + 1 + step) % n_fsdp
        send = (got.astype(jnp.float32) + lax.dynamic_index_in_dim(acc, chunk, 0, keepdims=False)).astype(jnp.bfloat16)
    halves = []
    for h in range(2):
        order = chip_bits(n_dp)
        order = order if h == 0 else order[::-1]
        part, hb = [send[h]], []
        for bit in order:
            part, hb = exchange(part, hb, bit, d, n_dp)
        halves.append(part[0])
    both = jnp.stack(halves, axis=len(hb))
    if n_dp > 1:
        (both,), hb = exchange([both], hb, 0, d, n_dp)
    return both.reshape(rows // n_fsdp, cols).astype(jnp.float32)


def gather_weights_native(shards, n_dp, n_fsdp):
    return [lax.all_gather(s, "fsdp", axis=0, tiled=True) for s in shards]


def reduce_weights_native(grads, n_dp, n_fsdp):
    return [
        lax.psum(lax.psum_scatter(g, "fsdp", scatter_dimension=0, tiled=True), "dp").astype(jnp.float32)
        for g in grads
    ]


def unpack_vectors(packed, sizes, n_fsdp):
    rows = packed.reshape(n_fsdp, -1)
    out = []
    offset = 0
    for size in sizes:
        width = size // n_fsdp
        out.append(rows[:, offset : offset + width].reshape(size))
        offset += width
    return out


def column_sums(values):
    return jnp.sum(values.astype(jnp.float32), axis=0)

def local(
    tokens,
    cotangent,
    crop_group,
    group_tokens,
    qkv_weight,
    query_bias,
    value_bias,
    out_weight,
    out_bias,
    attn_gain,
    attn_shift,
    mlp_gain,
    mlp_shift,
    up_weight,
    up_bias,
    down_weight,
    down_bias,
    n_dp,
    n_fsdp,
):
    small = n_dp * n_fsdp <= 64
    vectors = (query_bias, value_bias, out_bias, attn_gain, attn_shift, mlp_gain, mlp_shift, up_bias, down_bias)
    sizes = [v.shape[0] * n_fsdp for v in vectors]
    vec_local = jnp.concatenate([v.astype(jnp.bfloat16) for v in vectors])
    low = [w.astype(jnp.bfloat16) for w in (qkv_weight, out_weight, up_weight, down_weight)]
    if small:
        qkv_low, vec_rows = gather_chain(low[0], vec_local, n_dp, n_fsdp)
        out_low, _ = gather_chain(low[1], None, n_dp, n_fsdp)
        up_low, _ = gather_chain(low[2], None, n_dp, n_fsdp)
        down_low, _ = gather_chain(low[3], None, n_dp, n_fsdp)
    else:
        qkv_low, out_low, up_low, down_low = gather_weights_native(low, n_dp, n_fsdp)
        vec_rows = lax.all_gather(vec_local, "fsdp", axis=0, tiled=False)
    (
        query_add,
        value_add,
        out_add,
        gain_one,
        shift_one,
        gain_two,
        shift_two,
        up_add,
        down_add,
    ) = [v.astype(jnp.float32) for v in unpack_vectors(vec_rows, sizes, n_fsdp)]
    is_global = crop_group[0] == 1
    totals = (group_tokens[0] + group_tokens[1]).astype(jnp.float32)
    loss_share = jnp.where(is_global, group_tokens[1], group_tokens[0]).astype(jnp.float32) / totals
    inputs = tokens.astype(jnp.float32)
    scaled_one, inverse_one = normalize(inputs)
    normed_one = (scaled_one * gain_one + shift_one).astype(jnp.bfloat16)
    projected = jnp.dot(normed_one, qkv_low, preferred_element_type=jnp.float32)
    projected = projected + jnp.concatenate([query_add, jnp.zeros_like(query_add), value_add])
    projected_low = projected.astype(jnp.bfloat16)
    queries = projected_low[:, :D]
    key_rows = projected_low[:, D : 2 * D]
    value_rows = projected_low[:, 2 * D :]
    context, logsum = lax.cond(
        is_global,
        lambda parts: attend_crops(parts[0], parts[1], parts[2], GLEN),
        lambda parts: attend_crops(parts[0], parts[1], parts[2], LLEN),
        (queries, key_rows, value_rows),
    )
    context_low = context.astype(jnp.bfloat16)
    middle = inputs + (jnp.dot(context_low, out_low, preferred_element_type=jnp.float32) + out_add)
    scaled_two, inverse_two = normalize(middle)
    normed_two = (scaled_two * gain_two + shift_two).astype(jnp.bfloat16)
    preacts = jnp.dot(normed_two, up_low, preferred_element_type=jnp.float32) + up_add
    error_part = 1.0 + jax.scipy.special.erf(preacts * ROOT_HALF)
    activated = (0.5 * preacts * error_part).astype(jnp.bfloat16)
    mixed_out = (
        middle + (jnp.dot(activated, down_low, preferred_element_type=jnp.float32) + down_add)
    ).astype(jnp.bfloat16)
    upstream = cotangent.astype(jnp.float32) * loss_share
    upstream_low = upstream.astype(jnp.bfloat16)
    grad_down_weight = jnp.dot(activated.T, upstream_low, preferred_element_type=jnp.float32)
    grad_down_bias = column_sums(upstream_low)
    grad_activated = jnp.dot(upstream_low, down_low.T, preferred_element_type=jnp.float32)
    slope = 0.5 * error_part + preacts * jnp.exp(-0.5 * preacts * preacts) * INV_ROOT_TAU
    grad_preacts = (grad_activated * slope).astype(jnp.bfloat16)
    grad_up_weight = jnp.dot(normed_two.T, grad_preacts, preferred_element_type=jnp.float32)
    grad_up_bias = column_sums(grad_preacts)
    grad_normed_two = jnp.dot(grad_preacts, up_low.T, preferred_element_type=jnp.float32)
    grad_mlp_gain = jnp.sum(grad_normed_two * scaled_two, axis=0)
    grad_mlp_shift = jnp.sum(grad_normed_two, axis=0)
    grad_middle = upstream + norm_back(grad_normed_two, gain_two, scaled_two, inverse_two)
    grad_branch = grad_middle.astype(jnp.bfloat16)
    grad_out_weight = jnp.dot(context_low.T, grad_branch, preferred_element_type=jnp.float32)
    grad_out_bias = column_sums(grad_branch)
    grad_context = jnp.dot(grad_branch, out_low.T, preferred_element_type=jnp.float32).astype(
        jnp.bfloat16
    )
    grad_projected = lax.cond(
        is_global,
        lambda parts: attend_crops_back(parts[0], parts[1], parts[2], parts[3], parts[4], GLEN),
        lambda parts: attend_crops_back(parts[0], parts[1], parts[2], parts[3], parts[4], LLEN),
        (queries, key_rows, value_rows, logsum, grad_context),
    )
    grad_qkv_weight = jnp.dot(normed_one.T, grad_projected, preferred_element_type=jnp.float32)
    grad_query_bias = column_sums(grad_projected[:, :D])
    grad_value_bias = column_sums(grad_projected[:, 2 * D :])
    grad_normed_one = jnp.dot(grad_projected, qkv_low.T, preferred_element_type=jnp.float32)
    grad_attn_gain = jnp.sum(grad_normed_one * scaled_one, axis=0)
    grad_attn_shift = jnp.sum(grad_normed_one, axis=0)
    grad_tokens = (
        grad_middle + norm_back(grad_normed_one, gain_one, scaled_one, inverse_one)
    ).astype(jnp.bfloat16)
    grad_vectors = (
        grad_query_bias,
        grad_value_bias,
        grad_out_bias,
        grad_attn_gain,
        grad_attn_shift,
        grad_mlp_gain,
        grad_mlp_shift,
        grad_up_bias,
        grad_down_bias,
    )
    vec_grads = jnp.concatenate(
        [g.astype(jnp.bfloat16).reshape(n_fsdp, -1) for g in grad_vectors], axis=1
    )
    if small:
        grad_down_shard = reduce_chain(grad_down_weight, n_dp, n_fsdp)
        grad_up_shard = reduce_chain(grad_up_weight, n_dp, n_fsdp)
        grad_out_shard = reduce_chain(grad_out_weight, n_dp, n_fsdp)
        grad_qkv_shard = reduce_chain(grad_qkv_weight, n_dp, n_fsdp)
        vec_total = lax.psum(vec_grads.astype(jnp.float32), ("dp", "fsdp"))
        vec_flat = lax.dynamic_index_in_dim(vec_total, lax.axis_index("fsdp"), 0, keepdims=False)
    else:
        grad_qkv_shard, grad_out_shard, grad_up_shard, grad_down_shard = reduce_weights_native(
            [w.astype(jnp.bfloat16) for w in (grad_qkv_weight, grad_out_weight, grad_up_weight, grad_down_weight)],
            n_dp,
            n_fsdp,
        )
        (vec_flat,) = reduce_weights_native([vec_grads], n_dp, n_fsdp)
    vec_out = unpack_vectors(vec_flat.reshape(1, -1), [s // n_fsdp for s in sizes], 1)
    return (
        mixed_out,
        grad_tokens,
        grad_qkv_shard,
        vec_out[0],
        vec_out[1],
        grad_out_shard,
        vec_out[2],
        vec_out[3],
        vec_out[4],
        vec_out[5],
        vec_out[6],
        grad_up_shard,
        vec_out[7],
        grad_down_shard,
        vec_out[8],
    )


def solution(mesh):
    placed = (
        P(("dp", "fsdp"), None),
        P(("dp", "fsdp"), None),
        P("dp"),
        P(),
        P("fsdp", None),
        P("fsdp"),
        P("fsdp"),
        P("fsdp", None),
        P("fsdp"),
        P("fsdp"),
        P("fsdp"),
        P("fsdp"),
        P("fsdp"),
        P("fsdp", None),
        P("fsdp"),
        P("fsdp", None),
        P("fsdp"),
    )
    n_dp = mesh.shape["dp"]
    n_fsdp = mesh.shape["fsdp"]
    return jax.shard_map(
        functools.partial(local, n_dp=n_dp, n_fsdp=n_fsdp),
        mesh=mesh,
        in_specs=placed,
        out_specs=(
            P(("dp", "fsdp"), None),
            P(("dp", "fsdp"), None),
            P("fsdp", None),
            P("fsdp"),
            P("fsdp"),
            P("fsdp", None),
            P("fsdp"),
            P("fsdp"),
            P("fsdp"),
            P("fsdp"),
            P("fsdp"),
            P("fsdp", None),
            P("fsdp"),
            P("fsdp", None),
            P("fsdp"),
        ),
        check_vma=False,
    )
```

```python
import functools

import jax
import jax.numpy as jnp
from jax import lax
from jax.sharding import PartitionSpec as P

D = 1024
HEADS = 16
HEAD_DIM = 64
GLEN = 50
LLEN = 10


EPSILON = 1e-06
ROOT_HALF = 0.7071067811865476
INV_ROOT_TAU = 0.3989422804014327


def normalize(values):
    middle = jnp.mean(values, axis=-1, keepdims=True)
    centered = values - middle
    inverse = lax.rsqrt(jnp.mean(centered * centered, axis=-1, keepdims=True) + EPSILON)
    return (centered * inverse, inverse)


def norm_back(grad_out, gain, scaled, inverse):
    grad_scaled = grad_out * gain
    return inverse * (
        grad_scaled
        - jnp.mean(grad_scaled, axis=-1, keepdims=True)
        - scaled * jnp.mean(grad_scaled * scaled, axis=-1, keepdims=True)
    )


def by_crops(values, crop):
    return values.reshape(values.shape[0] // crop, crop, HEADS, HEAD_DIM)


def crop_scores(queries, key_rows):
    factor = HEAD_DIM ** (-0.5)
    return (
        jnp.einsum("cqhd,ckhd->chqk", queries, key_rows, preferred_element_type=jnp.float32)
        * factor
    )


def attend_crops(queries, key_rows, value_rows, crop):
    length = queries.shape[0]
    crop_q, crop_k, crop_v = (
        by_crops(queries, crop),
        by_crops(key_rows, crop),
        by_crops(value_rows, crop),
    )
    scores = crop_scores(crop_q, crop_k)
    highest = jnp.max(scores, axis=-1, keepdims=True)
    exponent = jnp.exp(scores - highest)
    summed = jnp.sum(exponent, axis=-1, keepdims=True)
    attention = (exponent / summed).astype(jnp.bfloat16)
    context = jnp.einsum("chqk,ckhd->cqhd", attention, crop_v, preferred_element_type=jnp.float32)
    logsum = (highest + jnp.log(summed))[..., 0]
    return (
        context.reshape(length, HEADS * HEAD_DIM),
        jnp.transpose(logsum, (0, 2, 1)).reshape(length, HEADS),
    )


def attend_crops_back(queries, key_rows, value_rows, logsum, grad_context, crop):
    length = queries.shape[0]
    factor = HEAD_DIM ** (-0.5)
    crop_q, crop_k, crop_v = (
        by_crops(queries, crop),
        by_crops(key_rows, crop),
        by_crops(value_rows, crop),
    )
    crop_g = by_crops(grad_context, crop)
    crop_l = jnp.transpose(logsum.reshape(length // crop, crop, HEADS), (0, 2, 1))
    scores = crop_scores(crop_q, crop_k)
    probs = jnp.exp(scores - crop_l[..., None])
    probs_low = probs.astype(jnp.bfloat16)
    grad_values = jnp.einsum(
        "chqk,cqhd->ckhd", probs_low, crop_g, preferred_element_type=jnp.float32
    )
    grad_probs = jnp.einsum("cqhd,ckhd->chqk", crop_g, crop_v, preferred_element_type=jnp.float32)
    delta = jnp.sum(probs * grad_probs, axis=-1, keepdims=True)
    grad_scores = (probs * (grad_probs - delta)).astype(jnp.bfloat16)
    grad_queries = (
        jnp.einsum("chqk,ckhd->cqhd", grad_scores, crop_k, preferred_element_type=jnp.float32)
        * factor
    )
    grad_keys = (
        jnp.einsum("chqk,cqhd->ckhd", grad_scores, crop_q, preferred_element_type=jnp.float32)
        * factor
    )
    width = HEADS * HEAD_DIM
    return jnp.concatenate(
        [
            grad_queries.reshape(length, width),
            grad_keys.reshape(length, width),
            grad_values.reshape(length, width),
        ],
        axis=1,
    ).astype(jnp.bfloat16)


VECTOR_ORDER = (1, 2, 4, 5, 6, 7, 8, 10, 12)


def xor_pairs(n, mask):
    return [(i, i ^ mask) for i in range(n)]


def exchange(leaves, held, bit, d, n_dp):
    got = lax.ppermute(leaves, "dp", xor_pairs(n_dp, 1 << bit))
    pos = sum(1 for b in held if b > bit)
    mine = ((d >> bit) & 1) == 0
    out = [
        jnp.where(mine, jnp.stack([a, g], axis=pos), jnp.stack([g, a], axis=pos))
        for a, g in zip(leaves, got)
    ]
    return out, sorted(held + [bit], reverse=True)


def split_bit(leaves, held, bit, d, n_dp, lead):
    axis = lead + held.index(bit)
    mine = (d >> bit) & 1
    send = [lax.dynamic_index_in_dim(a, 1 - mine, axis, keepdims=False) for a in leaves]
    keep = [lax.dynamic_index_in_dim(a, mine, axis, keepdims=False) for a in leaves]
    got = lax.ppermute([v.astype(jnp.bfloat16) for v in send], "dp", xor_pairs(n_dp, 1 << bit))
    return [k.astype(jnp.float32) + g.astype(jnp.float32) for k, g in zip(keep, got)], [b for b in held if b != bit]


def chip_bits(n_dp):
    return list(range(1, n_dp.bit_length() - 1))


def gather_chain(shard, vec, n_dp, n_fsdp):
    d = lax.axis_index("dp")
    f = lax.axis_index("fsdp")
    rows, cols = shard.shape
    pieces = shard.reshape(n_dp, 2, rows // (2 * n_dp), cols)
    own = lax.dynamic_index_in_dim(pieces, d, 0, keepdims=False)
    down = [(i, (i - 1) % n_fsdp) for i in range(n_fsdp)]
    ring, vring = [], []
    buf = [own] + ([vec] if vec is not None else [])
    for _ in range(1, n_fsdp):
        buf = lax.ppermute(buf, "fsdp", down)
        ring.append(buf[0])
        if vec is not None:
            vring.append(buf[1])
    vecs = None
    if vec is not None:
        vecs = jnp.roll(jnp.stack([vec] + vring, axis=0), f, axis=0)
    if n_fsdp == 1:
        return shard, vecs
    zrel = jnp.stack(ring, axis=0)
    halves = []
    for h in range(2):
        order = chip_bits(n_dp)
        order = order if h == 0 else order[::-1]
        leaves, held = [zrel[:, h]], []
        for bit in order:
            leaves, held = exchange(leaves, held, bit, d, n_dp)
        halves.append(leaves[0])
    both = jnp.stack(halves, axis=-3)
    held = chip_bits(n_dp)[::-1]
    if n_dp > 1:
        (both,), held = exchange([both], held, 0, d, n_dp)
    plane = both.reshape((n_dp, n_fsdp - 1) + both.shape[-3:])
    rel = jnp.concatenate([pieces[None], jnp.swapaxes(plane, 0, 1)], axis=0)
    return jnp.roll(rel, f, axis=0).reshape(n_fsdp * rows, cols), vecs


def reduce_chain(grads, n_dp, n_fsdp):
    d = lax.axis_index("dp")
    f = lax.axis_index("fsdp")
    bits = n_dp.bit_length() - 1
    leaves = [
        g.astype(jnp.bfloat16).reshape((n_fsdp,) + (2,) * bits + (2, g.shape[0] // (n_fsdp * 2 * n_dp), g.shape[1]))
        for g in grads
    ]
    held = list(range(bits - 1, -1, -1))
    if bits > 0:
        leaves, held = split_bit(leaves, held, 0, d, n_dp, 1)
    finals = []
    for h in range(2):
        order = chip_bits(n_dp)
        order = order[::-1] if h == 0 else order
        part = [lax.index_in_dim(a, h, 1 + len(held), keepdims=False) for a in leaves]
        hb = list(held)
        for bit in order:
            part, hb = split_bit(part, hb, bit, d, n_dp, 1)
        finals.append(part)
    acc = [jnp.stack([finals[0][i], finals[1][i]], axis=1) for i in range(len(grads))]
    down = [(i, (i - 1) % n_fsdp) for i in range(n_fsdp)]
    if n_fsdp == 1:
        send = [a[0].astype(jnp.bfloat16) for a in acc]
    else:
        send = [lax.dynamic_index_in_dim(a, (f + 1) % n_fsdp, 0, keepdims=False).astype(jnp.bfloat16) for a in acc]
    for step in range(1, n_fsdp):
        got = lax.ppermute(send, "fsdp", down)
        chunk = (f + 1 + step) % n_fsdp
        send = [
            (g.astype(jnp.float32) + lax.dynamic_index_in_dim(a, chunk, 0, keepdims=False)).astype(jnp.bfloat16)
            for g, a in zip(got, acc)
        ]
    halves = []
    for h in range(2):
        order = chip_bits(n_dp)
        order = order if h == 0 else order[::-1]
        part, hb = [v[h] for v in send], []
        for bit in order:
            part, hb = exchange(part, hb, bit, d, n_dp)
        halves.append(part)
    both = [jnp.stack([halves[0][i], halves[1][i]], axis=len(hb)) for i in range(len(grads))]
    if n_dp > 1:
        both, hb = exchange(both, hb, 0, d, n_dp)
    return [b.reshape(g.shape[0] // n_fsdp, g.shape[1]).astype(jnp.float32) for b, g in zip(both, grads)]


def gather_weights_native(shards, n_dp, n_fsdp):
    return [lax.all_gather(s, "fsdp", axis=0, tiled=True) for s in shards]


def reduce_weights_native(grads, n_dp, n_fsdp):
    return [
        lax.psum(lax.psum_scatter(g, "fsdp", scatter_dimension=0, tiled=True), "dp").astype(jnp.float32)
        for g in grads
    ]


def unpack_vectors(packed, sizes, n_fsdp):
    rows = packed.reshape(n_fsdp, -1)
    out = []
    offset = 0
    for size in sizes:
        width = size // n_fsdp
        out.append(rows[:, offset : offset + width].reshape(size))
        offset += width
    return out


def column_sums(values):
    return jnp.sum(values.astype(jnp.float32), axis=0)

def local(
    tokens,
    cotangent,
    crop_group,
    group_tokens,
    qkv_weight,
    query_bias,
    value_bias,
    out_weight,
    out_bias,
    attn_gain,
    attn_shift,
    mlp_gain,
    mlp_shift,
    up_weight,
    up_bias,
    down_weight,
    down_bias,
    n_dp,
    n_fsdp,
):
    small = n_dp * n_fsdp <= 64
    vectors = (query_bias, value_bias, out_bias, attn_gain, attn_shift, mlp_gain, mlp_shift, up_bias, down_bias)
    sizes = [v.shape[0] * n_fsdp for v in vectors]
    vec_local = jnp.concatenate([v.astype(jnp.bfloat16) for v in vectors])
    low = [w.astype(jnp.bfloat16) for w in (qkv_weight, out_weight, up_weight, down_weight)]
    if small:
        qkv_low, vec_rows = gather_chain(low[0], vec_local, n_dp, n_fsdp)
        out_low, _ = gather_chain(low[1], None, n_dp, n_fsdp)
        up_low, _ = gather_chain(low[2], None, n_dp, n_fsdp)
        down_low, _ = gather_chain(low[3], None, n_dp, n_fsdp)
    else:
        qkv_low, out_low, up_low, down_low = gather_weights_native(low, n_dp, n_fsdp)
        vec_rows = lax.all_gather(vec_local, "fsdp", axis=0, tiled=False)
    (
        query_add,
        value_add,
        out_add,
        gain_one,
        shift_one,
        gain_two,
        shift_two,
        up_add,
        down_add,
    ) = [v.astype(jnp.float32) for v in unpack_vectors(vec_rows, sizes, n_fsdp)]
    is_global = crop_group[0] == 1
    totals = (group_tokens[0] + group_tokens[1]).astype(jnp.float32)
    loss_share = jnp.where(is_global, group_tokens[1], group_tokens[0]).astype(jnp.float32) / totals
    inputs = tokens.astype(jnp.float32)
    scaled_one, inverse_one = normalize(inputs)
    normed_one = (scaled_one * gain_one + shift_one).astype(jnp.bfloat16)
    projected = jnp.dot(normed_one, qkv_low, preferred_element_type=jnp.float32)
    projected = projected + jnp.concatenate([query_add, jnp.zeros_like(query_add), value_add])
    projected_low = projected.astype(jnp.bfloat16)
    queries = projected_low[:, :D]
    key_rows = projected_low[:, D : 2 * D]
    value_rows = projected_low[:, 2 * D :]
    context, logsum = lax.cond(
        is_global,
        lambda parts: attend_crops(parts[0], parts[1], parts[2], GLEN),
        lambda parts: attend_crops(parts[0], parts[1], parts[2], LLEN),
        (queries, key_rows, value_rows),
    )
    context_low = context.astype(jnp.bfloat16)
    middle = inputs + (jnp.dot(context_low, out_low, preferred_element_type=jnp.float32) + out_add)
    scaled_two, inverse_two = normalize(middle)
    normed_two = (scaled_two * gain_two + shift_two).astype(jnp.bfloat16)
    preacts = jnp.dot(normed_two, up_low, preferred_element_type=jnp.float32) + up_add
    error_part = 1.0 + jax.scipy.special.erf(preacts * ROOT_HALF)
    activated = (0.5 * preacts * error_part).astype(jnp.bfloat16)
    mixed_out = (
        middle + (jnp.dot(activated, down_low, preferred_element_type=jnp.float32) + down_add)
    ).astype(jnp.bfloat16)
    upstream = cotangent.astype(jnp.float32) * loss_share
    upstream_low = upstream.astype(jnp.bfloat16)
    grad_down_weight = jnp.dot(activated.T, upstream_low, preferred_element_type=jnp.float32)
    grad_down_bias = column_sums(upstream_low)
    grad_activated = jnp.dot(upstream_low, down_low.T, preferred_element_type=jnp.float32)
    slope = 0.5 * error_part + preacts * jnp.exp(-0.5 * preacts * preacts) * INV_ROOT_TAU
    grad_preacts = (grad_activated * slope).astype(jnp.bfloat16)
    grad_up_weight = jnp.dot(normed_two.T, grad_preacts, preferred_element_type=jnp.float32)
    grad_up_bias = column_sums(grad_preacts)
    grad_normed_two = jnp.dot(grad_preacts, up_low.T, preferred_element_type=jnp.float32)
    grad_mlp_gain = jnp.sum(grad_normed_two * scaled_two, axis=0)
    grad_mlp_shift = jnp.sum(grad_normed_two, axis=0)
    grad_middle = upstream + norm_back(grad_normed_two, gain_two, scaled_two, inverse_two)
    grad_branch = grad_middle.astype(jnp.bfloat16)
    grad_out_weight = jnp.dot(context_low.T, grad_branch, preferred_element_type=jnp.float32)
    grad_out_bias = column_sums(grad_branch)
    grad_context = jnp.dot(grad_branch, out_low.T, preferred_element_type=jnp.float32).astype(
        jnp.bfloat16
    )
    grad_projected = lax.cond(
        is_global,
        lambda parts: attend_crops_back(parts[0], parts[1], parts[2], parts[3], parts[4], GLEN),
        lambda parts: attend_crops_back(parts[0], parts[1], parts[2], parts[3], parts[4], LLEN),
        (queries, key_rows, value_rows, logsum, grad_context),
    )
    grad_qkv_weight = jnp.dot(normed_one.T, grad_projected, preferred_element_type=jnp.float32)
    grad_query_bias = column_sums(grad_projected[:, :D])
    grad_value_bias = column_sums(grad_projected[:, 2 * D :])
    grad_normed_one = jnp.dot(grad_projected, qkv_low.T, preferred_element_type=jnp.float32)
    grad_attn_gain = jnp.sum(grad_normed_one * scaled_one, axis=0)
    grad_attn_shift = jnp.sum(grad_normed_one, axis=0)
    grad_tokens = (
        grad_middle + norm_back(grad_normed_one, gain_one, scaled_one, inverse_one)
    ).astype(jnp.bfloat16)
    grad_vectors = (
        grad_query_bias,
        grad_value_bias,
        grad_out_bias,
        grad_attn_gain,
        grad_attn_shift,
        grad_mlp_gain,
        grad_mlp_shift,
        grad_up_bias,
        grad_down_bias,
    )
    vec_grads = jnp.concatenate(
        [g.astype(jnp.bfloat16).reshape(n_fsdp, -1) for g in grad_vectors], axis=1
    )
    if small:
        (grad_down_shard,) = reduce_chain([grad_down_weight], n_dp, n_fsdp)
        (grad_up_shard,) = reduce_chain([grad_up_weight], n_dp, n_fsdp)
        (grad_out_shard,) = reduce_chain([grad_out_weight], n_dp, n_fsdp)
        grad_qkv_shard, vec_flat = reduce_chain(
            [grad_qkv_weight, vec_grads.reshape(n_fsdp * 2 * n_dp, -1)], n_dp, n_fsdp
        )
    else:
        grad_qkv_shard, grad_out_shard, grad_up_shard, grad_down_shard = reduce_weights_native(
            [w.astype(jnp.bfloat16) for w in (grad_qkv_weight, grad_out_weight, grad_up_weight, grad_down_weight)],
            n_dp,
            n_fsdp,
        )
        (vec_flat,) = reduce_weights_native([vec_grads], n_dp, n_fsdp)
    vec_out = unpack_vectors(vec_flat.reshape(1, -1), [s // n_fsdp for s in sizes], 1)
    return (
        mixed_out,
        grad_tokens,
        grad_qkv_shard,
        vec_out[0],
        vec_out[1],
        grad_out_shard,
        vec_out[2],
        vec_out[3],
        vec_out[4],
        vec_out[5],
        vec_out[6],
        grad_up_shard,
        vec_out[7],
        grad_down_shard,
        vec_out[8],
    )


def solution(mesh):
    placed = (
        P(("dp", "fsdp"), None),
        P(("dp", "fsdp"), None),
        P("dp"),
        P(),
        P("fsdp", None),
        P("fsdp"),
        P("fsdp"),
        P("fsdp", None),
        P("fsdp"),
        P("fsdp"),
        P("fsdp"),
        P("fsdp"),
        P("fsdp"),
        P("fsdp", None),
        P("fsdp"),
        P("fsdp", None),
        P("fsdp"),
    )
    n_dp = mesh.shape["dp"]
    n_fsdp = mesh.shape["fsdp"]
    return jax.shard_map(
        functools.partial(local, n_dp=n_dp, n_fsdp=n_fsdp),
        mesh=mesh,
        in_specs=placed,
        out_specs=(
            P(("dp", "fsdp"), None),
            P(("dp", "fsdp"), None),
            P("fsdp", None),
            P("fsdp"),
            P("fsdp"),
            P("fsdp", None),
            P("fsdp"),
            P("fsdp"),
            P("fsdp"),
            P("fsdp"),
            P("fsdp"),
            P("fsdp", None),
            P("fsdp"),
            P("fsdp", None),
            P("fsdp"),
        ),
        check_vma=False,
    )
```

```python
import functools

import jax
import jax.numpy as jnp
from jax import lax
from jax.sharding import PartitionSpec as P


D = 1024
HEADS = 16
HEAD_DIM = 64
GLEN = 50
LLEN = 10


EPSILON = 1e-06
BIG_NEGATIVE = -1000000000.0
ROOT_HALF = 0.7071067811865476
INV_ROOT_TAU = 0.3989422804014327


def normalize(values):
    middle = jnp.mean(values, axis=-1, keepdims=True)
    centered = values - middle
    inverse = lax.rsqrt(jnp.mean(centered * centered, axis=-1, keepdims=True) + EPSILON)
    return (centered * inverse, inverse)


def norm_back(grad_out, gain, scaled, inverse):
    grad_scaled = grad_out * gain
    return inverse * (
        grad_scaled
        - jnp.mean(grad_scaled, axis=-1, keepdims=True)
        - scaled * jnp.mean(grad_scaled * scaled, axis=-1, keepdims=True)
    )


def by_crops(values, crop):
    return values.reshape(values.shape[0] // crop, crop, HEADS, HEAD_DIM)


def crop_scores(queries, key_rows):
    factor = HEAD_DIM ** (-0.5)
    return (
        jnp.einsum("cqhd,ckhd->chqk", queries, key_rows, preferred_element_type=jnp.float32)
        * factor
    )


def crop_mask(crop):
    segment = lax.iota(jnp.int32, GLEN) // crop
    return segment[:, None] == segment[None, :]


def attend_crops(queries, key_rows, value_rows, crop):
    length = queries.shape[0]
    crop_q, crop_k, crop_v = (
        by_crops(queries, GLEN),
        by_crops(key_rows, GLEN),
        by_crops(value_rows, GLEN),
    )
    scores = jnp.where(crop_mask(crop), crop_scores(crop_q, crop_k), BIG_NEGATIVE)
    highest = jnp.max(scores, axis=-1, keepdims=True)
    exponent = jnp.exp(scores - highest)
    summed = jnp.sum(exponent, axis=-1, keepdims=True)
    attention = (exponent / summed).astype(jnp.bfloat16)
    context = jnp.einsum("chqk,ckhd->cqhd", attention, crop_v, preferred_element_type=jnp.float32)
    logsum = (highest + jnp.log(summed))[..., 0]
    return (
        context.reshape(length, HEADS * HEAD_DIM),
        jnp.transpose(logsum, (0, 2, 1)).reshape(length, HEADS),
    )


def attend_crops_back(queries, key_rows, value_rows, logsum, grad_context, crop):
    length = queries.shape[0]
    factor = HEAD_DIM ** (-0.5)
    crop_q, crop_k, crop_v = (
        by_crops(queries, GLEN),
        by_crops(key_rows, GLEN),
        by_crops(value_rows, GLEN),
    )
    crop_g = by_crops(grad_context, GLEN)
    crop_l = jnp.transpose(logsum.reshape(length // GLEN, GLEN, HEADS), (0, 2, 1))
    scores = jnp.where(crop_mask(crop), crop_scores(crop_q, crop_k), BIG_NEGATIVE)
    probs = jnp.exp(scores - crop_l[..., None])
    probs_low = probs.astype(jnp.bfloat16)
    grad_values = jnp.einsum(
        "chqk,cqhd->ckhd", probs_low, crop_g, preferred_element_type=jnp.float32
    )
    grad_probs = jnp.einsum("cqhd,ckhd->chqk", crop_g, crop_v, preferred_element_type=jnp.float32)
    delta = jnp.sum(probs * grad_probs, axis=-1, keepdims=True)
    grad_scores = (probs * (grad_probs - delta)).astype(jnp.bfloat16)
    grad_queries = (
        jnp.einsum("chqk,ckhd->cqhd", grad_scores, crop_k, preferred_element_type=jnp.float32)
        * factor
    )
    grad_keys = (
        jnp.einsum("chqk,cqhd->ckhd", grad_scores, crop_q, preferred_element_type=jnp.float32)
        * factor
    )
    width = HEADS * HEAD_DIM
    return jnp.concatenate(
        [
            grad_queries.reshape(length, width),
            grad_keys.reshape(length, width),
            grad_values.reshape(length, width),
        ],
        axis=1,
    ).astype(jnp.bfloat16)


def xor_pairs(n, mask):
    return [(i, i ^ mask) for i in range(n)]


def exchange(leaves, held, bit, d, n_dp):
    got = lax.ppermute(leaves, "dp", xor_pairs(n_dp, 1 << bit))
    pos = sum(1 for b in held if b > bit)
    mine = ((d >> bit) & 1) == 0
    out = [
        jnp.where(mine, jnp.stack([a, g], axis=pos), jnp.stack([g, a], axis=pos))
        for a, g in zip(leaves, got)
    ]
    return out, sorted(held + [bit], reverse=True)


def split_bit(leaves, held, bit, d, n_dp, lead):
    axis = lead + held.index(bit)
    mine = (d >> bit) & 1
    send = [lax.dynamic_index_in_dim(a, 1 - mine, axis, keepdims=False) for a in leaves]
    keep = [lax.dynamic_index_in_dim(a, mine, axis, keepdims=False) for a in leaves]
    got = lax.ppermute([v.astype(jnp.bfloat16) for v in send], "dp", xor_pairs(n_dp, 1 << bit))
    return [k.astype(jnp.float32) + g.astype(jnp.float32) for k, g in zip(keep, got)], [b for b in held if b != bit]


def chip_bits(n_dp):
    return list(range(1, n_dp.bit_length() - 1))


def gather_chain(shard, vec, n_dp, n_fsdp):
    d = lax.axis_index("dp")
    f = lax.axis_index("fsdp")
    rows, cols = shard.shape
    pieces = shard.reshape(n_dp, 2, rows // (2 * n_dp), cols)
    own = lax.dynamic_index_in_dim(pieces, d, 0, keepdims=False)
    down = [(i, (i - 1) % n_fsdp) for i in range(n_fsdp)]
    ring, vring = [], []
    buf = [own] + ([vec] if vec is not None else [])
    for _ in range(1, n_fsdp):
        buf = lax.ppermute(buf, "fsdp", down)
        ring.append(buf[0])
        if vec is not None:
            vring.append(buf[1])
    vecs = None
    if vec is not None:
        vecs = jnp.roll(jnp.stack([vec] + vring, axis=0), f, axis=0)
    if n_fsdp == 1:
        return shard, vecs
    zrel = jnp.stack(ring, axis=0)
    halves = []
    for h in range(2):
        order = chip_bits(n_dp)
        order = order if h == 0 else order[::-1]
        leaves, held = [zrel[:, h]], []
        for bit in order:
            leaves, held = exchange(leaves, held, bit, d, n_dp)
        halves.append(leaves[0])
    both = jnp.stack(halves, axis=-3)
    held = chip_bits(n_dp)[::-1]
    if n_dp > 1:
        (both,), held = exchange([both], held, 0, d, n_dp)
    plane = both.reshape((n_dp, n_fsdp - 1) + both.shape[-3:])
    rel = jnp.concatenate([pieces[None], jnp.swapaxes(plane, 0, 1)], axis=0)
    return jnp.roll(rel, f, axis=0).reshape(n_fsdp * rows, cols), vecs


def reduce_chain(grads, n_dp, n_fsdp):
    d = lax.axis_index("dp")
    f = lax.axis_index("fsdp")
    bits = n_dp.bit_length() - 1
    leaves = [
        g.astype(jnp.bfloat16).reshape((n_fsdp,) + (2,) * bits + (2, g.shape[0] // (n_fsdp * 2 * n_dp), g.shape[1]))
        for g in grads
    ]
    held = list(range(bits - 1, -1, -1))
    if bits > 0:
        leaves, held = split_bit(leaves, held, 0, d, n_dp, 1)
    finals = []
    for h in range(2):
        order = chip_bits(n_dp)
        order = order[::-1] if h == 0 else order
        part = [lax.index_in_dim(a, h, 1 + len(held), keepdims=False) for a in leaves]
        hb = list(held)
        for bit in order:
            part, hb = split_bit(part, hb, bit, d, n_dp, 1)
        finals.append(part)
    acc = [jnp.stack([finals[0][i], finals[1][i]], axis=1) for i in range(len(grads))]
    down = [(i, (i - 1) % n_fsdp) for i in range(n_fsdp)]
    if n_fsdp == 1:
        send = [a[0].astype(jnp.bfloat16) for a in acc]
    else:
        send = [lax.dynamic_index_in_dim(a, (f + 1) % n_fsdp, 0, keepdims=False).astype(jnp.bfloat16) for a in acc]
    for step in range(1, n_fsdp):
        got = lax.ppermute(send, "fsdp", down)
        chunk = (f + 1 + step) % n_fsdp
        send = [
            (g.astype(jnp.float32) + lax.dynamic_index_in_dim(a, chunk, 0, keepdims=False)).astype(jnp.bfloat16)
            for g, a in zip(got, acc)
        ]
    halves = []
    for h in range(2):
        order = chip_bits(n_dp)
        order = order if h == 0 else order[::-1]
        part, hb = [v[h] for v in send], []
        for bit in order:
            part, hb = exchange(part, hb, bit, d, n_dp)
        halves.append(part)
    both = [jnp.stack([halves[0][i], halves[1][i]], axis=len(hb)) for i in range(len(grads))]
    if n_dp > 1:
        both, hb = exchange(both, hb, 0, d, n_dp)
    return [b.reshape(g.shape[0] // n_fsdp, g.shape[1]).astype(jnp.float32) for b, g in zip(both, grads)]


def gather_weights_native(shards):
    return [lax.all_gather(s, "fsdp", axis=0, tiled=True) for s in shards]


def reduce_weights_native(grads):
    return [
        lax.psum(lax.psum_scatter(g, "fsdp", scatter_dimension=0, tiled=True), "dp").astype(jnp.float32)
        for g in grads
    ]


def unpack_vectors(packed, sizes, n_fsdp):
    rows = packed.reshape(n_fsdp, -1)
    out = []
    offset = 0
    for size in sizes:
        width = size // n_fsdp
        out.append(rows[:, offset : offset + width].reshape(size))
        offset += width
    return out


def column_sums(values):
    return jnp.sum(values.astype(jnp.float32), axis=0)


def local_body(
    tokens,
    cotangent,
    crop_group,
    group_tokens,
    qkv_weight,
    query_bias,
    value_bias,
    out_weight,
    out_bias,
    attn_gain,
    attn_shift,
    mlp_gain,
    mlp_shift,
    up_weight,
    up_bias,
    down_weight,
    down_bias,
    n_dp,
    n_fsdp,
):
    small = n_dp * n_fsdp <= 64
    vectors = (query_bias, value_bias, out_bias, attn_gain, attn_shift, mlp_gain, mlp_shift, up_bias, down_bias)
    sizes = [v.shape[0] * n_fsdp for v in vectors]
    vec_local = jnp.concatenate([v.astype(jnp.bfloat16) for v in vectors])
    low = [w.astype(jnp.bfloat16) for w in (qkv_weight, out_weight, up_weight, down_weight)]
    if small:
        qkv_low, vec_rows = gather_chain(low[0], vec_local, n_dp, n_fsdp)
        out_low, _ = gather_chain(low[1], None, n_dp, n_fsdp)
        up_low, _ = gather_chain(low[2], None, n_dp, n_fsdp)
        down_low, _ = gather_chain(low[3], None, n_dp, n_fsdp)
    else:
        qkv_low, out_low, up_low, down_low = gather_weights_native(low)
        vec_rows = lax.all_gather(vec_local, "fsdp", axis=0, tiled=False)
    (
        query_add,
        value_add,
        out_add,
        gain_one,
        shift_one,
        gain_two,
        shift_two,
        up_add,
        down_add,
    ) = [v.astype(jnp.float32) for v in unpack_vectors(vec_rows, sizes, n_fsdp)]
    is_global = crop_group[0] == 1
    totals = (group_tokens[0] + group_tokens[1]).astype(jnp.float32)
    loss_share = jnp.where(is_global, group_tokens[1], group_tokens[0]).astype(jnp.float32) / totals
    inputs = tokens.astype(jnp.float32)
    scaled_one, inverse_one = normalize(inputs)
    normed_one = (scaled_one * gain_one + shift_one).astype(jnp.bfloat16)
    projected = jnp.dot(normed_one, qkv_low, preferred_element_type=jnp.float32)
    projected = projected + jnp.concatenate([query_add, jnp.zeros_like(query_add), value_add])
    projected_low = projected.astype(jnp.bfloat16)
    queries = projected_low[:, :D]
    key_rows = projected_low[:, D : 2 * D]
    value_rows = projected_low[:, 2 * D :]
    crop = jnp.where(is_global, GLEN, LLEN)
    context, logsum = attend_crops(queries, key_rows, value_rows, crop)
    context_low = context.astype(jnp.bfloat16)
    middle = inputs + (jnp.dot(context_low, out_low, preferred_element_type=jnp.float32) + out_add)
    scaled_two, inverse_two = normalize(middle)
    normed_two = (scaled_two * gain_two + shift_two).astype(jnp.bfloat16)
    preacts = jnp.dot(normed_two, up_low, preferred_element_type=jnp.float32) + up_add
    error_part = 1.0 + jax.scipy.special.erf(preacts * ROOT_HALF)
    activated = (0.5 * preacts * error_part).astype(jnp.bfloat16)
    mixed_out = (
        middle + (jnp.dot(activated, down_low, preferred_element_type=jnp.float32) + down_add)
    ).astype(jnp.bfloat16)
    upstream = cotangent.astype(jnp.float32) * loss_share
    upstream_low = upstream.astype(jnp.bfloat16)
    grad_down_weight = jnp.dot(activated.T, upstream_low, preferred_element_type=jnp.float32)
    grad_down_bias = column_sums(upstream_low)
    grad_activated = jnp.dot(upstream_low, down_low.T, preferred_element_type=jnp.float32)
    slope = 0.5 * error_part + preacts * jnp.exp(-0.5 * preacts * preacts) * INV_ROOT_TAU
    grad_preacts = (grad_activated * slope).astype(jnp.bfloat16)
    grad_up_weight = jnp.dot(normed_two.T, grad_preacts, preferred_element_type=jnp.float32)
    grad_up_bias = column_sums(grad_preacts)
    grad_normed_two = jnp.dot(grad_preacts, up_low.T, preferred_element_type=jnp.float32)
    grad_mlp_gain = jnp.sum(grad_normed_two * scaled_two, axis=0)
    grad_mlp_shift = jnp.sum(grad_normed_two, axis=0)
    grad_middle = upstream + norm_back(grad_normed_two, gain_two, scaled_two, inverse_two)
    grad_branch = grad_middle.astype(jnp.bfloat16)
    grad_out_weight = jnp.dot(context_low.T, grad_branch, preferred_element_type=jnp.float32)
    grad_out_bias = column_sums(grad_branch)
    grad_context = jnp.dot(grad_branch, out_low.T, preferred_element_type=jnp.float32).astype(
        jnp.bfloat16
    )
    grad_projected = attend_crops_back(queries, key_rows, value_rows, logsum, grad_context, crop)
    grad_qkv_weight = jnp.dot(normed_one.T, grad_projected, preferred_element_type=jnp.float32)
    grad_query_bias = column_sums(grad_projected[:, :D])
    grad_value_bias = column_sums(grad_projected[:, 2 * D :])
    grad_normed_one = jnp.dot(grad_projected, qkv_low.T, preferred_element_type=jnp.float32)
    grad_attn_gain = jnp.sum(grad_normed_one * scaled_one, axis=0)
    grad_attn_shift = jnp.sum(grad_normed_one, axis=0)
    grad_tokens = (
        grad_middle + norm_back(grad_normed_one, gain_one, scaled_one, inverse_one)
    ).astype(jnp.bfloat16)
    grad_vectors = (
        grad_query_bias,
        grad_value_bias,
        grad_out_bias,
        grad_attn_gain,
        grad_attn_shift,
        grad_mlp_gain,
        grad_mlp_shift,
        grad_up_bias,
        grad_down_bias,
    )
    vec_grads = jnp.concatenate(
        [g.astype(jnp.bfloat16).reshape(n_fsdp, -1) for g in grad_vectors], axis=1
    )
    if small:
        (grad_down_shard,) = reduce_chain([grad_down_weight], n_dp, n_fsdp)
        (grad_up_shard,) = reduce_chain([grad_up_weight], n_dp, n_fsdp)
        (grad_out_shard,) = reduce_chain([grad_out_weight], n_dp, n_fsdp)
        grad_qkv_shard, vec_flat = reduce_chain(
            [grad_qkv_weight, vec_grads.reshape(n_fsdp * 2 * n_dp, -1)], n_dp, n_fsdp
        )
    else:
        grad_qkv_shard, grad_out_shard, grad_up_shard, grad_down_shard = reduce_weights_native(
            [w.astype(jnp.bfloat16) for w in (grad_qkv_weight, grad_out_weight, grad_up_weight, grad_down_weight)],
        )
        (vec_flat,) = reduce_weights_native([vec_grads])
    vec_out = unpack_vectors(vec_flat.reshape(1, -1), [s // n_fsdp for s in sizes], 1)
    return (
        mixed_out,
        grad_tokens,
        grad_qkv_shard,
        vec_out[0],
        vec_out[1],
        grad_out_shard,
        vec_out[2],
        vec_out[3],
        vec_out[4],
        vec_out[5],
        vec_out[6],
        grad_up_shard,
        vec_out[7],
        grad_down_shard,
        vec_out[8],
    )


def solution(mesh):
    placed = (
        P(("dp", "fsdp"), None),
        P(("dp", "fsdp"), None),
        P("dp"),
        P(),
        P("fsdp", None),
        P("fsdp"),
        P("fsdp"),
        P("fsdp", None),
        P("fsdp"),
        P("fsdp"),
        P("fsdp"),
        P("fsdp"),
        P("fsdp"),
        P("fsdp", None),
        P("fsdp"),
        P("fsdp", None),
        P("fsdp"),
    )
    n_dp = mesh.shape["dp"]
    n_fsdp = mesh.shape["fsdp"]
    return jax.shard_map(
        functools.partial(local_body, n_dp=n_dp, n_fsdp=n_fsdp),
        mesh=mesh,
        in_specs=placed,
        out_specs=(
            P(("dp", "fsdp"), None),
            P(("dp", "fsdp"), None),
            P("fsdp", None),
            P("fsdp"),
            P("fsdp"),
            P("fsdp", None),
            P("fsdp"),
            P("fsdp"),
            P("fsdp"),
            P("fsdp"),
            P("fsdp"),
            P("fsdp", None),
            P("fsdp"),
            P("fsdp", None),
            P("fsdp"),
        ),
        check_vma=False,
    )
```

```python
import functools

import jax
import jax.numpy as jnp
from jax import lax
from jax.sharding import PartitionSpec as P


D = 1024
HEADS = 16
HEAD_DIM = 64
GLEN = 50
LLEN = 10


EPSILON = 1e-06
BIG_NEGATIVE = -1000000000.0
ROOT_HALF = 0.7071067811865476
INV_ROOT_TAU = 0.3989422804014327


def normalize(values):
    middle = jnp.mean(values, axis=-1, keepdims=True)
    centered = values - middle
    inverse = lax.rsqrt(jnp.mean(centered * centered, axis=-1, keepdims=True) + EPSILON)
    return (centered * inverse, inverse)


def norm_back(grad_out, gain, scaled, inverse):
    grad_scaled = grad_out * gain
    return inverse * (
        grad_scaled
        - jnp.mean(grad_scaled, axis=-1, keepdims=True)
        - scaled * jnp.mean(grad_scaled * scaled, axis=-1, keepdims=True)
    )


def by_crops(values, crop):
    return values.reshape(values.shape[0] // crop, crop, HEADS, HEAD_DIM)


def crop_scores(queries, key_rows):
    factor = HEAD_DIM ** (-0.5)
    return (
        jnp.einsum("cqhd,ckhd->chqk", queries, key_rows, preferred_element_type=jnp.float32)
        * factor
    )


def crop_mask(crop):
    segment = lax.iota(jnp.int32, GLEN) // crop
    return segment[:, None] == segment[None, :]


def attend_crops(queries, key_rows, value_rows, crop):
    length = queries.shape[0]
    crop_q, crop_k, crop_v = (
        by_crops(queries, GLEN),
        by_crops(key_rows, GLEN),
        by_crops(value_rows, GLEN),
    )
    scores = jnp.where(crop_mask(crop), crop_scores(crop_q, crop_k), BIG_NEGATIVE)
    highest = jnp.max(scores, axis=-1, keepdims=True)
    exponent = jnp.exp(scores - highest)
    summed = jnp.sum(exponent, axis=-1, keepdims=True)
    attention = (exponent / summed).astype(jnp.bfloat16)
    context = jnp.einsum("chqk,ckhd->cqhd", attention, crop_v, preferred_element_type=jnp.float32)
    logsum = (highest + jnp.log(summed))[..., 0]
    return (
        context.reshape(length, HEADS * HEAD_DIM),
        jnp.transpose(logsum, (0, 2, 1)).reshape(length, HEADS),
    )


def attend_crops_back(queries, key_rows, value_rows, logsum, grad_context, crop):
    length = queries.shape[0]
    factor = HEAD_DIM ** (-0.5)
    crop_q, crop_k, crop_v = (
        by_crops(queries, GLEN),
        by_crops(key_rows, GLEN),
        by_crops(value_rows, GLEN),
    )
    crop_g = by_crops(grad_context, GLEN)
    crop_l = jnp.transpose(logsum.reshape(length // GLEN, GLEN, HEADS), (0, 2, 1))
    scores = jnp.where(crop_mask(crop), crop_scores(crop_q, crop_k), BIG_NEGATIVE)
    probs = jnp.exp(scores - crop_l[..., None])
    probs_low = probs.astype(jnp.bfloat16)
    grad_values = jnp.einsum(
        "chqk,cqhd->ckhd", probs_low, crop_g, preferred_element_type=jnp.float32
    )
    grad_probs = jnp.einsum("cqhd,ckhd->chqk", crop_g, crop_v, preferred_element_type=jnp.float32)
    delta = jnp.sum(probs * grad_probs, axis=-1, keepdims=True)
    grad_scores = (probs * (grad_probs - delta)).astype(jnp.bfloat16)
    grad_queries = (
        jnp.einsum("chqk,ckhd->cqhd", grad_scores, crop_k, preferred_element_type=jnp.float32)
        * factor
    )
    grad_keys = (
        jnp.einsum("chqk,cqhd->ckhd", grad_scores, crop_q, preferred_element_type=jnp.float32)
        * factor
    )
    width = HEADS * HEAD_DIM
    return jnp.concatenate(
        [
            grad_queries.reshape(length, width),
            grad_keys.reshape(length, width),
            grad_values.reshape(length, width),
        ],
        axis=1,
    ).astype(jnp.bfloat16)


def xor_pairs(n, mask):
    return [(i, i ^ mask) for i in range(n)]


def exchange(leaves, held, bit, d, n_dp, lead=0):
    got = lax.ppermute(leaves, "dp", xor_pairs(n_dp, 1 << bit))
    pos = lead + sum(1 for b in held if b > bit)
    mine = ((d >> bit) & 1) == 0
    out = [
        jnp.where(mine, jnp.stack([a, g], axis=pos), jnp.stack([g, a], axis=pos))
        for a, g in zip(leaves, got)
    ]
    return out, sorted(held + [bit], reverse=True)


def split_bit(leaves, held, bit, d, n_dp, lead):
    axis = lead + held.index(bit)
    mine = (d >> bit) & 1
    send = [lax.dynamic_index_in_dim(a, 1 - mine, axis, keepdims=False) for a in leaves]
    keep = [lax.dynamic_index_in_dim(a, mine, axis, keepdims=False) for a in leaves]
    got = lax.ppermute([v.astype(jnp.bfloat16) for v in send], "dp", xor_pairs(n_dp, 1 << bit))
    return [k.astype(jnp.float32) + g.astype(jnp.float32) for k, g in zip(keep, got)], [b for b in held if b != bit]


def chip_bits(n_dp):
    return list(range(1, n_dp.bit_length() - 1))


def gather_chain(shard, vec, n_dp, n_fsdp):
    d = lax.axis_index("dp")
    f = lax.axis_index("fsdp")
    rows, cols = shard.shape
    pieces = shard.reshape(n_dp, 2, rows // (2 * n_dp), cols)
    own = lax.dynamic_index_in_dim(pieces, d, 0, keepdims=False)
    down = [(i, (i - 1) % n_fsdp) for i in range(n_fsdp)]
    ring, vring = [], []
    buf = [own] + ([vec] if vec is not None else [])
    for _ in range(1, n_fsdp):
        buf = lax.ppermute(buf, "fsdp", down)
        ring.append(buf[0])
        if vec is not None:
            vring.append(buf[1])
    vecs = None
    if vec is not None:
        vecs = jnp.roll(jnp.stack([vec] + vring, axis=0), f, axis=0)
    if n_fsdp == 1:
        return shard, vecs
    zrel = jnp.stack(ring, axis=0)
    halves = []
    for h in range(2):
        order = chip_bits(n_dp)
        order = order if h == 0 else order[::-1]
        leaves, held = [zrel[:, h]], []
        for bit in order:
            leaves, held = exchange(leaves, held, bit, d, n_dp, 1)
        halves.append(leaves[0])
    both = jnp.stack(halves, axis=-3)
    held = chip_bits(n_dp)[::-1]
    if n_dp > 1:
        (both,), held = exchange([both], held, 0, d, n_dp, 1)
    plane = both.reshape((n_fsdp - 1, n_dp) + both.shape[-3:])
    rel = jnp.concatenate([pieces[None], plane], axis=0)
    return jnp.roll(rel, f, axis=0).reshape(n_fsdp * rows, cols), vecs


def reduce_chain(grads, n_dp, n_fsdp):
    d = lax.axis_index("dp")
    f = lax.axis_index("fsdp")
    bits = n_dp.bit_length() - 1
    leaves = [
        g.astype(jnp.bfloat16).reshape((n_fsdp,) + (2,) * bits + (2, g.shape[0] // (n_fsdp * 2 * n_dp), g.shape[1]))
        for g in grads
    ]
    held = list(range(bits - 1, -1, -1))
    if bits > 0:
        leaves, held = split_bit(leaves, held, 0, d, n_dp, 1)
    finals = []
    for h in range(2):
        order = chip_bits(n_dp)
        order = order[::-1] if h == 0 else order
        part = [lax.index_in_dim(a, h, 1 + len(held), keepdims=False) for a in leaves]
        hb = list(held)
        for bit in order:
            part, hb = split_bit(part, hb, bit, d, n_dp, 1)
        finals.append(part)
    acc = [jnp.stack([finals[0][i], finals[1][i]], axis=1) for i in range(len(grads))]
    down = [(i, (i - 1) % n_fsdp) for i in range(n_fsdp)]
    if n_fsdp == 1:
        send = [a[0].astype(jnp.bfloat16) for a in acc]
    else:
        send = [lax.dynamic_index_in_dim(a, (f + 1) % n_fsdp, 0, keepdims=False).astype(jnp.bfloat16) for a in acc]
    for step in range(1, n_fsdp):
        got = lax.ppermute(send, "fsdp", down)
        chunk = (f + 1 + step) % n_fsdp
        send = [
            (g.astype(jnp.float32) + lax.dynamic_index_in_dim(a, chunk, 0, keepdims=False)).astype(jnp.bfloat16)
            for g, a in zip(got, acc)
        ]
    halves = []
    for h in range(2):
        order = chip_bits(n_dp)
        order = order if h == 0 else order[::-1]
        part, hb = [v[h] for v in send], []
        for bit in order:
            part, hb = exchange(part, hb, bit, d, n_dp)
        halves.append(part)
    both = [jnp.stack([halves[0][i], halves[1][i]], axis=len(hb)) for i in range(len(grads))]
    if n_dp > 1:
        both, hb = exchange(both, hb, 0, d, n_dp)
    return [b.reshape(g.shape[0] // n_fsdp, g.shape[1]).astype(jnp.float32) for b, g in zip(both, grads)]


def gather_weights_native(shards):
    return [lax.all_gather(s, "fsdp", axis=0, tiled=True) for s in shards]


def reduce_weights_native(grads):
    return [
        lax.psum(lax.psum_scatter(g, "fsdp", scatter_dimension=0, tiled=True), "dp").astype(jnp.float32)
        for g in grads
    ]


def unpack_vectors(packed, sizes, n_fsdp):
    rows = packed.reshape(n_fsdp, -1)
    out = []
    offset = 0
    for size in sizes:
        width = size // n_fsdp
        out.append(rows[:, offset : offset + width].reshape(size))
        offset += width
    return out


def column_sums(values):
    return jnp.sum(values.astype(jnp.float32), axis=0)


def local_body(
    tokens,
    cotangent,
    crop_group,
    group_tokens,
    qkv_weight,
    query_bias,
    value_bias,
    out_weight,
    out_bias,
    attn_gain,
    attn_shift,
    mlp_gain,
    mlp_shift,
    up_weight,
    up_bias,
    down_weight,
    down_bias,
    n_dp,
    n_fsdp,
):
    small = n_dp * n_fsdp <= 64
    vectors = (query_bias, value_bias, out_bias, attn_gain, attn_shift, mlp_gain, mlp_shift, up_bias, down_bias)
    sizes = [v.shape[0] * n_fsdp for v in vectors]
    vec_local = jnp.concatenate([v.astype(jnp.bfloat16) for v in vectors])
    low = [w.astype(jnp.bfloat16) for w in (qkv_weight, out_weight, up_weight, down_weight)]
    if small:
        qkv_low, vec_rows = gather_chain(low[0], vec_local, n_dp, n_fsdp)
        out_low, _ = gather_chain(low[1], None, n_dp, n_fsdp)
        up_low, _ = gather_chain(low[2], None, n_dp, n_fsdp)
        down_low, _ = gather_chain(low[3], None, n_dp, n_fsdp)
    else:
        qkv_low, out_low, up_low, down_low = gather_weights_native(low)
        vec_rows = lax.all_gather(vec_local, "fsdp", axis=0, tiled=False)
    (
        query_add,
        value_add,
        out_add,
        gain_one,
        shift_one,
        gain_two,
        shift_two,
        up_add,
        down_add,
    ) = [v.astype(jnp.float32) for v in unpack_vectors(vec_rows, sizes, n_fsdp)]
    is_global = crop_group[0] == 1
    totals = (group_tokens[0] + group_tokens[1]).astype(jnp.float32)
    loss_share = jnp.where(is_global, group_tokens[1], group_tokens[0]).astype(jnp.float32) / totals
    inputs = tokens.astype(jnp.float32)
    scaled_one, inverse_one = normalize(inputs)
    normed_one = (scaled_one * gain_one + shift_one).astype(jnp.bfloat16)
    projected = jnp.dot(normed_one, qkv_low, preferred_element_type=jnp.float32)
    projected = projected + jnp.concatenate([query_add, jnp.zeros_like(query_add), value_add])
    projected_low = projected.astype(jnp.bfloat16)
    queries = projected_low[:, :D]
    key_rows = projected_low[:, D : 2 * D]
    value_rows = projected_low[:, 2 * D :]
    crop = jnp.where(is_global, GLEN, LLEN)
    context, logsum = attend_crops(queries, key_rows, value_rows, crop)
    context_low = context.astype(jnp.bfloat16)
    middle = inputs + (jnp.dot(context_low, out_low, preferred_element_type=jnp.float32) + out_add)
    scaled_two, inverse_two = normalize(middle)
    normed_two = (scaled_two * gain_two + shift_two).astype(jnp.bfloat16)
    preacts = jnp.dot(normed_two, up_low, preferred_element_type=jnp.float32) + up_add
    error_part = 1.0 + jax.scipy.special.erf(preacts * ROOT_HALF)
    activated = (0.5 * preacts * error_part).astype(jnp.bfloat16)
    mixed_out = (
        middle + (jnp.dot(activated, down_low, preferred_element_type=jnp.float32) + down_add)
    ).astype(jnp.bfloat16)
    upstream = cotangent.astype(jnp.float32) * loss_share
    upstream_low = upstream.astype(jnp.bfloat16)
    grad_down_weight = jnp.dot(activated.T, upstream_low, preferred_element_type=jnp.float32)
    grad_down_bias = column_sums(upstream_low)
    grad_activated = jnp.dot(upstream_low, down_low.T, preferred_element_type=jnp.float32)
    slope = 0.5 * error_part + preacts * jnp.exp(-0.5 * preacts * preacts) * INV_ROOT_TAU
    grad_preacts = (grad_activated * slope).astype(jnp.bfloat16)
    grad_up_weight = jnp.dot(normed_two.T, grad_preacts, preferred_element_type=jnp.float32)
    grad_up_bias = column_sums(grad_preacts)
    grad_normed_two = jnp.dot(grad_preacts, up_low.T, preferred_element_type=jnp.float32)
    grad_mlp_gain = jnp.sum(grad_normed_two * scaled_two, axis=0)
    grad_mlp_shift = jnp.sum(grad_normed_two, axis=0)
    grad_middle = upstream + norm_back(grad_normed_two, gain_two, scaled_two, inverse_two)
    grad_branch = grad_middle.astype(jnp.bfloat16)
    grad_out_weight = jnp.dot(context_low.T, grad_branch, preferred_element_type=jnp.float32)
    grad_out_bias = column_sums(grad_branch)
    grad_context = jnp.dot(grad_branch, out_low.T, preferred_element_type=jnp.float32).astype(
        jnp.bfloat16
    )
    grad_projected = attend_crops_back(queries, key_rows, value_rows, logsum, grad_context, crop)
    grad_qkv_weight = jnp.dot(normed_one.T, grad_projected, preferred_element_type=jnp.float32)
    grad_query_bias = column_sums(grad_projected[:, :D])
    grad_value_bias = column_sums(grad_projected[:, 2 * D :])
    grad_normed_one = jnp.dot(grad_projected, qkv_low.T, preferred_element_type=jnp.float32)
    grad_attn_gain = jnp.sum(grad_normed_one * scaled_one, axis=0)
    grad_attn_shift = jnp.sum(grad_normed_one, axis=0)
    grad_tokens = (
        grad_middle + norm_back(grad_normed_one, gain_one, scaled_one, inverse_one)
    ).astype(jnp.bfloat16)
    grad_vectors = (
        grad_query_bias,
        grad_value_bias,
        grad_out_bias,
        grad_attn_gain,
        grad_attn_shift,
        grad_mlp_gain,
        grad_mlp_shift,
        grad_up_bias,
        grad_down_bias,
    )
    vec_grads = jnp.concatenate(
        [g.astype(jnp.bfloat16).reshape(n_fsdp, -1) for g in grad_vectors], axis=1
    )
    if small:
        (grad_down_shard,) = reduce_chain([grad_down_weight], n_dp, n_fsdp)
        (grad_up_shard,) = reduce_chain([grad_up_weight], n_dp, n_fsdp)
        (grad_out_shard,) = reduce_chain([grad_out_weight], n_dp, n_fsdp)
        grad_qkv_shard, vec_flat = reduce_chain(
            [grad_qkv_weight, vec_grads.reshape(n_fsdp * 2 * n_dp, -1)], n_dp, n_fsdp
        )
    else:
        grad_qkv_shard, grad_out_shard, grad_up_shard, grad_down_shard = reduce_weights_native(
            [w.astype(jnp.bfloat16) for w in (grad_qkv_weight, grad_out_weight, grad_up_weight, grad_down_weight)],
        )
        (vec_flat,) = reduce_weights_native([vec_grads])
    vec_out = unpack_vectors(vec_flat.reshape(1, -1), [s // n_fsdp for s in sizes], 1)
    return (
        mixed_out,
        grad_tokens,
        grad_qkv_shard,
        vec_out[0],
        vec_out[1],
        grad_out_shard,
        vec_out[2],
        vec_out[3],
        vec_out[4],
        vec_out[5],
        vec_out[6],
        grad_up_shard,
        vec_out[7],
        grad_down_shard,
        vec_out[8],
    )


def solution(mesh):
    placed = (
        P(("dp", "fsdp"), None),
        P(("dp", "fsdp"), None),
        P("dp"),
        P(),
        P("fsdp", None),
        P("fsdp"),
        P("fsdp"),
        P("fsdp", None),
        P("fsdp"),
        P("fsdp"),
        P("fsdp"),
        P("fsdp"),
        P("fsdp"),
        P("fsdp", None),
        P("fsdp"),
        P("fsdp", None),
        P("fsdp"),
    )
    n_dp = mesh.shape["dp"]
    n_fsdp = mesh.shape["fsdp"]
    return jax.shard_map(
        functools.partial(local_body, n_dp=n_dp, n_fsdp=n_fsdp),
        mesh=mesh,
        in_specs=placed,
        out_specs=(
            P(("dp", "fsdp"), None),
            P(("dp", "fsdp"), None),
            P("fsdp", None),
            P("fsdp"),
            P("fsdp"),
            P("fsdp", None),
            P("fsdp"),
            P("fsdp"),
            P("fsdp"),
            P("fsdp"),
            P("fsdp"),
            P("fsdp", None),
            P("fsdp"),
            P("fsdp", None),
            P("fsdp"),
        ),
        check_vma=False,
    )
```

```python
import functools

import jax
import jax.numpy as jnp
from jax import lax
from jax.sharding import PartitionSpec as P


D = 1024
HEADS = 16
HEAD_DIM = 64
GLEN = 50
LLEN = 10


EPSILON = 1e-06
BIG_NEGATIVE = -1000000000.0
ROOT_HALF = 0.7071067811865476
INV_ROOT_TAU = 0.3989422804014327


def normalize(values):
    middle = jnp.mean(values, axis=-1, keepdims=True)
    centered = values - middle
    inverse = lax.rsqrt(jnp.mean(centered * centered, axis=-1, keepdims=True) + EPSILON)
    return (centered * inverse, inverse)


def norm_back(grad_out, gain, scaled, inverse):
    grad_scaled = grad_out * gain
    return inverse * (
        grad_scaled
        - jnp.mean(grad_scaled, axis=-1, keepdims=True)
        - scaled * jnp.mean(grad_scaled * scaled, axis=-1, keepdims=True)
    )


def by_crops(values, crop):
    return values.reshape(values.shape[0] // crop, crop, HEADS, HEAD_DIM)


def crop_scores(queries, key_rows):
    factor = HEAD_DIM ** (-0.5)
    return (
        jnp.einsum("cqhd,ckhd->chqk", queries, key_rows, preferred_element_type=jnp.float32)
        * factor
    )


def crop_mask(crop):
    segment = lax.iota(jnp.int32, GLEN) // crop
    return segment[:, None] == segment[None, :]


def attend_crops(queries, key_rows, value_rows, crop):
    length = queries.shape[0]
    crop_q, crop_k, crop_v = (
        by_crops(queries, GLEN),
        by_crops(key_rows, GLEN),
        by_crops(value_rows, GLEN),
    )
    scores = jnp.where(crop_mask(crop), crop_scores(crop_q, crop_k), BIG_NEGATIVE)
    highest = jnp.max(scores, axis=-1, keepdims=True)
    exponent = jnp.exp(scores - highest)
    summed = jnp.sum(exponent, axis=-1, keepdims=True)
    attention = (exponent / summed).astype(jnp.bfloat16)
    context = jnp.einsum("chqk,ckhd->cqhd", attention, crop_v, preferred_element_type=jnp.float32)
    logsum = (highest + jnp.log(summed))[..., 0]
    return (
        context.reshape(length, HEADS * HEAD_DIM),
        jnp.transpose(logsum, (0, 2, 1)).reshape(length, HEADS),
    )


def attend_crops_back(queries, key_rows, value_rows, logsum, grad_context, crop):
    length = queries.shape[0]
    factor = HEAD_DIM ** (-0.5)
    crop_q, crop_k, crop_v = (
        by_crops(queries, GLEN),
        by_crops(key_rows, GLEN),
        by_crops(value_rows, GLEN),
    )
    crop_g = by_crops(grad_context, GLEN)
    crop_l = jnp.transpose(logsum.reshape(length // GLEN, GLEN, HEADS), (0, 2, 1))
    scores = jnp.where(crop_mask(crop), crop_scores(crop_q, crop_k), BIG_NEGATIVE)
    probs = jnp.exp(scores - crop_l[..., None])
    probs_low = probs.astype(jnp.bfloat16)
    grad_values = jnp.einsum(
        "chqk,cqhd->ckhd", probs_low, crop_g, preferred_element_type=jnp.float32
    )
    grad_probs = jnp.einsum("cqhd,ckhd->chqk", crop_g, crop_v, preferred_element_type=jnp.float32)
    delta = jnp.sum(probs * grad_probs, axis=-1, keepdims=True)
    grad_scores = (probs * (grad_probs - delta)).astype(jnp.bfloat16)
    grad_queries = (
        jnp.einsum("chqk,ckhd->cqhd", grad_scores, crop_k, preferred_element_type=jnp.float32)
        * factor
    )
    grad_keys = (
        jnp.einsum("chqk,cqhd->ckhd", grad_scores, crop_q, preferred_element_type=jnp.float32)
        * factor
    )
    width = HEADS * HEAD_DIM
    return jnp.concatenate(
        [
            grad_queries.reshape(length, width),
            grad_keys.reshape(length, width),
            grad_values.reshape(length, width),
        ],
        axis=1,
    ).astype(jnp.bfloat16)


def xor_pairs(n, mask):
    return [(i, i ^ mask) for i in range(n)]


def exchange(leaves, held, bit, d, n_dp, lead=0):
    got = lax.ppermute(leaves, "dp", xor_pairs(n_dp, 1 << bit))
    pos = lead + sum(1 for b in held if b > bit)
    mine = ((d >> bit) & 1) == 0
    out = [
        jnp.where(mine, jnp.stack([a, g], axis=pos), jnp.stack([g, a], axis=pos))
        for a, g in zip(leaves, got)
    ]
    return out, sorted(held + [bit], reverse=True)


def split_bit(leaves, held, bit, d, n_dp, lead):
    axis = lead + held.index(bit)
    mine = (d >> bit) & 1
    send = [lax.dynamic_index_in_dim(a, 1 - mine, axis, keepdims=False) for a in leaves]
    keep = [lax.dynamic_index_in_dim(a, mine, axis, keepdims=False) for a in leaves]
    got = lax.ppermute([v.astype(jnp.bfloat16) for v in send], "dp", xor_pairs(n_dp, 1 << bit))
    return [k.astype(jnp.float32) + g.astype(jnp.float32) for k, g in zip(keep, got)], [b for b in held if b != bit]


def chip_bits(n_dp):
    return list(range(1, n_dp.bit_length() - 1))


def gather_chain(shard, vec, n_dp, n_fsdp):
    d = lax.axis_index("dp")
    f = lax.axis_index("fsdp")
    rows, cols = shard.shape
    pieces = shard.reshape(n_dp, 2, rows // (2 * n_dp), cols)
    own = lax.dynamic_index_in_dim(pieces, d, 0, keepdims=False)
    down = [(i, (i - 1) % n_fsdp) for i in range(n_fsdp)]
    ring, vring = [], []
    buf = [own] + ([vec] if vec is not None else [])
    for _ in range(1, n_fsdp):
        buf = lax.ppermute(buf, "fsdp", down)
        ring.append(buf[0])
        if vec is not None:
            vring.append(buf[1])
    vecs = None
    if vec is not None:
        vecs = jnp.roll(jnp.stack([vec] + vring, axis=0), f, axis=0)
    if n_fsdp == 1:
        return shard, vecs
    zrel = jnp.stack(ring, axis=0)
    halves = []
    for h in range(2):
        order = chip_bits(n_dp)
        order = order if h == 0 else order[::-1]
        leaves, held = [zrel[:, h]], []
        for bit in order:
            leaves, held = exchange(leaves, held, bit, d, n_dp, 1)
        halves.append(leaves[0])
    both = jnp.stack(halves, axis=-3)
    held = chip_bits(n_dp)[::-1]
    if n_dp > 1:
        (both,), held = exchange([both], held, 0, d, n_dp, 1)
    plane = both.reshape((n_fsdp - 1, n_dp) + both.shape[-3:])
    rel = jnp.concatenate([pieces[None], plane], axis=0)
    return jnp.roll(rel, f, axis=0).reshape(n_fsdp * rows, cols), vecs


def reduce_chain(grads, n_dp, n_fsdp):
    d = lax.axis_index("dp")
    f = lax.axis_index("fsdp")
    bits = n_dp.bit_length() - 1
    leaves = [
        g.astype(jnp.bfloat16).reshape((n_fsdp,) + (2,) * bits + (2, g.shape[0] // (n_fsdp * 2 * n_dp), g.shape[1]))
        for g in grads
    ]
    held = list(range(bits - 1, -1, -1))
    if bits > 0:
        leaves, held = split_bit(leaves, held, 0, d, n_dp, 1)
    finals = []
    for h in range(2):
        order = chip_bits(n_dp)
        order = order[::-1] if h == 0 else order
        part = [lax.index_in_dim(a, h, 1 + len(held), keepdims=False) for a in leaves]
        hb = list(held)
        for bit in order:
            part, hb = split_bit(part, hb, bit, d, n_dp, 1)
        finals.append(part)
    acc = [jnp.stack([finals[0][i], finals[1][i]], axis=1) for i in range(len(grads))]
    down = [(i, (i - 1) % n_fsdp) for i in range(n_fsdp)]
    if n_fsdp == 1:
        send = [a[0].astype(jnp.bfloat16) for a in acc]
    else:
        send = [lax.dynamic_index_in_dim(a, (f + 1) % n_fsdp, 0, keepdims=False).astype(jnp.bfloat16) for a in acc]
    for step in range(1, n_fsdp):
        got = lax.ppermute(send, "fsdp", down)
        chunk = (f + 1 + step) % n_fsdp
        send = [
            (g.astype(jnp.float32) + lax.dynamic_index_in_dim(a, chunk, 0, keepdims=False)).astype(jnp.bfloat16)
            for g, a in zip(got, acc)
        ]
    part, hb = send, []
    for bit in chip_bits(n_dp):
        part, hb = exchange(part, hb, bit, d, n_dp)
    both = part
    if n_dp > 1:
        both, hb = exchange(both, hb, 0, d, n_dp)
    return [b.reshape(g.shape[0] // n_fsdp, g.shape[1]).astype(jnp.float32) for b, g in zip(both, grads)]


def gather_weights_native(shards):
    return [lax.all_gather(s, "fsdp", axis=0, tiled=True) for s in shards]


def reduce_weights_native(grads):
    return [
        lax.psum(lax.psum_scatter(g, "fsdp", scatter_dimension=0, tiled=True), "dp").astype(jnp.float32)
        for g in grads
    ]


def unpack_vectors(packed, sizes, n_fsdp):
    rows = packed.reshape(n_fsdp, -1)
    out = []
    offset = 0
    for size in sizes:
        width = size // n_fsdp
        out.append(rows[:, offset : offset + width].reshape(size))
        offset += width
    return out


def column_sums(values):
    return jnp.sum(values.astype(jnp.float32), axis=0)


def local_body(
    tokens,
    cotangent,
    crop_group,
    group_tokens,
    qkv_weight,
    query_bias,
    value_bias,
    out_weight,
    out_bias,
    attn_gain,
    attn_shift,
    mlp_gain,
    mlp_shift,
    up_weight,
    up_bias,
    down_weight,
    down_bias,
    n_dp,
    n_fsdp,
):
    small = n_dp * n_fsdp <= 64
    vectors = (query_bias, value_bias, out_bias, attn_gain, attn_shift, mlp_gain, mlp_shift, up_bias, down_bias)
    sizes = [v.shape[0] * n_fsdp for v in vectors]
    vec_local = jnp.concatenate([v.astype(jnp.bfloat16) for v in vectors])
    low = [w.astype(jnp.bfloat16) for w in (qkv_weight, out_weight, up_weight, down_weight)]
    if small:
        qkv_low, vec_rows = gather_chain(low[0], vec_local, n_dp, n_fsdp)
        out_low, _ = gather_chain(low[1], None, n_dp, n_fsdp)
        up_low, _ = gather_chain(low[2], None, n_dp, n_fsdp)
        down_low, _ = gather_chain(low[3], None, n_dp, n_fsdp)
    else:
        qkv_low, out_low, up_low, down_low = gather_weights_native(low)
        vec_rows = lax.all_gather(vec_local, "fsdp", axis=0, tiled=False)
    (
        query_add,
        value_add,
        out_add,
        gain_one,
        shift_one,
        gain_two,
        shift_two,
        up_add,
        down_add,
    ) = [v.astype(jnp.float32) for v in unpack_vectors(vec_rows, sizes, n_fsdp)]
    is_global = crop_group[0] == 1
    totals = (group_tokens[0] + group_tokens[1]).astype(jnp.float32)
    loss_share = jnp.where(is_global, group_tokens[1], group_tokens[0]).astype(jnp.float32) / totals
    inputs = tokens.astype(jnp.float32)
    scaled_one, inverse_one = normalize(inputs)
    normed_one = (scaled_one * gain_one + shift_one).astype(jnp.bfloat16)
    projected = jnp.dot(normed_one, qkv_low, preferred_element_type=jnp.float32)
    projected = projected + jnp.concatenate([query_add, jnp.zeros_like(query_add), value_add])
    projected_low = projected.astype(jnp.bfloat16)
    queries = projected_low[:, :D]
    key_rows = projected_low[:, D : 2 * D]
    value_rows = projected_low[:, 2 * D :]
    crop = jnp.where(is_global, GLEN, LLEN)
    context, logsum = attend_crops(queries, key_rows, value_rows, crop)
    context_low = context.astype(jnp.bfloat16)
    middle = inputs + (jnp.dot(context_low, out_low, preferred_element_type=jnp.float32) + out_add)
    scaled_two, inverse_two = normalize(middle)
    normed_two = (scaled_two * gain_two + shift_two).astype(jnp.bfloat16)
    preacts = jnp.dot(normed_two, up_low, preferred_element_type=jnp.float32) + up_add
    error_part = 1.0 + jax.scipy.special.erf(preacts * ROOT_HALF)
    activated = (0.5 * preacts * error_part).astype(jnp.bfloat16)
    mixed_out = (
        middle + (jnp.dot(activated, down_low, preferred_element_type=jnp.float32) + down_add)
    ).astype(jnp.bfloat16)
    upstream = cotangent.astype(jnp.float32) * loss_share
    upstream_low = upstream.astype(jnp.bfloat16)
    grad_down_weight = jnp.dot(activated.T, upstream_low, preferred_element_type=jnp.float32)
    grad_down_bias = column_sums(upstream_low)
    grad_activated = jnp.dot(upstream_low, down_low.T, preferred_element_type=jnp.float32)
    slope = 0.5 * error_part + preacts * jnp.exp(-0.5 * preacts * preacts) * INV_ROOT_TAU
    grad_preacts = (grad_activated * slope).astype(jnp.bfloat16)
    grad_up_weight = jnp.dot(normed_two.T, grad_preacts, preferred_element_type=jnp.float32)
    grad_up_bias = column_sums(grad_preacts)
    grad_normed_two = jnp.dot(grad_preacts, up_low.T, preferred_element_type=jnp.float32)
    grad_mlp_gain = jnp.sum(grad_normed_two * scaled_two, axis=0)
    grad_mlp_shift = jnp.sum(grad_normed_two, axis=0)
    grad_middle = upstream + norm_back(grad_normed_two, gain_two, scaled_two, inverse_two)
    grad_branch = grad_middle.astype(jnp.bfloat16)
    grad_out_weight = jnp.dot(context_low.T, grad_branch, preferred_element_type=jnp.float32)
    grad_out_bias = column_sums(grad_branch)
    grad_context = jnp.dot(grad_branch, out_low.T, preferred_element_type=jnp.float32).astype(
        jnp.bfloat16
    )
    grad_projected = attend_crops_back(queries, key_rows, value_rows, logsum, grad_context, crop)
    grad_qkv_weight = jnp.dot(normed_one.T, grad_projected, preferred_element_type=jnp.float32)
    grad_query_bias = column_sums(grad_projected[:, :D])
    grad_value_bias = column_sums(grad_projected[:, 2 * D :])
    grad_normed_one = jnp.dot(grad_projected, qkv_low.T, preferred_element_type=jnp.float32)
    grad_attn_gain = jnp.sum(grad_normed_one * scaled_one, axis=0)
    grad_attn_shift = jnp.sum(grad_normed_one, axis=0)
    grad_tokens = (
        grad_middle + norm_back(grad_normed_one, gain_one, scaled_one, inverse_one)
    ).astype(jnp.bfloat16)
    grad_vectors = (
        grad_query_bias,
        grad_value_bias,
        grad_out_bias,
        grad_attn_gain,
        grad_attn_shift,
        grad_mlp_gain,
        grad_mlp_shift,
        grad_up_bias,
        grad_down_bias,
    )
    vec_grads = jnp.concatenate(
        [g.astype(jnp.bfloat16).reshape(n_fsdp, -1) for g in grad_vectors], axis=1
    )
    if small:
        (grad_down_shard,) = reduce_chain([grad_down_weight], n_dp, n_fsdp)
        (grad_up_shard,) = reduce_chain([grad_up_weight], n_dp, n_fsdp)
        (grad_out_shard,) = reduce_chain([grad_out_weight], n_dp, n_fsdp)
        rows = grad_qkv_weight.shape[0] // (n_fsdp * 2 * n_dp)
        slot = vec_grads.shape[1] // (2 * n_dp)
        if slot % rows == 0:
            qkv_view = grad_qkv_weight.astype(jnp.bfloat16).reshape(n_fsdp, n_dp, 2, rows, -1)
            vec_view = vec_grads.reshape(n_fsdp, n_dp, 2, rows, slot // rows)
            pad = -(slot // rows) % 128
            vec_view = jnp.pad(vec_view, ((0, 0),) * 4 + ((0, pad),))
            joined = jnp.concatenate([qkv_view, vec_view], axis=-1)
            (both_shard,) = reduce_chain([joined.reshape(grad_qkv_weight.shape[0], -1)], n_dp, n_fsdp)
            cols = grad_qkv_weight.shape[1]
            grad_qkv_shard = both_shard[:, :cols]
            vec_flat = both_shard[:, cols : cols + slot // rows].reshape(-1)
        else:
            grad_qkv_shard, vec_flat = reduce_chain(
                [grad_qkv_weight, vec_grads.reshape(n_fsdp * 2 * n_dp, -1)], n_dp, n_fsdp
            )
    else:
        grad_qkv_shard, grad_out_shard, grad_up_shard, grad_down_shard = reduce_weights_native(
            [w.astype(jnp.bfloat16) for w in (grad_qkv_weight, grad_out_weight, grad_up_weight, grad_down_weight)],
        )
        (vec_flat,) = reduce_weights_native([vec_grads])
    vec_out = unpack_vectors(vec_flat.reshape(1, -1), [s // n_fsdp for s in sizes], 1)
    return (
        mixed_out,
        grad_tokens,
        grad_qkv_shard,
        vec_out[0],
        vec_out[1],
        grad_out_shard,
        vec_out[2],
        vec_out[3],
        vec_out[4],
        vec_out[5],
        vec_out[6],
        grad_up_shard,
        vec_out[7],
        grad_down_shard,
        vec_out[8],
    )


def solution(mesh):
    placed = (
        P(("dp", "fsdp"), None),
        P(("dp", "fsdp"), None),
        P("dp"),
        P(),
        P("fsdp", None),
        P("fsdp"),
        P("fsdp"),
        P("fsdp", None),
        P("fsdp"),
        P("fsdp"),
        P("fsdp"),
        P("fsdp"),
        P("fsdp"),
        P("fsdp", None),
        P("fsdp"),
        P("fsdp", None),
        P("fsdp"),
    )
    n_dp = mesh.shape["dp"]
    n_fsdp = mesh.shape["fsdp"]
    return jax.shard_map(
        functools.partial(local_body, n_dp=n_dp, n_fsdp=n_fsdp),
        mesh=mesh,
        in_specs=placed,
        out_specs=(
            P(("dp", "fsdp"), None),
            P(("dp", "fsdp"), None),
            P("fsdp", None),
            P("fsdp"),
            P("fsdp"),
            P("fsdp", None),
            P("fsdp"),
            P("fsdp"),
            P("fsdp"),
            P("fsdp"),
            P("fsdp"),
            P("fsdp", None),
            P("fsdp"),
            P("fsdp", None),
            P("fsdp"),
        ),
        check_vma=False,
    )
```

```python
import functools

import jax
import jax.numpy as jnp
from jax import lax
from jax.sharding import PartitionSpec as P


D = 1024
HEADS = 16
HEAD_DIM = 64
GLEN = 50
LLEN = 10


EPSILON = 1e-06
BIG_NEGATIVE = -1000000000.0
ROOT_HALF = 0.7071067811865476
INV_ROOT_TAU = 0.3989422804014327


def normalize(values):
    middle = jnp.mean(values, axis=-1, keepdims=True)
    centered = values - middle
    inverse = lax.rsqrt(jnp.mean(centered * centered, axis=-1, keepdims=True) + EPSILON)
    return (centered * inverse, inverse)


def norm_back(grad_out, gain, scaled, inverse):
    grad_scaled = grad_out * gain
    return inverse * (
        grad_scaled
        - jnp.mean(grad_scaled, axis=-1, keepdims=True)
        - scaled * jnp.mean(grad_scaled * scaled, axis=-1, keepdims=True)
    )


def by_crops(values, crop):
    return values.reshape(values.shape[0] // crop, crop, HEADS, HEAD_DIM)


def crop_scores(queries, key_rows):
    factor = HEAD_DIM ** (-0.5)
    return (
        jnp.einsum("cqhd,ckhd->chqk", queries, key_rows, preferred_element_type=jnp.float32)
        * factor
    )


def crop_mask(crop):
    segment = lax.iota(jnp.int32, GLEN) // crop
    return segment[:, None] == segment[None, :]


def attend_crops(queries, key_rows, value_rows, crop):
    length = queries.shape[0]
    crop_q, crop_k, crop_v = (
        by_crops(queries, GLEN),
        by_crops(key_rows, GLEN),
        by_crops(value_rows, GLEN),
    )
    scores = jnp.where(crop_mask(crop), crop_scores(crop_q, crop_k), BIG_NEGATIVE)
    highest = jnp.max(scores, axis=-1, keepdims=True)
    exponent = jnp.exp(scores - highest)
    summed = jnp.sum(exponent, axis=-1, keepdims=True)
    attention = (exponent / summed).astype(jnp.bfloat16)
    context = jnp.einsum("chqk,ckhd->cqhd", attention, crop_v, preferred_element_type=jnp.float32)
    logsum = (highest + jnp.log(summed))[..., 0]
    return (
        context.reshape(length, HEADS * HEAD_DIM),
        jnp.transpose(logsum, (0, 2, 1)).reshape(length, HEADS),
    )


def attend_crops_back(queries, key_rows, value_rows, logsum, grad_context, crop):
    length = queries.shape[0]
    factor = HEAD_DIM ** (-0.5)
    crop_q, crop_k, crop_v = (
        by_crops(queries, GLEN),
        by_crops(key_rows, GLEN),
        by_crops(value_rows, GLEN),
    )
    crop_g = by_crops(grad_context, GLEN)
    crop_l = jnp.transpose(logsum.reshape(length // GLEN, GLEN, HEADS), (0, 2, 1))
    scores = jnp.where(crop_mask(crop), crop_scores(crop_q, crop_k), BIG_NEGATIVE)
    probs = jnp.exp(scores - crop_l[..., None])
    probs_low = probs.astype(jnp.bfloat16)
    grad_values = jnp.einsum(
        "chqk,cqhd->ckhd", probs_low, crop_g, preferred_element_type=jnp.float32
    )
    grad_probs = jnp.einsum("cqhd,ckhd->chqk", crop_g, crop_v, preferred_element_type=jnp.float32)
    delta = jnp.sum(probs * grad_probs, axis=-1, keepdims=True)
    grad_scores = (probs * (grad_probs - delta)).astype(jnp.bfloat16)
    grad_queries = (
        jnp.einsum("chqk,ckhd->cqhd", grad_scores, crop_k, preferred_element_type=jnp.float32)
        * factor
    )
    grad_keys = (
        jnp.einsum("chqk,cqhd->ckhd", grad_scores, crop_q, preferred_element_type=jnp.float32)
        * factor
    )
    width = HEADS * HEAD_DIM
    return jnp.concatenate(
        [
            grad_queries.reshape(length, width),
            grad_keys.reshape(length, width),
            grad_values.reshape(length, width),
        ],
        axis=1,
    ).astype(jnp.bfloat16)


def xor_pairs(n, mask):
    return [(i, i ^ mask) for i in range(n)]


def exchange(leaves, held, bit, d, n_dp, lead=0):
    got = lax.ppermute(leaves, "dp", xor_pairs(n_dp, 1 << bit))
    pos = lead + sum(1 for b in held if b > bit)
    mine = ((d >> bit) & 1) == 0
    out = [
        jnp.where(mine, jnp.stack([a, g], axis=pos), jnp.stack([g, a], axis=pos))
        for a, g in zip(leaves, got)
    ]
    return out, sorted(held + [bit], reverse=True)


def split_bit(leaves, held, bit, d, n_dp, lead):
    axis = lead + held.index(bit)
    mine = (d >> bit) & 1
    send = [lax.dynamic_index_in_dim(a, 1 - mine, axis, keepdims=False) for a in leaves]
    keep = [lax.dynamic_index_in_dim(a, mine, axis, keepdims=False) for a in leaves]
    got = lax.ppermute([v.astype(jnp.bfloat16) for v in send], "dp", xor_pairs(n_dp, 1 << bit))
    return [k.astype(jnp.float32) + g.astype(jnp.float32) for k, g in zip(keep, got)], [b for b in held if b != bit]


def chip_bits(n_dp):
    return list(range(1, n_dp.bit_length() - 1))


def gather_chain(shard, vec, n_dp, n_fsdp):
    d = lax.axis_index("dp")
    f = lax.axis_index("fsdp")
    rows, cols = shard.shape
    pieces = shard.reshape(n_dp, 2, rows // (2 * n_dp), cols)
    own = lax.dynamic_index_in_dim(pieces, d, 0, keepdims=False)
    down = [(i, (i - 1) % n_fsdp) for i in range(n_fsdp)]
    ring, vring = [], []
    buf = [own] + ([vec] if vec is not None else [])
    for _ in range(1, n_fsdp):
        buf = lax.ppermute(buf, "fsdp", down)
        ring.append(buf[0])
        if vec is not None:
            vring.append(buf[1])
    vecs = None
    if vec is not None:
        vecs = jnp.roll(jnp.stack([vec] + vring, axis=0), f, axis=0)
    if n_fsdp == 1:
        return shard, vecs
    zrel = jnp.stack(ring, axis=0)
    halves = []
    for h in range(2):
        order = chip_bits(n_dp)
        order = order if h == 0 else order[::-1]
        leaves, held = [zrel[:, h]], []
        for bit in order:
            leaves, held = exchange(leaves, held, bit, d, n_dp, 1)
        halves.append(leaves[0])
    both = jnp.stack(halves, axis=-3)
    held = chip_bits(n_dp)[::-1]
    if n_dp > 1:
        (both,), held = exchange([both], held, 0, d, n_dp, 1)
    plane = both.reshape((n_fsdp - 1, n_dp) + both.shape[-3:])
    rel = jnp.concatenate([pieces[None], plane], axis=0)
    return jnp.roll(rel, f, axis=0).reshape(n_fsdp * rows, cols), vecs


def reduce_chain(grads, n_dp, n_fsdp):
    d = lax.axis_index("dp")
    f = lax.axis_index("fsdp")
    bits = n_dp.bit_length() - 1
    leaves = [
        g.astype(jnp.bfloat16).reshape((n_fsdp,) + (2,) * bits + (2, g.shape[0] // (n_fsdp * 2 * n_dp), g.shape[1]))
        for g in grads
    ]
    held = list(range(bits - 1, -1, -1))
    if bits > 0:
        leaves, held = split_bit(leaves, held, 0, d, n_dp, 1)
    finals = []
    for h in range(2):
        order = chip_bits(n_dp)
        order = order[::-1] if h == 0 else order
        part = [lax.index_in_dim(a, h, 1 + len(held), keepdims=False) for a in leaves]
        hb = list(held)
        for bit in order:
            part, hb = split_bit(part, hb, bit, d, n_dp, 1)
        finals.append(part)
    acc = [jnp.stack([finals[0][i], finals[1][i]], axis=1) for i in range(len(grads))]
    down = [(i, (i - 1) % n_fsdp) for i in range(n_fsdp)]
    if n_fsdp == 1:
        send = [a[0].astype(jnp.bfloat16) for a in acc]
    else:
        send = [lax.dynamic_index_in_dim(a, (f + 1) % n_fsdp, 0, keepdims=False).astype(jnp.bfloat16) for a in acc]
    for step in range(1, n_fsdp):
        got = lax.ppermute(send, "fsdp", down)
        chunk = (f + 1 + step) % n_fsdp
        send = [
            (g.astype(jnp.float32) + lax.dynamic_index_in_dim(a, chunk, 0, keepdims=False)).astype(jnp.bfloat16)
            for g, a in zip(got, acc)
        ]
    part, hb = send, []
    for bit in chip_bits(n_dp):
        part, hb = exchange(part, hb, bit, d, n_dp)
    both = part
    if n_dp > 1:
        both, hb = exchange(both, hb, 0, d, n_dp)
    return [b.reshape(g.shape[0] // n_fsdp, g.shape[1]).astype(jnp.float32) for b, g in zip(both, grads)]


def gather_weights_native(shards):
    return [lax.all_gather(s, "fsdp", axis=0, tiled=True) for s in shards]


def reduce_weights_native(grads):
    return [
        lax.psum(lax.psum_scatter(g, "fsdp", scatter_dimension=0, tiled=True), "dp").astype(jnp.float32)
        for g in grads
    ]


def unpack_vectors(packed, sizes, n_fsdp):
    rows = packed.reshape(n_fsdp, -1)
    out = []
    offset = 0
    for size in sizes:
        width = size // n_fsdp
        out.append(rows[:, offset : offset + width].reshape(size))
        offset += width
    return out


def column_sums(values):
    return jnp.sum(values.astype(jnp.float32), axis=0)


def local_body(
    tokens,
    cotangent,
    crop_group,
    group_tokens,
    qkv_weight,
    query_bias,
    value_bias,
    out_weight,
    out_bias,
    attn_gain,
    attn_shift,
    mlp_gain,
    mlp_shift,
    up_weight,
    up_bias,
    down_weight,
    down_bias,
    n_dp,
    n_fsdp,
):
    small = n_dp * n_fsdp <= 64
    vectors = (query_bias, value_bias, out_bias, attn_gain, attn_shift, mlp_gain, mlp_shift, up_bias, down_bias)
    sizes = [v.shape[0] * n_fsdp for v in vectors]
    vec_local = jnp.concatenate([v.astype(jnp.bfloat16) for v in vectors])
    low = [w.astype(jnp.bfloat16) for w in (qkv_weight, out_weight, up_weight, down_weight)]
    if small:
        qkv_low, vec_rows = gather_chain(low[0], vec_local, n_dp, n_fsdp)
        out_low, _ = gather_chain(low[1], None, n_dp, n_fsdp)
        up_low, _ = gather_chain(low[2], None, n_dp, n_fsdp)
        down_low, _ = gather_chain(low[3], None, n_dp, n_fsdp)
    else:
        qkv_low, out_low, up_low, down_low = gather_weights_native(low)
        vec_rows = lax.all_gather(vec_local, "fsdp", axis=0, tiled=False)
    (
        query_add,
        value_add,
        out_add,
        gain_one,
        shift_one,
        gain_two,
        shift_two,
        up_add,
        down_add,
    ) = [v.astype(jnp.float32) for v in unpack_vectors(vec_rows, sizes, n_fsdp)]
    is_global = crop_group[0] == 1
    totals = (group_tokens[0] + group_tokens[1]).astype(jnp.float32)
    loss_share = jnp.where(is_global, group_tokens[1], group_tokens[0]).astype(jnp.float32) / totals
    inputs = tokens.astype(jnp.float32)
    scaled_one, inverse_one = normalize(inputs)
    normed_one = (scaled_one * gain_one + shift_one).astype(jnp.bfloat16)
    projected = jnp.dot(normed_one, qkv_low, preferred_element_type=jnp.float32)
    projected = projected + jnp.concatenate([query_add, jnp.zeros_like(query_add), value_add])
    projected_low = projected.astype(jnp.bfloat16)
    queries = projected_low[:, :D]
    key_rows = projected_low[:, D : 2 * D]
    value_rows = projected_low[:, 2 * D :]
    crop = jnp.where(is_global, GLEN, LLEN)
    context, logsum = attend_crops(queries, key_rows, value_rows, crop)
    context_low = context.astype(jnp.bfloat16)
    middle = inputs + (jnp.dot(context_low, out_low, preferred_element_type=jnp.float32) + out_add)
    scaled_two, inverse_two = normalize(middle)
    normed_two = (scaled_two * gain_two + shift_two).astype(jnp.bfloat16)
    preacts = jnp.dot(normed_two, up_low, preferred_element_type=jnp.float32) + up_add
    error_part = 1.0 + jax.scipy.special.erf(preacts * ROOT_HALF)
    activated = (0.5 * preacts * error_part).astype(jnp.bfloat16)
    mixed_out = (
        middle + (jnp.dot(activated, down_low, preferred_element_type=jnp.float32) + down_add)
    ).astype(jnp.bfloat16)
    upstream = cotangent.astype(jnp.float32) * loss_share
    upstream_low = upstream.astype(jnp.bfloat16)
    grad_down_weight = jnp.dot(activated.T, upstream_low, preferred_element_type=jnp.float32)
    grad_down_bias = column_sums(upstream_low)
    grad_activated = jnp.dot(upstream_low, down_low.T, preferred_element_type=jnp.float32)
    slope = 0.5 * error_part + preacts * jnp.exp(-0.5 * preacts * preacts) * INV_ROOT_TAU
    grad_preacts = (grad_activated * slope).astype(jnp.bfloat16)
    grad_up_weight = jnp.dot(normed_two.T, grad_preacts, preferred_element_type=jnp.float32)
    grad_up_bias = column_sums(grad_preacts)
    grad_normed_two = jnp.dot(grad_preacts, up_low.T, preferred_element_type=jnp.float32)
    grad_mlp_gain = jnp.sum(grad_normed_two * scaled_two, axis=0)
    grad_mlp_shift = jnp.sum(grad_normed_two, axis=0)
    grad_middle = upstream + norm_back(grad_normed_two, gain_two, scaled_two, inverse_two)
    grad_branch = grad_middle.astype(jnp.bfloat16)
    grad_out_weight = jnp.dot(context_low.T, grad_branch, preferred_element_type=jnp.float32)
    grad_out_bias = column_sums(grad_branch)
    grad_context = jnp.dot(grad_branch, out_low.T, preferred_element_type=jnp.float32).astype(
        jnp.bfloat16
    )
    grad_projected = attend_crops_back(queries, key_rows, value_rows, logsum, grad_context, crop)
    grad_qkv_weight = jnp.dot(normed_one.T, grad_projected, preferred_element_type=jnp.float32)
    grad_query_bias = column_sums(grad_projected[:, :D])
    grad_value_bias = column_sums(grad_projected[:, 2 * D :])
    grad_normed_one = jnp.dot(grad_projected, qkv_low.T, preferred_element_type=jnp.float32)
    grad_attn_gain = jnp.sum(grad_normed_one * scaled_one, axis=0)
    grad_attn_shift = jnp.sum(grad_normed_one, axis=0)
    grad_tokens = (
        grad_middle + norm_back(grad_normed_one, gain_one, scaled_one, inverse_one)
    ).astype(jnp.bfloat16)
    grad_vectors = (
        grad_query_bias,
        grad_value_bias,
        grad_out_bias,
        grad_attn_gain,
        grad_attn_shift,
        grad_mlp_gain,
        grad_mlp_shift,
        grad_up_bias,
        grad_down_bias,
    )
    vec_grads = jnp.concatenate(
        [g.astype(jnp.bfloat16).reshape(n_fsdp, -1) for g in grad_vectors], axis=1
    )
    if small:
        width = grad_down_weight.shape[1]
        up_view = grad_up_weight.astype(jnp.bfloat16).reshape(n_fsdp, n_dp, 2, -1, width)
        down_view = grad_down_weight.astype(jnp.bfloat16).reshape(n_fsdp, n_dp, 2, -1, width)
        split = up_view.shape[3]
        mlp = jnp.concatenate([up_view, down_view], axis=3)
        (mlp_shard,) = reduce_chain([mlp.reshape(-1, width)], n_dp, n_fsdp)
        mlp_shard = mlp_shard.reshape(n_dp, 2, -1, width)
        grad_up_shard = mlp_shard[:, :, :split].reshape(grad_up_weight.shape[0] // n_fsdp, -1)
        grad_down_shard = mlp_shard[:, :, split:].reshape(grad_down_weight.shape[0] // n_fsdp, -1)
        (grad_out_shard,) = reduce_chain([grad_out_weight], n_dp, n_fsdp)
        rows = grad_qkv_weight.shape[0] // (n_fsdp * 2 * n_dp)
        slot = vec_grads.shape[1] // (2 * n_dp)
        if slot % rows == 0:
            qkv_view = grad_qkv_weight.astype(jnp.bfloat16).reshape(n_fsdp, n_dp, 2, rows, -1)
            vec_view = vec_grads.reshape(n_fsdp, n_dp, 2, rows, slot // rows)
            pad = -(slot // rows) % 128
            vec_view = jnp.pad(vec_view, ((0, 0),) * 4 + ((0, pad),))
            joined = jnp.concatenate([qkv_view, vec_view], axis=-1)
            (both_shard,) = reduce_chain([joined.reshape(grad_qkv_weight.shape[0], -1)], n_dp, n_fsdp)
            cols = grad_qkv_weight.shape[1]
            grad_qkv_shard = both_shard[:, :cols]
            vec_flat = both_shard[:, cols : cols + slot // rows].reshape(-1)
        else:
            grad_qkv_shard, vec_flat = reduce_chain(
                [grad_qkv_weight, vec_grads.reshape(n_fsdp * 2 * n_dp, -1)], n_dp, n_fsdp
            )
    else:
        grad_qkv_shard, grad_out_shard, grad_up_shard, grad_down_shard = reduce_weights_native(
            [w.astype(jnp.bfloat16) for w in (grad_qkv_weight, grad_out_weight, grad_up_weight, grad_down_weight)],
        )
        (vec_flat,) = reduce_weights_native([vec_grads])
    vec_out = unpack_vectors(vec_flat.reshape(1, -1), [s // n_fsdp for s in sizes], 1)
    return (
        mixed_out,
        grad_tokens,
        grad_qkv_shard,
        vec_out[0],
        vec_out[1],
        grad_out_shard,
        vec_out[2],
        vec_out[3],
        vec_out[4],
        vec_out[5],
        vec_out[6],
        grad_up_shard,
        vec_out[7],
        grad_down_shard,
        vec_out[8],
    )


def solution(mesh):
    placed = (
        P(("dp", "fsdp"), None),
        P(("dp", "fsdp"), None),
        P("dp"),
        P(),
        P("fsdp", None),
        P("fsdp"),
        P("fsdp"),
        P("fsdp", None),
        P("fsdp"),
        P("fsdp"),
        P("fsdp"),
        P("fsdp"),
        P("fsdp"),
        P("fsdp", None),
        P("fsdp"),
        P("fsdp", None),
        P("fsdp"),
    )
    n_dp = mesh.shape["dp"]
    n_fsdp = mesh.shape["fsdp"]
    return jax.shard_map(
        functools.partial(local_body, n_dp=n_dp, n_fsdp=n_fsdp),
        mesh=mesh,
        in_specs=placed,
        out_specs=(
            P(("dp", "fsdp"), None),
            P(("dp", "fsdp"), None),
            P("fsdp", None),
            P("fsdp"),
            P("fsdp"),
            P("fsdp", None),
            P("fsdp"),
            P("fsdp"),
            P("fsdp"),
            P("fsdp"),
            P("fsdp"),
            P("fsdp", None),
            P("fsdp"),
            P("fsdp", None),
            P("fsdp"),
        ),
        check_vma=False,
    )
```

```python
import functools

import jax
import jax.numpy as jnp
from jax import lax
from jax.sharding import PartitionSpec as P


D = 1024
HEADS = 16
HEAD_DIM = 64
GLEN = 50
LLEN = 10


EPSILON = 1e-06
BIG_NEGATIVE = -1000000000.0
ROOT_HALF = 0.7071067811865476
INV_ROOT_TAU = 0.3989422804014327


def normalize(values):
    middle = jnp.mean(values, axis=-1, keepdims=True)
    centered = values - middle
    inverse = lax.rsqrt(jnp.mean(centered * centered, axis=-1, keepdims=True) + EPSILON)
    return (centered * inverse, inverse)


def norm_back(grad_out, gain, scaled, inverse):
    grad_scaled = grad_out * gain
    return inverse * (
        grad_scaled
        - jnp.mean(grad_scaled, axis=-1, keepdims=True)
        - scaled * jnp.mean(grad_scaled * scaled, axis=-1, keepdims=True)
    )


def by_crops(values, crop):
    return values.reshape(values.shape[0] // crop, crop, HEADS, HEAD_DIM)


def crop_scores(queries, key_rows):
    factor = HEAD_DIM ** (-0.5)
    return (
        jnp.einsum("cqhd,ckhd->chqk", queries, key_rows, preferred_element_type=jnp.float32)
        * factor
    )


def crop_mask(crop):
    segment = lax.iota(jnp.int32, GLEN) // crop
    return segment[:, None] == segment[None, :]


def attend_crops(queries, key_rows, value_rows, crop):
    length = queries.shape[0]
    crop_q, crop_k, crop_v = (
        by_crops(queries, GLEN),
        by_crops(key_rows, GLEN),
        by_crops(value_rows, GLEN),
    )
    scores = jnp.where(crop_mask(crop), crop_scores(crop_q, crop_k), BIG_NEGATIVE)
    highest = jnp.max(scores, axis=-1, keepdims=True)
    exponent = jnp.exp(scores - highest)
    summed = jnp.sum(exponent, axis=-1, keepdims=True)
    attention = (exponent / summed).astype(jnp.bfloat16)
    context = jnp.einsum("chqk,ckhd->cqhd", attention, crop_v, preferred_element_type=jnp.float32)
    logsum = (highest + jnp.log(summed))[..., 0]
    return (
        context.reshape(length, HEADS * HEAD_DIM),
        jnp.transpose(logsum, (0, 2, 1)).reshape(length, HEADS),
    )


def attend_crops_back(queries, key_rows, value_rows, logsum, grad_context, crop):
    length = queries.shape[0]
    factor = HEAD_DIM ** (-0.5)
    crop_q, crop_k, crop_v = (
        by_crops(queries, GLEN),
        by_crops(key_rows, GLEN),
        by_crops(value_rows, GLEN),
    )
    crop_g = by_crops(grad_context, GLEN)
    crop_l = jnp.transpose(logsum.reshape(length // GLEN, GLEN, HEADS), (0, 2, 1))
    scores = jnp.where(crop_mask(crop), crop_scores(crop_q, crop_k), BIG_NEGATIVE)
    probs = jnp.exp(scores - crop_l[..., None])
    probs_low = probs.astype(jnp.bfloat16)
    grad_values = jnp.einsum(
        "chqk,cqhd->ckhd", probs_low, crop_g, preferred_element_type=jnp.float32
    )
    grad_probs = jnp.einsum("cqhd,ckhd->chqk", crop_g, crop_v, preferred_element_type=jnp.float32)
    delta = jnp.sum(probs * grad_probs, axis=-1, keepdims=True)
    grad_scores = (probs * (grad_probs - delta)).astype(jnp.bfloat16)
    grad_queries = (
        jnp.einsum("chqk,ckhd->cqhd", grad_scores, crop_k, preferred_element_type=jnp.float32)
        * factor
    )
    grad_keys = (
        jnp.einsum("chqk,cqhd->ckhd", grad_scores, crop_q, preferred_element_type=jnp.float32)
        * factor
    )
    width = HEADS * HEAD_DIM
    return jnp.concatenate(
        [
            grad_queries.reshape(length, width),
            grad_keys.reshape(length, width),
            grad_values.reshape(length, width),
        ],
        axis=1,
    ).astype(jnp.bfloat16)


def xor_pairs(n, mask):
    return [(i, i ^ mask) for i in range(n)]


def exchange(leaves, held, bit, d, n_dp, lead=0):
    got = lax.ppermute(leaves, "dp", xor_pairs(n_dp, 1 << bit))
    pos = lead + sum(1 for b in held if b > bit)
    mine = ((d >> bit) & 1) == 0
    out = [
        jnp.where(mine, jnp.stack([a, g], axis=pos), jnp.stack([g, a], axis=pos))
        for a, g in zip(leaves, got)
    ]
    return out, sorted(held + [bit], reverse=True)


def split_bit(leaves, held, bit, d, n_dp, lead):
    axis = lead + held.index(bit)
    mine = (d >> bit) & 1
    send = [lax.dynamic_index_in_dim(a, 1 - mine, axis, keepdims=False) for a in leaves]
    keep = [lax.dynamic_index_in_dim(a, mine, axis, keepdims=False) for a in leaves]
    got = lax.ppermute([v.astype(jnp.bfloat16) for v in send], "dp", xor_pairs(n_dp, 1 << bit))
    return [k.astype(jnp.float32) + g.astype(jnp.float32) for k, g in zip(keep, got)], [b for b in held if b != bit]


def chip_bits(n_dp):
    return list(range(1, n_dp.bit_length() - 1))


def gather_chain(shard, vec, n_dp, n_fsdp):
    d = lax.axis_index("dp")
    f = lax.axis_index("fsdp")
    rows, cols = shard.shape
    pieces = shard.reshape(n_dp, 2, rows // (2 * n_dp), cols)
    own = lax.dynamic_index_in_dim(pieces, d, 0, keepdims=False)
    down = [(i, (i - 1) % n_fsdp) for i in range(n_fsdp)]
    ring, vring = [], []
    buf = [own] + ([vec] if vec is not None else [])
    for _ in range(1, n_fsdp):
        buf = lax.ppermute(buf, "fsdp", down)
        ring.append(buf[0])
        if vec is not None:
            vring.append(buf[1])
    vecs = None
    if vec is not None:
        vecs = jnp.roll(jnp.stack([vec] + vring, axis=0), f, axis=0)
    if n_fsdp == 1:
        return shard, vecs
    zrel = jnp.stack(ring, axis=0)
    halves = []
    for h in range(2):
        order = chip_bits(n_dp)
        order = order if h == 0 else order[::-1]
        leaves, held = [zrel[:, h]], []
        for bit in order:
            leaves, held = exchange(leaves, held, bit, d, n_dp, 1)
        halves.append(leaves[0])
    both = jnp.stack(halves, axis=-3)
    held = chip_bits(n_dp)[::-1]
    if n_dp > 1:
        (both,), held = exchange([both], held, 0, d, n_dp, 1)
    plane = both.reshape((n_fsdp - 1, n_dp) + both.shape[-3:])
    rel = jnp.concatenate([pieces[None], plane], axis=0)
    return jnp.roll(rel, f, axis=0).reshape(n_fsdp * rows, cols), vecs


def reduce_chain(grads, n_dp, n_fsdp):
    d = lax.axis_index("dp")
    f = lax.axis_index("fsdp")
    bits = n_dp.bit_length() - 1
    leaves = [
        g.astype(jnp.bfloat16).reshape((n_fsdp,) + (2,) * bits + (2, g.shape[0] // (n_fsdp * 2 * n_dp), g.shape[1]))
        for g in grads
    ]
    held = list(range(bits - 1, -1, -1))
    if bits > 0:
        leaves, held = split_bit(leaves, held, 0, d, n_dp, 1)
    finals = []
    for h in range(2):
        order = chip_bits(n_dp)
        order = order[::-1] if h == 0 else order
        part = [lax.index_in_dim(a, h, 1 + len(held), keepdims=False) for a in leaves]
        hb = list(held)
        for bit in order:
            part, hb = split_bit(part, hb, bit, d, n_dp, 1)
        finals.append(part)
    acc = [jnp.stack([finals[0][i], finals[1][i]], axis=1) for i in range(len(grads))]
    down = [(i, (i - 1) % n_fsdp) for i in range(n_fsdp)]
    if n_fsdp == 1:
        send = [a[0].astype(jnp.bfloat16) for a in acc]
    else:
        send = [lax.dynamic_index_in_dim(a, (f + 1) % n_fsdp, 0, keepdims=False).astype(jnp.bfloat16) for a in acc]
    for step in range(1, n_fsdp):
        got = lax.ppermute(send, "fsdp", down)
        chunk = (f + 1 + step) % n_fsdp
        send = [
            (g.astype(jnp.float32) + lax.dynamic_index_in_dim(a, chunk, 0, keepdims=False)).astype(jnp.bfloat16)
            for g, a in zip(got, acc)
        ]
    part, hb = send, []
    for bit in chip_bits(n_dp):
        part, hb = exchange(part, hb, bit, d, n_dp)
    both = part
    if n_dp > 1:
        both, hb = exchange(both, hb, 0, d, n_dp)
    return [b.reshape(g.shape[0] // n_fsdp, g.shape[1]).astype(jnp.float32) for b, g in zip(both, grads)]


def gather_weights_native(shards):
    return [lax.all_gather(s, "fsdp", axis=0, tiled=True) for s in shards]


def reduce_weights_native(grads):
    return [
        lax.psum(lax.psum_scatter(g, "fsdp", scatter_dimension=0, tiled=True), "dp").astype(jnp.float32)
        for g in grads
    ]


def unpack_vectors(packed, sizes, n_fsdp):
    rows = packed.reshape(n_fsdp, -1)
    out = []
    offset = 0
    for size in sizes:
        width = size // n_fsdp
        out.append(rows[:, offset : offset + width].reshape(size))
        offset += width
    return out


def column_sums(values):
    return jnp.sum(values.astype(jnp.float32), axis=0)


def local_body(
    tokens,
    cotangent,
    crop_group,
    group_tokens,
    qkv_weight,
    query_bias,
    value_bias,
    out_weight,
    out_bias,
    attn_gain,
    attn_shift,
    mlp_gain,
    mlp_shift,
    up_weight,
    up_bias,
    down_weight,
    down_bias,
    n_dp,
    n_fsdp,
):
    small = n_dp * n_fsdp <= 64
    vectors = (query_bias, value_bias, out_bias, attn_gain, attn_shift, mlp_gain, mlp_shift, up_bias, down_bias)
    sizes = [v.shape[0] * n_fsdp for v in vectors]
    vec_local = jnp.concatenate([v.astype(jnp.bfloat16) for v in vectors])
    low = [w.astype(jnp.bfloat16) for w in (qkv_weight, out_weight, up_weight, down_weight)]
    if small:
        rows = low[0].shape[0] // (2 * n_dp)
        slot = vec_local.shape[0] // (2 * n_dp)
        if slot % rows == 0:
            cols = low[0].shape[1]
            vec_view = vec_local.reshape(2 * n_dp * rows, slot // rows)
            vec_view = jnp.pad(vec_view, ((0, 0), (0, -(slot // rows) % 128)))
            joined, _ = gather_chain(jnp.concatenate([low[0], vec_view], axis=1), None, n_dp, n_fsdp)
            qkv_low = joined[:, :cols]
            vec_rows = joined[:, cols : cols + slot // rows].reshape(n_fsdp, -1)
        else:
            qkv_low, vec_rows = gather_chain(low[0], vec_local, n_dp, n_fsdp)
        out_low, _ = gather_chain(low[1], None, n_dp, n_fsdp)
        up_low, _ = gather_chain(low[2], None, n_dp, n_fsdp)
        down_low, _ = gather_chain(low[3], None, n_dp, n_fsdp)
    else:
        qkv_low, out_low, up_low, down_low = gather_weights_native(low)
        vec_rows = lax.all_gather(vec_local, "fsdp", axis=0, tiled=False)
    (
        query_add,
        value_add,
        out_add,
        gain_one,
        shift_one,
        gain_two,
        shift_two,
        up_add,
        down_add,
    ) = [v.astype(jnp.float32) for v in unpack_vectors(vec_rows, sizes, n_fsdp)]
    is_global = crop_group[0] == 1
    totals = (group_tokens[0] + group_tokens[1]).astype(jnp.float32)
    loss_share = jnp.where(is_global, group_tokens[1], group_tokens[0]).astype(jnp.float32) / totals
    inputs = tokens.astype(jnp.float32)
    scaled_one, inverse_one = normalize(inputs)
    normed_one = (scaled_one * gain_one + shift_one).astype(jnp.bfloat16)
    projected = jnp.dot(normed_one, qkv_low, preferred_element_type=jnp.float32)
    projected = projected + jnp.concatenate([query_add, jnp.zeros_like(query_add), value_add])
    projected_low = projected.astype(jnp.bfloat16)
    queries = projected_low[:, :D]
    key_rows = projected_low[:, D : 2 * D]
    value_rows = projected_low[:, 2 * D :]
    crop = jnp.where(is_global, GLEN, LLEN)
    context, logsum = attend_crops(queries, key_rows, value_rows, crop)
    context_low = context.astype(jnp.bfloat16)
    middle = inputs + (jnp.dot(context_low, out_low, preferred_element_type=jnp.float32) + out_add)
    scaled_two, inverse_two = normalize(middle)
    normed_two = (scaled_two * gain_two + shift_two).astype(jnp.bfloat16)
    preacts = jnp.dot(normed_two, up_low, preferred_element_type=jnp.float32) + up_add
    error_part = 1.0 + jax.scipy.special.erf(preacts * ROOT_HALF)
    activated = (0.5 * preacts * error_part).astype(jnp.bfloat16)
    mixed_out = (
        middle + (jnp.dot(activated, down_low, preferred_element_type=jnp.float32) + down_add)
    ).astype(jnp.bfloat16)
    upstream = cotangent.astype(jnp.float32) * loss_share
    upstream_low = upstream.astype(jnp.bfloat16)
    grad_down_weight = jnp.dot(activated.T, upstream_low, preferred_element_type=jnp.float32)
    grad_down_bias = column_sums(upstream_low)
    grad_activated = jnp.dot(upstream_low, down_low.T, preferred_element_type=jnp.float32)
    slope = 0.5 * error_part + preacts * jnp.exp(-0.5 * preacts * preacts) * INV_ROOT_TAU
    grad_preacts = (grad_activated * slope).astype(jnp.bfloat16)
    grad_up_weight = jnp.dot(normed_two.T, grad_preacts, preferred_element_type=jnp.float32)
    grad_up_bias = column_sums(grad_preacts)
    grad_normed_two = jnp.dot(grad_preacts, up_low.T, preferred_element_type=jnp.float32)
    grad_mlp_gain = jnp.sum(grad_normed_two * scaled_two, axis=0)
    grad_mlp_shift = jnp.sum(grad_normed_two, axis=0)
    grad_middle = upstream + norm_back(grad_normed_two, gain_two, scaled_two, inverse_two)
    grad_branch = grad_middle.astype(jnp.bfloat16)
    grad_out_weight = jnp.dot(context_low.T, grad_branch, preferred_element_type=jnp.float32)
    grad_out_bias = column_sums(grad_branch)
    grad_context = jnp.dot(grad_branch, out_low.T, preferred_element_type=jnp.float32).astype(
        jnp.bfloat16
    )
    grad_projected = attend_crops_back(queries, key_rows, value_rows, logsum, grad_context, crop)
    grad_qkv_weight = jnp.dot(normed_one.T, grad_projected, preferred_element_type=jnp.float32)
    grad_query_bias = column_sums(grad_projected[:, :D])
    grad_value_bias = column_sums(grad_projected[:, 2 * D :])
    grad_normed_one = jnp.dot(grad_projected, qkv_low.T, preferred_element_type=jnp.float32)
    grad_attn_gain = jnp.sum(grad_normed_one * scaled_one, axis=0)
    grad_attn_shift = jnp.sum(grad_normed_one, axis=0)
    grad_tokens = (
        grad_middle + norm_back(grad_normed_one, gain_one, scaled_one, inverse_one)
    ).astype(jnp.bfloat16)
    grad_vectors = (
        grad_query_bias,
        grad_value_bias,
        grad_out_bias,
        grad_attn_gain,
        grad_attn_shift,
        grad_mlp_gain,
        grad_mlp_shift,
        grad_up_bias,
        grad_down_bias,
    )
    vec_grads = jnp.concatenate(
        [g.astype(jnp.bfloat16).reshape(n_fsdp, -1) for g in grad_vectors], axis=1
    )
    if small:
        (grad_down_shard,) = reduce_chain([grad_down_weight], n_dp, n_fsdp)
        (grad_up_shard,) = reduce_chain([grad_up_weight], n_dp, n_fsdp)
        (grad_out_shard,) = reduce_chain([grad_out_weight], n_dp, n_fsdp)
        rows = grad_qkv_weight.shape[0] // (n_fsdp * 2 * n_dp)
        slot = vec_grads.shape[1] // (2 * n_dp)
        if slot % rows == 0:
            qkv_view = grad_qkv_weight.astype(jnp.bfloat16).reshape(n_fsdp, n_dp, 2, rows, -1)
            vec_view = vec_grads.reshape(n_fsdp, n_dp, 2, rows, slot // rows)
            pad = -(slot // rows) % 128
            vec_view = jnp.pad(vec_view, ((0, 0),) * 4 + ((0, pad),))
            joined = jnp.concatenate([qkv_view, vec_view], axis=-1)
            (both_shard,) = reduce_chain([joined.reshape(grad_qkv_weight.shape[0], -1)], n_dp, n_fsdp)
            cols = grad_qkv_weight.shape[1]
            grad_qkv_shard = both_shard[:, :cols]
            vec_flat = both_shard[:, cols : cols + slot // rows].reshape(-1)
        else:
            grad_qkv_shard, vec_flat = reduce_chain(
                [grad_qkv_weight, vec_grads.reshape(n_fsdp * 2 * n_dp, -1)], n_dp, n_fsdp
            )
    else:
        grad_qkv_shard, grad_out_shard, grad_up_shard, grad_down_shard = reduce_weights_native(
            [w.astype(jnp.bfloat16) for w in (grad_qkv_weight, grad_out_weight, grad_up_weight, grad_down_weight)],
        )
        (vec_flat,) = reduce_weights_native([vec_grads])
    vec_out = unpack_vectors(vec_flat.reshape(1, -1), [s // n_fsdp for s in sizes], 1)
    return (
        mixed_out,
        grad_tokens,
        grad_qkv_shard,
        vec_out[0],
        vec_out[1],
        grad_out_shard,
        vec_out[2],
        vec_out[3],
        vec_out[4],
        vec_out[5],
        vec_out[6],
        grad_up_shard,
        vec_out[7],
        grad_down_shard,
        vec_out[8],
    )


def solution(mesh):
    placed = (
        P(("dp", "fsdp"), None),
        P(("dp", "fsdp"), None),
        P("dp"),
        P(),
        P("fsdp", None),
        P("fsdp"),
        P("fsdp"),
        P("fsdp", None),
        P("fsdp"),
        P("fsdp"),
        P("fsdp"),
        P("fsdp"),
        P("fsdp"),
        P("fsdp", None),
        P("fsdp"),
        P("fsdp", None),
        P("fsdp"),
    )
    n_dp = mesh.shape["dp"]
    n_fsdp = mesh.shape["fsdp"]
    return jax.shard_map(
        functools.partial(local_body, n_dp=n_dp, n_fsdp=n_fsdp),
        mesh=mesh,
        in_specs=placed,
        out_specs=(
            P(("dp", "fsdp"), None),
            P(("dp", "fsdp"), None),
            P("fsdp", None),
            P("fsdp"),
            P("fsdp"),
            P("fsdp", None),
            P("fsdp"),
            P("fsdp"),
            P("fsdp"),
            P("fsdp"),
            P("fsdp"),
            P("fsdp", None),
            P("fsdp"),
            P("fsdp", None),
            P("fsdp"),
        ),
        check_vma=False,
    )
```

```python
import functools

import jax
import jax.numpy as jnp
from jax import lax
from jax.sharding import PartitionSpec as P


D = 1024
HEADS = 16
HEAD_DIM = 64
GLEN = 50
LLEN = 10


EPSILON = 1e-06
BIG_NEGATIVE = -1000000000.0
ROOT_HALF = 0.7071067811865476
INV_ROOT_TAU = 0.3989422804014327


def normalize(values):
    middle = jnp.mean(values, axis=-1, keepdims=True)
    centered = values - middle
    inverse = lax.rsqrt(jnp.mean(centered * centered, axis=-1, keepdims=True) + EPSILON)
    return (centered * inverse, inverse)


def norm_back(grad_out, gain, scaled, inverse):
    grad_scaled = grad_out * gain
    return inverse * (
        grad_scaled
        - jnp.mean(grad_scaled, axis=-1, keepdims=True)
        - scaled * jnp.mean(grad_scaled * scaled, axis=-1, keepdims=True)
    )


def by_crops(values, crop):
    return values.reshape(values.shape[0] // crop, crop, HEADS, HEAD_DIM)


def crop_scores(queries, key_rows):
    factor = HEAD_DIM ** (-0.5)
    return (
        jnp.einsum("cqhd,ckhd->chqk", queries, key_rows, preferred_element_type=jnp.float32)
        * factor
    )


def crop_mask(crop):
    segment = lax.iota(jnp.int32, GLEN) // crop
    return segment[:, None] == segment[None, :]


def attend_crops(queries, key_rows, value_rows, crop):
    length = queries.shape[0]
    crop_q, crop_k, crop_v = (
        by_crops(queries, GLEN),
        by_crops(key_rows, GLEN),
        by_crops(value_rows, GLEN),
    )
    scores = jnp.where(crop_mask(crop), crop_scores(crop_q, crop_k), BIG_NEGATIVE)
    highest = jnp.max(scores, axis=-1, keepdims=True)
    exponent = jnp.exp(scores - highest)
    summed = jnp.sum(exponent, axis=-1, keepdims=True)
    attention = (exponent / summed).astype(jnp.bfloat16)
    context = jnp.einsum("chqk,ckhd->cqhd", attention, crop_v, preferred_element_type=jnp.float32)
    logsum = (highest + jnp.log(summed))[..., 0]
    return (
        context.reshape(length, HEADS * HEAD_DIM),
        jnp.transpose(logsum, (0, 2, 1)).reshape(length, HEADS),
    )


def attend_crops_back(queries, key_rows, value_rows, logsum, grad_context, crop):
    length = queries.shape[0]
    factor = HEAD_DIM ** (-0.5)
    crop_q, crop_k, crop_v = (
        by_crops(queries, GLEN),
        by_crops(key_rows, GLEN),
        by_crops(value_rows, GLEN),
    )
    crop_g = by_crops(grad_context, GLEN)
    crop_l = jnp.transpose(logsum.reshape(length // GLEN, GLEN, HEADS), (0, 2, 1))
    scores = jnp.where(crop_mask(crop), crop_scores(crop_q, crop_k), BIG_NEGATIVE)
    probs = jnp.exp(scores - crop_l[..., None])
    probs_low = probs.astype(jnp.bfloat16)
    grad_values = jnp.einsum(
        "chqk,cqhd->ckhd", probs_low, crop_g, preferred_element_type=jnp.float32
    )
    grad_probs = jnp.einsum("cqhd,ckhd->chqk", crop_g, crop_v, preferred_element_type=jnp.float32)
    delta = jnp.sum(probs * grad_probs, axis=-1, keepdims=True)
    grad_scores = (probs * (grad_probs - delta)).astype(jnp.bfloat16)
    grad_queries = (
        jnp.einsum("chqk,ckhd->cqhd", grad_scores, crop_k, preferred_element_type=jnp.float32)
        * factor
    )
    grad_keys = (
        jnp.einsum("chqk,cqhd->ckhd", grad_scores, crop_q, preferred_element_type=jnp.float32)
        * factor
    )
    width = HEADS * HEAD_DIM
    return jnp.concatenate(
        [
            grad_queries.reshape(length, width),
            grad_keys.reshape(length, width),
            grad_values.reshape(length, width),
        ],
        axis=1,
    ).astype(jnp.bfloat16)


def xor_pairs(n, mask):
    return [(i, i ^ mask) for i in range(n)]


def exchange(leaves, held, bit, d, n_dp, lead=0):
    got = lax.ppermute(leaves, "dp", xor_pairs(n_dp, 1 << bit))
    pos = lead + sum(1 for b in held if b > bit)
    mine = ((d >> bit) & 1) == 0
    out = [
        jnp.where(mine, jnp.stack([a, g], axis=pos), jnp.stack([g, a], axis=pos))
        for a, g in zip(leaves, got)
    ]
    return out, sorted(held + [bit], reverse=True)


def split_bit(leaves, held, bit, d, n_dp, lead):
    axis = lead + held.index(bit)
    mine = (d >> bit) & 1
    send = [lax.dynamic_index_in_dim(a, 1 - mine, axis, keepdims=False) for a in leaves]
    keep = [lax.dynamic_index_in_dim(a, mine, axis, keepdims=False) for a in leaves]
    got = lax.ppermute([v.astype(jnp.bfloat16) for v in send], "dp", xor_pairs(n_dp, 1 << bit))
    return [k.astype(jnp.float32) + g.astype(jnp.float32) for k, g in zip(keep, got)], [b for b in held if b != bit]


def chip_bits(n_dp):
    return list(range(1, n_dp.bit_length() - 1))


def gather_chain(shard, vec, n_dp, n_fsdp):
    d = lax.axis_index("dp")
    f = lax.axis_index("fsdp")
    rows, cols = shard.shape
    pieces = shard.reshape(n_dp, 2, rows // (2 * n_dp), cols)
    own = lax.dynamic_index_in_dim(pieces, d, 0, keepdims=False)
    ring, vring = [], []
    buf = [own] + ([vec] if vec is not None else [])
    for step in range(1, n_fsdp):
        got = lax.ppermute(buf, "fsdp", [(i, (i - step) % n_fsdp) for i in range(n_fsdp)])
        ring.append(got[0])
        if vec is not None:
            vring.append(got[1])
    vecs = None
    if vec is not None:
        vecs = jnp.roll(jnp.stack([vec] + vring, axis=0), f, axis=0)
    if n_fsdp == 1:
        return shard, vecs
    zrel = jnp.stack(ring, axis=0)
    halves = []
    for h in range(2):
        order = chip_bits(n_dp)
        order = order if h == 0 else order[::-1]
        leaves, held = [zrel[:, h]], []
        for bit in order:
            leaves, held = exchange(leaves, held, bit, d, n_dp, 1)
        halves.append(leaves[0])
    both = jnp.stack(halves, axis=-3)
    held = chip_bits(n_dp)[::-1]
    if n_dp > 1:
        (both,), held = exchange([both], held, 0, d, n_dp, 1)
    plane = both.reshape((n_fsdp - 1, n_dp) + both.shape[-3:])
    rel = jnp.concatenate([pieces[None], plane], axis=0)
    return jnp.roll(rel, f, axis=0).reshape(n_fsdp * rows, cols), vecs


def reduce_chain(grads, n_dp, n_fsdp):
    d = lax.axis_index("dp")
    f = lax.axis_index("fsdp")
    bits = n_dp.bit_length() - 1
    leaves = [
        g.astype(jnp.bfloat16).reshape((n_fsdp,) + (2,) * bits + (2, g.shape[0] // (n_fsdp * 2 * n_dp), g.shape[1]))
        for g in grads
    ]
    held = list(range(bits - 1, -1, -1))
    if bits > 0:
        leaves, held = split_bit(leaves, held, 0, d, n_dp, 1)
    finals = []
    for h in range(2):
        order = chip_bits(n_dp)
        order = order[::-1] if h == 0 else order
        part = [lax.index_in_dim(a, h, 1 + len(held), keepdims=False) for a in leaves]
        hb = list(held)
        for bit in order:
            part, hb = split_bit(part, hb, bit, d, n_dp, 1)
        finals.append(part)
    acc = [jnp.stack([finals[0][i], finals[1][i]], axis=1) for i in range(len(grads))]
    total = [lax.dynamic_index_in_dim(a, f, 0, keepdims=False) for a in acc]
    for step in range(1, n_fsdp):
        out = [lax.dynamic_index_in_dim(a, (f + step) % n_fsdp, 0, keepdims=False).astype(jnp.bfloat16) for a in acc]
        got = lax.ppermute(out, "fsdp", [(i, (i + step) % n_fsdp) for i in range(n_fsdp)])
        total = [t + g.astype(jnp.float32) for t, g in zip(total, got)]
    send = [t.astype(jnp.bfloat16) for t in total]
    part, hb = send, []
    for bit in chip_bits(n_dp):
        part, hb = exchange(part, hb, bit, d, n_dp)
    both = part
    if n_dp > 1:
        both, hb = exchange(both, hb, 0, d, n_dp)
    return [b.reshape(g.shape[0] // n_fsdp, g.shape[1]).astype(jnp.float32) for b, g in zip(both, grads)]


def gather_weights_native(shards):
    return [lax.all_gather(s, "fsdp", axis=0, tiled=True) for s in shards]


def reduce_weights_native(grads):
    return [
        lax.psum(lax.psum_scatter(g, "fsdp", scatter_dimension=0, tiled=True), "dp").astype(jnp.float32)
        for g in grads
    ]


def unpack_vectors(packed, sizes, n_fsdp):
    rows = packed.reshape(n_fsdp, -1)
    out = []
    offset = 0
    for size in sizes:
        width = size // n_fsdp
        out.append(rows[:, offset : offset + width].reshape(size))
        offset += width
    return out


def column_sums(values):
    return jnp.sum(values.astype(jnp.float32), axis=0)


def local_body(
    tokens,
    cotangent,
    crop_group,
    group_tokens,
    qkv_weight,
    query_bias,
    value_bias,
    out_weight,
    out_bias,
    attn_gain,
    attn_shift,
    mlp_gain,
    mlp_shift,
    up_weight,
    up_bias,
    down_weight,
    down_bias,
    n_dp,
    n_fsdp,
):
    small = n_dp * n_fsdp <= 64
    vectors = (query_bias, value_bias, out_bias, attn_gain, attn_shift, mlp_gain, mlp_shift, up_bias, down_bias)
    sizes = [v.shape[0] * n_fsdp for v in vectors]
    vec_local = jnp.concatenate([v.astype(jnp.bfloat16) for v in vectors])
    low = [w.astype(jnp.bfloat16) for w in (qkv_weight, out_weight, up_weight, down_weight)]
    if small:
        qkv_low, vec_rows = gather_chain(low[0], vec_local, n_dp, n_fsdp)
        out_low, _ = gather_chain(low[1], None, n_dp, n_fsdp)
        up_low, _ = gather_chain(low[2], None, n_dp, n_fsdp)
        down_low, _ = gather_chain(low[3], None, n_dp, n_fsdp)
    else:
        qkv_low, out_low, up_low, down_low = gather_weights_native(low)
        vec_rows = lax.all_gather(vec_local, "fsdp", axis=0, tiled=False)
    (
        query_add,
        value_add,
        out_add,
        gain_one,
        shift_one,
        gain_two,
        shift_two,
        up_add,
        down_add,
    ) = [v.astype(jnp.float32) for v in unpack_vectors(vec_rows, sizes, n_fsdp)]
    is_global = crop_group[0] == 1
    totals = (group_tokens[0] + group_tokens[1]).astype(jnp.float32)
    loss_share = jnp.where(is_global, group_tokens[1], group_tokens[0]).astype(jnp.float32) / totals
    inputs = tokens.astype(jnp.float32)
    scaled_one, inverse_one = normalize(inputs)
    normed_one = (scaled_one * gain_one + shift_one).astype(jnp.bfloat16)
    projected = jnp.dot(normed_one, qkv_low, preferred_element_type=jnp.float32)
    projected = projected + jnp.concatenate([query_add, jnp.zeros_like(query_add), value_add])
    projected_low = projected.astype(jnp.bfloat16)
    queries = projected_low[:, :D]
    key_rows = projected_low[:, D : 2 * D]
    value_rows = projected_low[:, 2 * D :]
    crop = jnp.where(is_global, GLEN, LLEN)
    context, logsum = attend_crops(queries, key_rows, value_rows, crop)
    context_low = context.astype(jnp.bfloat16)
    middle = inputs + (jnp.dot(context_low, out_low, preferred_element_type=jnp.float32) + out_add)
    scaled_two, inverse_two = normalize(middle)
    normed_two = (scaled_two * gain_two + shift_two).astype(jnp.bfloat16)
    preacts = jnp.dot(normed_two, up_low, preferred_element_type=jnp.float32) + up_add
    error_part = 1.0 + jax.scipy.special.erf(preacts * ROOT_HALF)
    activated = (0.5 * preacts * error_part).astype(jnp.bfloat16)
    mixed_out = (
        middle + (jnp.dot(activated, down_low, preferred_element_type=jnp.float32) + down_add)
    ).astype(jnp.bfloat16)
    upstream = cotangent.astype(jnp.float32) * loss_share
    upstream_low = upstream.astype(jnp.bfloat16)
    grad_down_weight = jnp.dot(activated.T, upstream_low, preferred_element_type=jnp.float32)
    grad_down_bias = column_sums(upstream_low)
    grad_activated = jnp.dot(upstream_low, down_low.T, preferred_element_type=jnp.float32)
    slope = 0.5 * error_part + preacts * jnp.exp(-0.5 * preacts * preacts) * INV_ROOT_TAU
    grad_preacts = (grad_activated * slope).astype(jnp.bfloat16)
    grad_up_weight = jnp.dot(normed_two.T, grad_preacts, preferred_element_type=jnp.float32)
    grad_up_bias = column_sums(grad_preacts)
    grad_normed_two = jnp.dot(grad_preacts, up_low.T, preferred_element_type=jnp.float32)
    grad_mlp_gain = jnp.sum(grad_normed_two * scaled_two, axis=0)
    grad_mlp_shift = jnp.sum(grad_normed_two, axis=0)
    grad_middle = upstream + norm_back(grad_normed_two, gain_two, scaled_two, inverse_two)
    grad_branch = grad_middle.astype(jnp.bfloat16)
    grad_out_weight = jnp.dot(context_low.T, grad_branch, preferred_element_type=jnp.float32)
    grad_out_bias = column_sums(grad_branch)
    grad_context = jnp.dot(grad_branch, out_low.T, preferred_element_type=jnp.float32).astype(
        jnp.bfloat16
    )
    grad_projected = attend_crops_back(queries, key_rows, value_rows, logsum, grad_context, crop)
    grad_qkv_weight = jnp.dot(normed_one.T, grad_projected, preferred_element_type=jnp.float32)
    grad_query_bias = column_sums(grad_projected[:, :D])
    grad_value_bias = column_sums(grad_projected[:, 2 * D :])
    grad_normed_one = jnp.dot(grad_projected, qkv_low.T, preferred_element_type=jnp.float32)
    grad_attn_gain = jnp.sum(grad_normed_one * scaled_one, axis=0)
    grad_attn_shift = jnp.sum(grad_normed_one, axis=0)
    grad_tokens = (
        grad_middle + norm_back(grad_normed_one, gain_one, scaled_one, inverse_one)
    ).astype(jnp.bfloat16)
    grad_vectors = (
        grad_query_bias,
        grad_value_bias,
        grad_out_bias,
        grad_attn_gain,
        grad_attn_shift,
        grad_mlp_gain,
        grad_mlp_shift,
        grad_up_bias,
        grad_down_bias,
    )
    vec_grads = jnp.concatenate(
        [g.astype(jnp.bfloat16).reshape(n_fsdp, -1) for g in grad_vectors], axis=1
    )
    if small:
        (grad_down_shard,) = reduce_chain([grad_down_weight], n_dp, n_fsdp)
        (grad_up_shard,) = reduce_chain([grad_up_weight], n_dp, n_fsdp)
        (grad_out_shard,) = reduce_chain([grad_out_weight], n_dp, n_fsdp)
        rows = grad_qkv_weight.shape[0] // (n_fsdp * 2 * n_dp)
        slot = vec_grads.shape[1] // (2 * n_dp)
        if slot % rows == 0:
            qkv_view = grad_qkv_weight.astype(jnp.bfloat16).reshape(n_fsdp, n_dp, 2, rows, -1)
            vec_view = vec_grads.reshape(n_fsdp, n_dp, 2, rows, slot // rows)
            pad = -(slot // rows) % 128
            vec_view = jnp.pad(vec_view, ((0, 0),) * 4 + ((0, pad),))
            joined = jnp.concatenate([qkv_view, vec_view], axis=-1)
            (both_shard,) = reduce_chain([joined.reshape(grad_qkv_weight.shape[0], -1)], n_dp, n_fsdp)
            cols = grad_qkv_weight.shape[1]
            grad_qkv_shard = both_shard[:, :cols]
            vec_flat = both_shard[:, cols : cols + slot // rows].reshape(-1)
        else:
            grad_qkv_shard, vec_flat = reduce_chain(
                [grad_qkv_weight, vec_grads.reshape(n_fsdp * 2 * n_dp, -1)], n_dp, n_fsdp
            )
    else:
        grad_qkv_shard, grad_out_shard, grad_up_shard, grad_down_shard = reduce_weights_native(
            [w.astype(jnp.bfloat16) for w in (grad_qkv_weight, grad_out_weight, grad_up_weight, grad_down_weight)],
        )
        (vec_flat,) = reduce_weights_native([vec_grads])
    vec_out = unpack_vectors(vec_flat.reshape(1, -1), [s // n_fsdp for s in sizes], 1)
    return (
        mixed_out,
        grad_tokens,
        grad_qkv_shard,
        vec_out[0],
        vec_out[1],
        grad_out_shard,
        vec_out[2],
        vec_out[3],
        vec_out[4],
        vec_out[5],
        vec_out[6],
        grad_up_shard,
        vec_out[7],
        grad_down_shard,
        vec_out[8],
    )


def solution(mesh):
    placed = (
        P(("dp", "fsdp"), None),
        P(("dp", "fsdp"), None),
        P("dp"),
        P(),
        P("fsdp", None),
        P("fsdp"),
        P("fsdp"),
        P("fsdp", None),
        P("fsdp"),
        P("fsdp"),
        P("fsdp"),
        P("fsdp"),
        P("fsdp"),
        P("fsdp", None),
        P("fsdp"),
        P("fsdp", None),
        P("fsdp"),
    )
    n_dp = mesh.shape["dp"]
    n_fsdp = mesh.shape["fsdp"]
    return jax.shard_map(
        functools.partial(local_body, n_dp=n_dp, n_fsdp=n_fsdp),
        mesh=mesh,
        in_specs=placed,
        out_specs=(
            P(("dp", "fsdp"), None),
            P(("dp", "fsdp"), None),
            P("fsdp", None),
            P("fsdp"),
            P("fsdp"),
            P("fsdp", None),
            P("fsdp"),
            P("fsdp"),
            P("fsdp"),
            P("fsdp"),
            P("fsdp"),
            P("fsdp", None),
            P("fsdp"),
            P("fsdp", None),
            P("fsdp"),
        ),
        check_vma=False,
    )
```

```python
import functools

import jax
import jax.numpy as jnp
from jax import lax
from jax.sharding import PartitionSpec as P


D = 1024
HEADS = 16
HEAD_DIM = 64
GLEN = 50
LLEN = 10


EPSILON = 1e-06
BIG_NEGATIVE = -1000000000.0
ROOT_HALF = 0.7071067811865476
INV_ROOT_TAU = 0.3989422804014327


def normalize(values):
    middle = jnp.mean(values, axis=-1, keepdims=True)
    centered = values - middle
    inverse = lax.rsqrt(jnp.mean(centered * centered, axis=-1, keepdims=True) + EPSILON)
    return (centered * inverse, inverse)


def norm_back(grad_out, gain, scaled, inverse):
    grad_scaled = grad_out * gain
    return inverse * (
        grad_scaled
        - jnp.mean(grad_scaled, axis=-1, keepdims=True)
        - scaled * jnp.mean(grad_scaled * scaled, axis=-1, keepdims=True)
    )


def by_crops(values, crop):
    return values.reshape(values.shape[0] // crop, crop, HEADS, HEAD_DIM)


def crop_scores(queries, key_rows):
    factor = HEAD_DIM ** (-0.5)
    return (
        jnp.einsum("cqhd,ckhd->chqk", queries, key_rows, preferred_element_type=jnp.float32)
        * factor
    )


def crop_mask(crop):
    segment = lax.iota(jnp.int32, GLEN) // crop
    return segment[:, None] == segment[None, :]


def attend_crops(queries, key_rows, value_rows, crop):
    length = queries.shape[0]
    crop_q, crop_k, crop_v = (
        by_crops(queries, GLEN),
        by_crops(key_rows, GLEN),
        by_crops(value_rows, GLEN),
    )
    scores = jnp.where(crop_mask(crop), crop_scores(crop_q, crop_k), BIG_NEGATIVE)
    highest = jnp.max(scores, axis=-1, keepdims=True)
    exponent = jnp.exp(scores - highest)
    summed = jnp.sum(exponent, axis=-1, keepdims=True)
    attention = (exponent / summed).astype(jnp.bfloat16)
    context = jnp.einsum("chqk,ckhd->cqhd", attention, crop_v, preferred_element_type=jnp.float32)
    logsum = (highest + jnp.log(summed))[..., 0]
    return (
        context.reshape(length, HEADS * HEAD_DIM),
        jnp.transpose(logsum, (0, 2, 1)).reshape(length, HEADS),
    )


def attend_crops_back(queries, key_rows, value_rows, logsum, grad_context, crop):
    length = queries.shape[0]
    factor = HEAD_DIM ** (-0.5)
    crop_q, crop_k, crop_v = (
        by_crops(queries, GLEN),
        by_crops(key_rows, GLEN),
        by_crops(value_rows, GLEN),
    )
    crop_g = by_crops(grad_context, GLEN)
    crop_l = jnp.transpose(logsum.reshape(length // GLEN, GLEN, HEADS), (0, 2, 1))
    scores = jnp.where(crop_mask(crop), crop_scores(crop_q, crop_k), BIG_NEGATIVE)
    probs = jnp.exp(scores - crop_l[..., None])
    probs_low = probs.astype(jnp.bfloat16)
    grad_values = jnp.einsum(
        "chqk,cqhd->ckhd", probs_low, crop_g, preferred_element_type=jnp.float32
    )
    grad_probs = jnp.einsum("cqhd,ckhd->chqk", crop_g, crop_v, preferred_element_type=jnp.float32)
    delta = jnp.sum(probs * grad_probs, axis=-1, keepdims=True)
    grad_scores = (probs * (grad_probs - delta)).astype(jnp.bfloat16)
    grad_queries = (
        jnp.einsum("chqk,ckhd->cqhd", grad_scores, crop_k, preferred_element_type=jnp.float32)
        * factor
    )
    grad_keys = (
        jnp.einsum("chqk,cqhd->ckhd", grad_scores, crop_q, preferred_element_type=jnp.float32)
        * factor
    )
    width = HEADS * HEAD_DIM
    return jnp.concatenate(
        [
            grad_queries.reshape(length, width),
            grad_keys.reshape(length, width),
            grad_values.reshape(length, width),
        ],
        axis=1,
    ).astype(jnp.bfloat16)


def xor_pairs(n, mask):
    return [(i, i ^ mask) for i in range(n)]


def exchange(leaves, held, bit, d, n_dp, lead=0):
    got = lax.ppermute(leaves, "dp", xor_pairs(n_dp, 1 << bit))
    pos = lead + sum(1 for b in held if b > bit)
    mine = ((d >> bit) & 1) == 0
    out = [
        jnp.where(mine, jnp.stack([a, g], axis=pos), jnp.stack([g, a], axis=pos))
        for a, g in zip(leaves, got)
    ]
    return out, sorted(held + [bit], reverse=True)


def split_bit(leaves, held, bit, d, n_dp, lead):
    axis = lead + held.index(bit)
    mine = (d >> bit) & 1
    send = [lax.dynamic_index_in_dim(a, 1 - mine, axis, keepdims=False) for a in leaves]
    keep = [lax.dynamic_index_in_dim(a, mine, axis, keepdims=False) for a in leaves]
    got = lax.ppermute([v.astype(jnp.bfloat16) for v in send], "dp", xor_pairs(n_dp, 1 << bit))
    return [k.astype(jnp.float32) + g.astype(jnp.float32) for k, g in zip(keep, got)], [b for b in held if b != bit]


def chip_bits(n_dp):
    return list(range(1, n_dp.bit_length() - 1))


def gather_chain(shard, vec, n_dp, n_fsdp, direct=False):
    d = lax.axis_index("dp")
    f = lax.axis_index("fsdp")
    rows, cols = shard.shape
    pieces = shard.reshape(n_dp, 2, rows // (2 * n_dp), cols)
    own = lax.dynamic_index_in_dim(pieces, d, 0, keepdims=False)
    down = [(i, (i - 1) % n_fsdp) for i in range(n_fsdp)]
    ring, vring = [], []
    buf = [own] + ([vec] if vec is not None else [])
    for step in range(1, n_fsdp):
        if direct:
            got = lax.ppermute(buf, "fsdp", [(i, (i - step) % n_fsdp) for i in range(n_fsdp)])
        else:
            got = buf = lax.ppermute(buf, "fsdp", down)
        ring.append(got[0])
        if vec is not None:
            vring.append(got[1])
    vecs = None
    if vec is not None:
        vecs = jnp.roll(jnp.stack([vec] + vring, axis=0), f, axis=0)
    if n_fsdp == 1:
        return shard, vecs
    zrel = jnp.stack(ring, axis=0)
    halves = []
    for h in range(2):
        order = chip_bits(n_dp)
        order = order if h == 0 else order[::-1]
        leaves, held = [zrel[:, h]], []
        for bit in order:
            leaves, held = exchange(leaves, held, bit, d, n_dp, 1)
        halves.append(leaves[0])
    both = jnp.stack(halves, axis=-3)
    held = chip_bits(n_dp)[::-1]
    if n_dp > 1:
        (both,), held = exchange([both], held, 0, d, n_dp, 1)
    plane = both.reshape((n_fsdp - 1, n_dp) + both.shape[-3:])
    rel = jnp.concatenate([pieces[None], plane], axis=0)
    return jnp.roll(rel, f, axis=0).reshape(n_fsdp * rows, cols), vecs


def reduce_chain(grads, n_dp, n_fsdp, direct=False):
    d = lax.axis_index("dp")
    f = lax.axis_index("fsdp")
    bits = n_dp.bit_length() - 1
    leaves = [
        g.astype(jnp.bfloat16).reshape((n_fsdp,) + (2,) * bits + (2, g.shape[0] // (n_fsdp * 2 * n_dp), g.shape[1]))
        for g in grads
    ]
    held = list(range(bits - 1, -1, -1))
    if bits > 0:
        leaves, held = split_bit(leaves, held, 0, d, n_dp, 1)
    finals = []
    for h in range(2):
        order = chip_bits(n_dp)
        order = order[::-1] if h == 0 else order
        part = [lax.index_in_dim(a, h, 1 + len(held), keepdims=False) for a in leaves]
        hb = list(held)
        for bit in order:
            part, hb = split_bit(part, hb, bit, d, n_dp, 1)
        finals.append(part)
    acc = [jnp.stack([finals[0][i], finals[1][i]], axis=1) for i in range(len(grads))]
    if direct:
        total = [lax.dynamic_index_in_dim(a, f, 0, keepdims=False) for a in acc]
        for step in range(1, n_fsdp):
            out = [lax.dynamic_index_in_dim(a, (f + step) % n_fsdp, 0, keepdims=False).astype(jnp.bfloat16) for a in acc]
            got = lax.ppermute(out, "fsdp", [(i, (i + step) % n_fsdp) for i in range(n_fsdp)])
            total = [t + g.astype(jnp.float32) for t, g in zip(total, got)]
        send = [t.astype(jnp.bfloat16) for t in total]
    else:
        down = [(i, (i - 1) % n_fsdp) for i in range(n_fsdp)]
        if n_fsdp == 1:
            send = [a[0].astype(jnp.bfloat16) for a in acc]
        else:
            send = [lax.dynamic_index_in_dim(a, (f + 1) % n_fsdp, 0, keepdims=False).astype(jnp.bfloat16) for a in acc]
        for step in range(1, n_fsdp):
            got = lax.ppermute(send, "fsdp", down)
            chunk = (f + 1 + step) % n_fsdp
            send = [
                (g.astype(jnp.float32) + lax.dynamic_index_in_dim(a, chunk, 0, keepdims=False)).astype(jnp.bfloat16)
                for g, a in zip(got, acc)
            ]
    part, hb = send, []
    for bit in chip_bits(n_dp):
        part, hb = exchange(part, hb, bit, d, n_dp)
    both = part
    if n_dp > 1:
        both, hb = exchange(both, hb, 0, d, n_dp)
    return [b.reshape(g.shape[0] // n_fsdp, g.shape[1]).astype(jnp.float32) for b, g in zip(both, grads)]


def gather_weights_native(shards):
    return [lax.all_gather(s, "fsdp", axis=0, tiled=True) for s in shards]


def reduce_weights_native(grads):
    return [
        lax.psum(lax.psum_scatter(g, "fsdp", scatter_dimension=0, tiled=True), "dp").astype(jnp.float32)
        for g in grads
    ]


def unpack_vectors(packed, sizes, n_fsdp):
    rows = packed.reshape(n_fsdp, -1)
    out = []
    offset = 0
    for size in sizes:
        width = size // n_fsdp
        out.append(rows[:, offset : offset + width].reshape(size))
        offset += width
    return out


def column_sums(values):
    return jnp.sum(values.astype(jnp.float32), axis=0)


def local_body(
    tokens,
    cotangent,
    crop_group,
    group_tokens,
    qkv_weight,
    query_bias,
    value_bias,
    out_weight,
    out_bias,
    attn_gain,
    attn_shift,
    mlp_gain,
    mlp_shift,
    up_weight,
    up_bias,
    down_weight,
    down_bias,
    n_dp,
    n_fsdp,
):
    small = n_dp * n_fsdp <= 64
    vectors = (query_bias, value_bias, out_bias, attn_gain, attn_shift, mlp_gain, mlp_shift, up_bias, down_bias)
    sizes = [v.shape[0] * n_fsdp for v in vectors]
    vec_local = jnp.concatenate([v.astype(jnp.bfloat16) for v in vectors])
    low = [w.astype(jnp.bfloat16) for w in (qkv_weight, out_weight, up_weight, down_weight)]
    if small:
        qkv_low, vec_rows = gather_chain(low[0], vec_local, n_dp, n_fsdp, True)
        out_low, _ = gather_chain(low[1], None, n_dp, n_fsdp)
        up_low, _ = gather_chain(low[2], None, n_dp, n_fsdp)
        down_low, _ = gather_chain(low[3], None, n_dp, n_fsdp)
    else:
        qkv_low, out_low, up_low, down_low = gather_weights_native(low)
        vec_rows = lax.all_gather(vec_local, "fsdp", axis=0, tiled=False)
    (
        query_add,
        value_add,
        out_add,
        gain_one,
        shift_one,
        gain_two,
        shift_two,
        up_add,
        down_add,
    ) = [v.astype(jnp.float32) for v in unpack_vectors(vec_rows, sizes, n_fsdp)]
    is_global = crop_group[0] == 1
    totals = (group_tokens[0] + group_tokens[1]).astype(jnp.float32)
    loss_share = jnp.where(is_global, group_tokens[1], group_tokens[0]).astype(jnp.float32) / totals
    inputs = tokens.astype(jnp.float32)
    scaled_one, inverse_one = normalize(inputs)
    normed_one = (scaled_one * gain_one + shift_one).astype(jnp.bfloat16)
    projected = jnp.dot(normed_one, qkv_low, preferred_element_type=jnp.float32)
    projected = projected + jnp.concatenate([query_add, jnp.zeros_like(query_add), value_add])
    projected_low = projected.astype(jnp.bfloat16)
    queries = projected_low[:, :D]
    key_rows = projected_low[:, D : 2 * D]
    value_rows = projected_low[:, 2 * D :]
    crop = jnp.where(is_global, GLEN, LLEN)
    context, logsum = attend_crops(queries, key_rows, value_rows, crop)
    context_low = context.astype(jnp.bfloat16)
    middle = inputs + (jnp.dot(context_low, out_low, preferred_element_type=jnp.float32) + out_add)
    scaled_two, inverse_two = normalize(middle)
    normed_two = (scaled_two * gain_two + shift_two).astype(jnp.bfloat16)
    preacts = jnp.dot(normed_two, up_low, preferred_element_type=jnp.float32) + up_add
    error_part = 1.0 + jax.scipy.special.erf(preacts * ROOT_HALF)
    activated = (0.5 * preacts * error_part).astype(jnp.bfloat16)
    mixed_out = (
        middle + (jnp.dot(activated, down_low, preferred_element_type=jnp.float32) + down_add)
    ).astype(jnp.bfloat16)
    upstream = cotangent.astype(jnp.float32) * loss_share
    upstream_low = upstream.astype(jnp.bfloat16)
    grad_down_weight = jnp.dot(activated.T, upstream_low, preferred_element_type=jnp.float32)
    grad_down_bias = column_sums(upstream_low)
    grad_activated = jnp.dot(upstream_low, down_low.T, preferred_element_type=jnp.float32)
    slope = 0.5 * error_part + preacts * jnp.exp(-0.5 * preacts * preacts) * INV_ROOT_TAU
    grad_preacts = (grad_activated * slope).astype(jnp.bfloat16)
    grad_up_weight = jnp.dot(normed_two.T, grad_preacts, preferred_element_type=jnp.float32)
    grad_up_bias = column_sums(grad_preacts)
    grad_normed_two = jnp.dot(grad_preacts, up_low.T, preferred_element_type=jnp.float32)
    grad_mlp_gain = jnp.sum(grad_normed_two * scaled_two, axis=0)
    grad_mlp_shift = jnp.sum(grad_normed_two, axis=0)
    grad_middle = upstream + norm_back(grad_normed_two, gain_two, scaled_two, inverse_two)
    grad_branch = grad_middle.astype(jnp.bfloat16)
    grad_out_weight = jnp.dot(context_low.T, grad_branch, preferred_element_type=jnp.float32)
    grad_out_bias = column_sums(grad_branch)
    grad_context = jnp.dot(grad_branch, out_low.T, preferred_element_type=jnp.float32).astype(
        jnp.bfloat16
    )
    grad_projected = attend_crops_back(queries, key_rows, value_rows, logsum, grad_context, crop)
    grad_qkv_weight = jnp.dot(normed_one.T, grad_projected, preferred_element_type=jnp.float32)
    grad_query_bias = column_sums(grad_projected[:, :D])
    grad_value_bias = column_sums(grad_projected[:, 2 * D :])
    grad_normed_one = jnp.dot(grad_projected, qkv_low.T, preferred_element_type=jnp.float32)
    grad_attn_gain = jnp.sum(grad_normed_one * scaled_one, axis=0)
    grad_attn_shift = jnp.sum(grad_normed_one, axis=0)
    grad_tokens = (
        grad_middle + norm_back(grad_normed_one, gain_one, scaled_one, inverse_one)
    ).astype(jnp.bfloat16)
    grad_vectors = (
        grad_query_bias,
        grad_value_bias,
        grad_out_bias,
        grad_attn_gain,
        grad_attn_shift,
        grad_mlp_gain,
        grad_mlp_shift,
        grad_up_bias,
        grad_down_bias,
    )
    vec_grads = jnp.concatenate(
        [g.astype(jnp.bfloat16).reshape(n_fsdp, -1) for g in grad_vectors], axis=1
    )
    if small:
        (grad_down_shard,) = reduce_chain([grad_down_weight], n_dp, n_fsdp)
        (grad_up_shard,) = reduce_chain([grad_up_weight], n_dp, n_fsdp)
        (grad_out_shard,) = reduce_chain([grad_out_weight], n_dp, n_fsdp)
        rows = grad_qkv_weight.shape[0] // (n_fsdp * 2 * n_dp)
        slot = vec_grads.shape[1] // (2 * n_dp)
        if slot % rows == 0:
            qkv_view = grad_qkv_weight.astype(jnp.bfloat16).reshape(n_fsdp, n_dp, 2, rows, -1)
            vec_view = vec_grads.reshape(n_fsdp, n_dp, 2, rows, slot // rows)
            pad = -(slot // rows) % 128
            vec_view = jnp.pad(vec_view, ((0, 0),) * 4 + ((0, pad),))
            joined = jnp.concatenate([qkv_view, vec_view], axis=-1)
            (both_shard,) = reduce_chain([joined.reshape(grad_qkv_weight.shape[0], -1)], n_dp, n_fsdp, True)
            cols = grad_qkv_weight.shape[1]
            grad_qkv_shard = both_shard[:, :cols]
            vec_flat = both_shard[:, cols : cols + slot // rows].reshape(-1)
        else:
            grad_qkv_shard, vec_flat = reduce_chain(
                [grad_qkv_weight, vec_grads.reshape(n_fsdp * 2 * n_dp, -1)], n_dp, n_fsdp
            )
    else:
        grad_qkv_shard, grad_out_shard, grad_up_shard, grad_down_shard = reduce_weights_native(
            [w.astype(jnp.bfloat16) for w in (grad_qkv_weight, grad_out_weight, grad_up_weight, grad_down_weight)],
        )
        (vec_flat,) = reduce_weights_native([vec_grads])
    vec_out = unpack_vectors(vec_flat.reshape(1, -1), [s // n_fsdp for s in sizes], 1)
    return (
        mixed_out,
        grad_tokens,
        grad_qkv_shard,
        vec_out[0],
        vec_out[1],
        grad_out_shard,
        vec_out[2],
        vec_out[3],
        vec_out[4],
        vec_out[5],
        vec_out[6],
        grad_up_shard,
        vec_out[7],
        grad_down_shard,
        vec_out[8],
    )


def solution(mesh):
    placed = (
        P(("dp", "fsdp"), None),
        P(("dp", "fsdp"), None),
        P("dp"),
        P(),
        P("fsdp", None),
        P("fsdp"),
        P("fsdp"),
        P("fsdp", None),
        P("fsdp"),
        P("fsdp"),
        P("fsdp"),
        P("fsdp"),
        P("fsdp"),
        P("fsdp", None),
        P("fsdp"),
        P("fsdp", None),
        P("fsdp"),
    )
    n_dp = mesh.shape["dp"]
    n_fsdp = mesh.shape["fsdp"]
    return jax.shard_map(
        functools.partial(local_body, n_dp=n_dp, n_fsdp=n_fsdp),
        mesh=mesh,
        in_specs=placed,
        out_specs=(
            P(("dp", "fsdp"), None),
            P(("dp", "fsdp"), None),
            P("fsdp", None),
            P("fsdp"),
            P("fsdp"),
            P("fsdp", None),
            P("fsdp"),
            P("fsdp"),
            P("fsdp"),
            P("fsdp"),
            P("fsdp"),
            P("fsdp", None),
            P("fsdp"),
            P("fsdp", None),
            P("fsdp"),
        ),
        check_vma=False,
    )
```

```python
import functools

import jax
import jax.numpy as jnp
from jax import lax
from jax.sharding import PartitionSpec as P


D = 1024
HEADS = 16
HEAD_DIM = 64
GLEN = 50
LLEN = 10


EPSILON = 1e-06
BIG_NEGATIVE = -1000000000.0
ROOT_HALF = 0.7071067811865476
INV_ROOT_TAU = 0.3989422804014327


def normalize(values):
    middle = jnp.mean(values, axis=-1, keepdims=True)
    centered = values - middle
    inverse = lax.rsqrt(jnp.mean(centered * centered, axis=-1, keepdims=True) + EPSILON)
    return (centered * inverse, inverse)


def norm_back(grad_out, gain, scaled, inverse):
    grad_scaled = grad_out * gain
    return inverse * (
        grad_scaled
        - jnp.mean(grad_scaled, axis=-1, keepdims=True)
        - scaled * jnp.mean(grad_scaled * scaled, axis=-1, keepdims=True)
    )


def by_crops(values, crop):
    return values.reshape(values.shape[0] // crop, crop, HEADS, HEAD_DIM)


def crop_scores(queries, key_rows):
    factor = HEAD_DIM ** (-0.5)
    return (
        jnp.einsum("cqhd,ckhd->chqk", queries, key_rows, preferred_element_type=jnp.float32)
        * factor
    )


def crop_mask(crop):
    segment = lax.iota(jnp.int32, GLEN) // crop
    return segment[:, None] == segment[None, :]


def attend_crops(queries, key_rows, value_rows, crop):
    length = queries.shape[0]
    crop_q, crop_k, crop_v = (
        by_crops(queries, GLEN),
        by_crops(key_rows, GLEN),
        by_crops(value_rows, GLEN),
    )
    scores = jnp.where(crop_mask(crop), crop_scores(crop_q, crop_k), BIG_NEGATIVE)
    highest = jnp.max(scores, axis=-1, keepdims=True)
    exponent = jnp.exp(scores - highest)
    summed = jnp.sum(exponent, axis=-1, keepdims=True)
    attention = (exponent / summed).astype(jnp.bfloat16)
    context = jnp.einsum("chqk,ckhd->cqhd", attention, crop_v, preferred_element_type=jnp.float32)
    logsum = (highest + jnp.log(summed))[..., 0]
    return (
        context.reshape(length, HEADS * HEAD_DIM),
        jnp.transpose(logsum, (0, 2, 1)).reshape(length, HEADS),
    )


def attend_crops_back(queries, key_rows, value_rows, logsum, grad_context, crop):
    length = queries.shape[0]
    factor = HEAD_DIM ** (-0.5)
    crop_q, crop_k, crop_v = (
        by_crops(queries, GLEN),
        by_crops(key_rows, GLEN),
        by_crops(value_rows, GLEN),
    )
    crop_g = by_crops(grad_context, GLEN)
    crop_l = jnp.transpose(logsum.reshape(length // GLEN, GLEN, HEADS), (0, 2, 1))
    scores = jnp.where(crop_mask(crop), crop_scores(crop_q, crop_k), BIG_NEGATIVE)
    probs = jnp.exp(scores - crop_l[..., None])
    probs_low = probs.astype(jnp.bfloat16)
    grad_values = jnp.einsum(
        "chqk,cqhd->ckhd", probs_low, crop_g, preferred_element_type=jnp.float32
    )
    grad_probs = jnp.einsum("cqhd,ckhd->chqk", crop_g, crop_v, preferred_element_type=jnp.float32)
    delta = jnp.sum(probs * grad_probs, axis=-1, keepdims=True)
    grad_scores = (probs * (grad_probs - delta)).astype(jnp.bfloat16)
    grad_queries = (
        jnp.einsum("chqk,ckhd->cqhd", grad_scores, crop_k, preferred_element_type=jnp.float32)
        * factor
    )
    grad_keys = (
        jnp.einsum("chqk,cqhd->ckhd", grad_scores, crop_q, preferred_element_type=jnp.float32)
        * factor
    )
    width = HEADS * HEAD_DIM
    return jnp.concatenate(
        [
            grad_queries.reshape(length, width),
            grad_keys.reshape(length, width),
            grad_values.reshape(length, width),
        ],
        axis=1,
    ).astype(jnp.bfloat16)


def xor_pairs(n, mask):
    return [(i, i ^ mask) for i in range(n)]


def exchange(leaves, held, bit, d, n_dp, lead=0):
    got = lax.ppermute(leaves, "dp", xor_pairs(n_dp, 1 << bit))
    pos = lead + sum(1 for b in held if b > bit)
    mine = ((d >> bit) & 1) == 0
    out = [
        jnp.where(mine, jnp.stack([a, g], axis=pos), jnp.stack([g, a], axis=pos))
        for a, g in zip(leaves, got)
    ]
    return out, sorted(held + [bit], reverse=True)


def split_bit(leaves, held, bit, d, n_dp, lead):
    axis = lead + held.index(bit)
    mine = (d >> bit) & 1
    send = [lax.dynamic_index_in_dim(a, 1 - mine, axis, keepdims=False) for a in leaves]
    keep = [lax.dynamic_index_in_dim(a, mine, axis, keepdims=False) for a in leaves]
    got = lax.ppermute([v.astype(jnp.bfloat16) for v in send], "dp", xor_pairs(n_dp, 1 << bit))
    return [k.astype(jnp.float32) + g.astype(jnp.float32) for k, g in zip(keep, got)], [b for b in held if b != bit]


def chip_bits(n_dp):
    return list(range(1, n_dp.bit_length() - 1))


def gather_chain(shard, vec, n_dp, n_fsdp, direct=False):
    d = lax.axis_index("dp")
    f = lax.axis_index("fsdp")
    rows, cols = shard.shape
    pieces = shard.reshape(n_dp, 2, rows // (2 * n_dp), cols)
    own = lax.dynamic_index_in_dim(pieces, d, 0, keepdims=False)
    down = [(i, (i - 1) % n_fsdp) for i in range(n_fsdp)]
    ring, vring = [], []
    buf = [own] + ([vec] if vec is not None else [])
    for step in range(1, n_fsdp):
        if direct:
            got = lax.ppermute(buf, "fsdp", [(i, (i - step) % n_fsdp) for i in range(n_fsdp)])
        else:
            got = buf = lax.ppermute(buf, "fsdp", down)
        ring.append(got[0])
        if vec is not None:
            vring.append(got[1])
    vecs = None
    if vec is not None:
        vecs = jnp.roll(jnp.stack([vec] + vring, axis=0), f, axis=0)
    if n_fsdp == 1:
        return shard, vecs
    zrel = jnp.stack(ring, axis=0)
    halves = []
    for h in range(2):
        order = chip_bits(n_dp)
        order = order if h == 0 else order[::-1]
        leaves, held = [zrel[:, h]], []
        for bit in order:
            leaves, held = exchange(leaves, held, bit, d, n_dp, 1)
        halves.append(leaves[0])
    both = jnp.stack(halves, axis=-3)
    held = chip_bits(n_dp)[::-1]
    if n_dp > 1:
        (both,), held = exchange([both], held, 0, d, n_dp, 1)
    plane = both.reshape((n_fsdp - 1, n_dp) + both.shape[-3:])
    rel = jnp.concatenate([pieces[None], plane], axis=0)
    return jnp.roll(rel, f, axis=0).reshape(n_fsdp * rows, cols), vecs


def reduce_chain(grads, n_dp, n_fsdp, direct=False):
    d = lax.axis_index("dp")
    f = lax.axis_index("fsdp")
    bits = n_dp.bit_length() - 1
    leaves = [
        g.astype(jnp.bfloat16).reshape((n_fsdp,) + (2,) * bits + (2, g.shape[0] // (n_fsdp * 2 * n_dp), g.shape[1]))
        for g in grads
    ]
    held = list(range(bits - 1, -1, -1))
    if bits > 0:
        leaves, held = split_bit(leaves, held, 0, d, n_dp, 1)
    finals = []
    for h in range(2):
        order = chip_bits(n_dp)
        order = order[::-1] if h == 0 else order
        part = [lax.index_in_dim(a, h, 1 + len(held), keepdims=False) for a in leaves]
        hb = list(held)
        for bit in order:
            part, hb = split_bit(part, hb, bit, d, n_dp, 1)
        finals.append(part)
    acc = [jnp.stack([finals[0][i], finals[1][i]], axis=1) for i in range(len(grads))]
    if direct:
        total = [lax.dynamic_index_in_dim(a, f, 0, keepdims=False) for a in acc]
        for step in range(1, n_fsdp):
            out = [lax.dynamic_index_in_dim(a, (f + step) % n_fsdp, 0, keepdims=False).astype(jnp.bfloat16) for a in acc]
            got = lax.ppermute(out, "fsdp", [(i, (i + step) % n_fsdp) for i in range(n_fsdp)])
            total = [t + g.astype(jnp.float32) for t, g in zip(total, got)]
        send = [t.astype(jnp.bfloat16) for t in total]
    else:
        down = [(i, (i - 1) % n_fsdp) for i in range(n_fsdp)]
        if n_fsdp == 1:
            send = [a[0].astype(jnp.bfloat16) for a in acc]
        else:
            send = [lax.dynamic_index_in_dim(a, (f + 1) % n_fsdp, 0, keepdims=False).astype(jnp.bfloat16) for a in acc]
        for step in range(1, n_fsdp):
            got = lax.ppermute(send, "fsdp", down)
            chunk = (f + 1 + step) % n_fsdp
            send = [
                (g.astype(jnp.float32) + lax.dynamic_index_in_dim(a, chunk, 0, keepdims=False)).astype(jnp.bfloat16)
                for g, a in zip(got, acc)
            ]
    bits_chip = chip_bits(n_dp)
    if direct and len(bits_chip) == 2:
        masks = [2, 4, 6]
        got = []
        for mask in masks:
            got.append(lax.ppermute(send, "dp", xor_pairs(n_dp, mask)))
        both = []
        for i, own in enumerate(send):
            cand = jnp.stack([own] + [g[i] for g in got]).reshape((2, 2) + own.shape)
            high = ((d >> 2) & 1) == 1
            low_bit = ((d >> 1) & 1) == 1
            cand = jnp.where(high, cand[::-1], cand)
            cand = jnp.where(low_bit, cand[:, ::-1], cand)
            both.append(cand)
        hb = [2, 1]
    else:
        part, hb = send, []
        for bit in bits_chip:
            part, hb = exchange(part, hb, bit, d, n_dp)
        both = part
    if n_dp > 1:
        both, hb = exchange(both, hb, 0, d, n_dp)
    return [b.reshape(g.shape[0] // n_fsdp, g.shape[1]).astype(jnp.float32) for b, g in zip(both, grads)]


def gather_weights_native(shards):
    return [lax.all_gather(s, "fsdp", axis=0, tiled=True) for s in shards]


def reduce_weights_native(grads):
    return [
        lax.psum(lax.psum_scatter(g, "fsdp", scatter_dimension=0, tiled=True), "dp").astype(jnp.float32)
        for g in grads
    ]


def unpack_vectors(packed, sizes, n_fsdp):
    rows = packed.reshape(n_fsdp, -1)
    out = []
    offset = 0
    for size in sizes:
        width = size // n_fsdp
        out.append(rows[:, offset : offset + width].reshape(size))
        offset += width
    return out


def column_sums(values):
    return jnp.sum(values.astype(jnp.float32), axis=0)


def local_body(
    tokens,
    cotangent,
    crop_group,
    group_tokens,
    qkv_weight,
    query_bias,
    value_bias,
    out_weight,
    out_bias,
    attn_gain,
    attn_shift,
    mlp_gain,
    mlp_shift,
    up_weight,
    up_bias,
    down_weight,
    down_bias,
    n_dp,
    n_fsdp,
):
    small = n_dp * n_fsdp <= 64
    vectors = (query_bias, value_bias, out_bias, attn_gain, attn_shift, mlp_gain, mlp_shift, up_bias, down_bias)
    sizes = [v.shape[0] * n_fsdp for v in vectors]
    vec_local = jnp.concatenate([v.astype(jnp.bfloat16) for v in vectors])
    low = [w.astype(jnp.bfloat16) for w in (qkv_weight, out_weight, up_weight, down_weight)]
    if small:
        qkv_low, vec_rows = gather_chain(low[0], vec_local, n_dp, n_fsdp, True)
        out_low, _ = gather_chain(low[1], None, n_dp, n_fsdp)
        up_low, _ = gather_chain(low[2], None, n_dp, n_fsdp)
        down_low, _ = gather_chain(low[3], None, n_dp, n_fsdp)
    else:
        qkv_low, out_low, up_low, down_low = gather_weights_native(low)
        vec_rows = lax.all_gather(vec_local, "fsdp", axis=0, tiled=False)
    (
        query_add,
        value_add,
        out_add,
        gain_one,
        shift_one,
        gain_two,
        shift_two,
        up_add,
        down_add,
    ) = [v.astype(jnp.float32) for v in unpack_vectors(vec_rows, sizes, n_fsdp)]
    is_global = crop_group[0] == 1
    totals = (group_tokens[0] + group_tokens[1]).astype(jnp.float32)
    loss_share = jnp.where(is_global, group_tokens[1], group_tokens[0]).astype(jnp.float32) / totals
    inputs = tokens.astype(jnp.float32)
    scaled_one, inverse_one = normalize(inputs)
    normed_one = (scaled_one * gain_one + shift_one).astype(jnp.bfloat16)
    projected = jnp.dot(normed_one, qkv_low, preferred_element_type=jnp.float32)
    projected = projected + jnp.concatenate([query_add, jnp.zeros_like(query_add), value_add])
    projected_low = projected.astype(jnp.bfloat16)
    queries = projected_low[:, :D]
    key_rows = projected_low[:, D : 2 * D]
    value_rows = projected_low[:, 2 * D :]
    crop = jnp.where(is_global, GLEN, LLEN)
    context, logsum = attend_crops(queries, key_rows, value_rows, crop)
    context_low = context.astype(jnp.bfloat16)
    middle = inputs + (jnp.dot(context_low, out_low, preferred_element_type=jnp.float32) + out_add)
    scaled_two, inverse_two = normalize(middle)
    normed_two = (scaled_two * gain_two + shift_two).astype(jnp.bfloat16)
    preacts = jnp.dot(normed_two, up_low, preferred_element_type=jnp.float32) + up_add
    error_part = 1.0 + jax.scipy.special.erf(preacts * ROOT_HALF)
    activated = (0.5 * preacts * error_part).astype(jnp.bfloat16)
    mixed_out = (
        middle + (jnp.dot(activated, down_low, preferred_element_type=jnp.float32) + down_add)
    ).astype(jnp.bfloat16)
    upstream = cotangent.astype(jnp.float32) * loss_share
    upstream_low = upstream.astype(jnp.bfloat16)
    grad_down_weight = jnp.dot(activated.T, upstream_low, preferred_element_type=jnp.float32)
    grad_down_bias = column_sums(upstream_low)
    grad_activated = jnp.dot(upstream_low, down_low.T, preferred_element_type=jnp.float32)
    slope = 0.5 * error_part + preacts * jnp.exp(-0.5 * preacts * preacts) * INV_ROOT_TAU
    grad_preacts = (grad_activated * slope).astype(jnp.bfloat16)
    grad_up_weight = jnp.dot(normed_two.T, grad_preacts, preferred_element_type=jnp.float32)
    grad_up_bias = column_sums(grad_preacts)
    grad_normed_two = jnp.dot(grad_preacts, up_low.T, preferred_element_type=jnp.float32)
    grad_mlp_gain = jnp.sum(grad_normed_two * scaled_two, axis=0)
    grad_mlp_shift = jnp.sum(grad_normed_two, axis=0)
    grad_middle = upstream + norm_back(grad_normed_two, gain_two, scaled_two, inverse_two)
    grad_branch = grad_middle.astype(jnp.bfloat16)
    grad_out_weight = jnp.dot(context_low.T, grad_branch, preferred_element_type=jnp.float32)
    grad_out_bias = column_sums(grad_branch)
    grad_context = jnp.dot(grad_branch, out_low.T, preferred_element_type=jnp.float32).astype(
        jnp.bfloat16
    )
    grad_projected = attend_crops_back(queries, key_rows, value_rows, logsum, grad_context, crop)
    grad_qkv_weight = jnp.dot(normed_one.T, grad_projected, preferred_element_type=jnp.float32)
    grad_query_bias = column_sums(grad_projected[:, :D])
    grad_value_bias = column_sums(grad_projected[:, 2 * D :])
    grad_normed_one = jnp.dot(grad_projected, qkv_low.T, preferred_element_type=jnp.float32)
    grad_attn_gain = jnp.sum(grad_normed_one * scaled_one, axis=0)
    grad_attn_shift = jnp.sum(grad_normed_one, axis=0)
    grad_tokens = (
        grad_middle + norm_back(grad_normed_one, gain_one, scaled_one, inverse_one)
    ).astype(jnp.bfloat16)
    grad_vectors = (
        grad_query_bias,
        grad_value_bias,
        grad_out_bias,
        grad_attn_gain,
        grad_attn_shift,
        grad_mlp_gain,
        grad_mlp_shift,
        grad_up_bias,
        grad_down_bias,
    )
    vec_grads = jnp.concatenate(
        [g.astype(jnp.bfloat16).reshape(n_fsdp, -1) for g in grad_vectors], axis=1
    )
    if small:
        (grad_down_shard,) = reduce_chain([grad_down_weight], n_dp, n_fsdp)
        (grad_up_shard,) = reduce_chain([grad_up_weight], n_dp, n_fsdp)
        (grad_out_shard,) = reduce_chain([grad_out_weight], n_dp, n_fsdp)
        rows = grad_qkv_weight.shape[0] // (n_fsdp * 2 * n_dp)
        slot = vec_grads.shape[1] // (2 * n_dp)
        if slot % rows == 0:
            qkv_view = grad_qkv_weight.astype(jnp.bfloat16).reshape(n_fsdp, n_dp, 2, rows, -1)
            vec_view = vec_grads.reshape(n_fsdp, n_dp, 2, rows, slot // rows)
            pad = -(slot // rows) % 128
            vec_view = jnp.pad(vec_view, ((0, 0),) * 4 + ((0, pad),))
            joined = jnp.concatenate([qkv_view, vec_view], axis=-1)
            (both_shard,) = reduce_chain([joined.reshape(grad_qkv_weight.shape[0], -1)], n_dp, n_fsdp, True)
            cols = grad_qkv_weight.shape[1]
            grad_qkv_shard = both_shard[:, :cols]
            vec_flat = both_shard[:, cols : cols + slot // rows].reshape(-1)
        else:
            grad_qkv_shard, vec_flat = reduce_chain(
                [grad_qkv_weight, vec_grads.reshape(n_fsdp * 2 * n_dp, -1)], n_dp, n_fsdp
            )
    else:
        grad_qkv_shard, grad_out_shard, grad_up_shard, grad_down_shard = reduce_weights_native(
            [w.astype(jnp.bfloat16) for w in (grad_qkv_weight, grad_out_weight, grad_up_weight, grad_down_weight)],
        )
        (vec_flat,) = reduce_weights_native([vec_grads])
    vec_out = unpack_vectors(vec_flat.reshape(1, -1), [s // n_fsdp for s in sizes], 1)
    return (
        mixed_out,
        grad_tokens,
        grad_qkv_shard,
        vec_out[0],
        vec_out[1],
        grad_out_shard,
        vec_out[2],
        vec_out[3],
        vec_out[4],
        vec_out[5],
        vec_out[6],
        grad_up_shard,
        vec_out[7],
        grad_down_shard,
        vec_out[8],
    )


def solution(mesh):
    placed = (
        P(("dp", "fsdp"), None),
        P(("dp", "fsdp"), None),
        P("dp"),
        P(),
        P("fsdp", None),
        P("fsdp"),
        P("fsdp"),
        P("fsdp", None),
        P("fsdp"),
        P("fsdp"),
        P("fsdp"),
        P("fsdp"),
        P("fsdp"),
        P("fsdp", None),
        P("fsdp"),
        P("fsdp", None),
        P("fsdp"),
    )
    n_dp = mesh.shape["dp"]
    n_fsdp = mesh.shape["fsdp"]
    return jax.shard_map(
        functools.partial(local_body, n_dp=n_dp, n_fsdp=n_fsdp),
        mesh=mesh,
        in_specs=placed,
        out_specs=(
            P(("dp", "fsdp"), None),
            P(("dp", "fsdp"), None),
            P("fsdp", None),
            P("fsdp"),
            P("fsdp"),
            P("fsdp", None),
            P("fsdp"),
            P("fsdp"),
            P("fsdp"),
            P("fsdp"),
            P("fsdp"),
            P("fsdp", None),
            P("fsdp"),
            P("fsdp", None),
            P("fsdp"),
        ),
        check_vma=False,
    )
```

```python
import functools

import jax
import jax.numpy as jnp
from jax import lax
from jax.sharding import PartitionSpec as P


D = 1024
HEADS = 16
HEAD_DIM = 64
GLEN = 50
LLEN = 10


EPSILON = 1e-06
BIG_NEGATIVE = -1000000000.0
ROOT_HALF = 0.7071067811865476
INV_ROOT_TAU = 0.3989422804014327


def normalize(values):
    middle = jnp.mean(values, axis=-1, keepdims=True)
    centered = values - middle
    inverse = lax.rsqrt(jnp.mean(centered * centered, axis=-1, keepdims=True) + EPSILON)
    return (centered * inverse, inverse)


def norm_back(grad_out, gain, scaled, inverse):
    grad_scaled = grad_out * gain
    return inverse * (
        grad_scaled
        - jnp.mean(grad_scaled, axis=-1, keepdims=True)
        - scaled * jnp.mean(grad_scaled * scaled, axis=-1, keepdims=True)
    )


def by_crops(values, crop):
    return values.reshape(values.shape[0] // crop, crop, HEADS, HEAD_DIM)


def crop_scores(queries, key_rows):
    factor = HEAD_DIM ** (-0.5)
    return (
        jnp.einsum("cqhd,ckhd->chqk", queries, key_rows, preferred_element_type=jnp.float32)
        * factor
    )


def crop_mask(crop):
    segment = lax.iota(jnp.int32, GLEN) // crop
    return segment[:, None] == segment[None, :]


def attend_crops(queries, key_rows, value_rows, crop):
    length = queries.shape[0]
    crop_q, crop_k, crop_v = (
        by_crops(queries, GLEN),
        by_crops(key_rows, GLEN),
        by_crops(value_rows, GLEN),
    )
    scores = jnp.where(crop_mask(crop), crop_scores(crop_q, crop_k), BIG_NEGATIVE)
    highest = jnp.max(scores, axis=-1, keepdims=True)
    exponent = jnp.exp(scores - highest)
    summed = jnp.sum(exponent, axis=-1, keepdims=True)
    attention = (exponent / summed).astype(jnp.bfloat16)
    context = jnp.einsum("chqk,ckhd->cqhd", attention, crop_v, preferred_element_type=jnp.float32)
    logsum = (highest + jnp.log(summed))[..., 0]
    return (
        context.reshape(length, HEADS * HEAD_DIM),
        jnp.transpose(logsum, (0, 2, 1)).reshape(length, HEADS),
    )


def attend_crops_back(queries, key_rows, value_rows, logsum, grad_context, crop):
    length = queries.shape[0]
    factor = HEAD_DIM ** (-0.5)
    crop_q, crop_k, crop_v = (
        by_crops(queries, GLEN),
        by_crops(key_rows, GLEN),
        by_crops(value_rows, GLEN),
    )
    crop_g = by_crops(grad_context, GLEN)
    crop_l = jnp.transpose(logsum.reshape(length // GLEN, GLEN, HEADS), (0, 2, 1))
    scores = jnp.where(crop_mask(crop), crop_scores(crop_q, crop_k), BIG_NEGATIVE)
    probs = jnp.exp(scores - crop_l[..., None])
    probs_low = probs.astype(jnp.bfloat16)
    grad_values = jnp.einsum(
        "chqk,cqhd->ckhd", probs_low, crop_g, preferred_element_type=jnp.float32
    )
    grad_probs = jnp.einsum("cqhd,ckhd->chqk", crop_g, crop_v, preferred_element_type=jnp.float32)
    delta = jnp.sum(probs * grad_probs, axis=-1, keepdims=True)
    grad_scores = (probs * (grad_probs - delta)).astype(jnp.bfloat16)
    grad_queries = (
        jnp.einsum("chqk,ckhd->cqhd", grad_scores, crop_k, preferred_element_type=jnp.float32)
        * factor
    )
    grad_keys = (
        jnp.einsum("chqk,cqhd->ckhd", grad_scores, crop_q, preferred_element_type=jnp.float32)
        * factor
    )
    width = HEADS * HEAD_DIM
    return jnp.concatenate(
        [
            grad_queries.reshape(length, width),
            grad_keys.reshape(length, width),
            grad_values.reshape(length, width),
        ],
        axis=1,
    ).astype(jnp.bfloat16)


def xor_pairs(n, mask):
    return [(i, i ^ mask) for i in range(n)]


def exchange(leaves, held, bit, d, n_dp, lead=0):
    got = lax.ppermute(leaves, "dp", xor_pairs(n_dp, 1 << bit))
    pos = lead + sum(1 for b in held if b > bit)
    mine = ((d >> bit) & 1) == 0
    out = [
        jnp.where(mine, jnp.stack([a, g], axis=pos), jnp.stack([g, a], axis=pos))
        for a, g in zip(leaves, got)
    ]
    return out, sorted(held + [bit], reverse=True)


def split_bit(leaves, held, bit, d, n_dp, lead):
    axis = lead + held.index(bit)
    mine = (d >> bit) & 1
    send = [lax.dynamic_index_in_dim(a, 1 - mine, axis, keepdims=False) for a in leaves]
    keep = [lax.dynamic_index_in_dim(a, mine, axis, keepdims=False) for a in leaves]
    got = lax.ppermute([v.astype(jnp.bfloat16) for v in send], "dp", xor_pairs(n_dp, 1 << bit))
    return [k.astype(jnp.float32) + g.astype(jnp.float32) for k, g in zip(keep, got)], [b for b in held if b != bit]


def chip_bits(n_dp):
    return list(range(1, n_dp.bit_length() - 1))


def gather_chain(shard, vec, n_dp, n_fsdp, direct=False):
    d = lax.axis_index("dp")
    f = lax.axis_index("fsdp")
    rows, cols = shard.shape
    pieces = shard.reshape(n_dp, 2, rows // (2 * n_dp), cols)
    own = lax.dynamic_index_in_dim(pieces, d, 0, keepdims=False)
    down = [(i, (i - 1) % n_fsdp) for i in range(n_fsdp)]
    ring, vring = [], []
    buf = [own] + ([vec] if vec is not None else [])
    for step in range(1, n_fsdp):
        if direct:
            got = lax.ppermute(buf, "fsdp", [(i, (i - step) % n_fsdp) for i in range(n_fsdp)])
        else:
            got = buf = lax.ppermute(buf, "fsdp", down)
        ring.append(got[0])
        if vec is not None:
            vring.append(got[1])
    vecs = None
    if vec is not None:
        vecs = jnp.roll(jnp.stack([vec] + vring, axis=0), f, axis=0)
    if n_fsdp == 1:
        return shard, vecs
    zrel = jnp.stack(ring, axis=0)
    halves = []
    for h in range(2):
        order = chip_bits(n_dp)
        order = order if h == 0 else order[::-1]
        leaves, held = [zrel[:, h]], []
        for bit in order:
            leaves, held = exchange(leaves, held, bit, d, n_dp, 1)
        halves.append(leaves[0])
    both = jnp.stack(halves, axis=-3)
    held = chip_bits(n_dp)[::-1]
    if n_dp > 1:
        (both,), held = exchange([both], held, 0, d, n_dp, 1)
    plane = both.reshape((n_fsdp - 1, n_dp) + both.shape[-3:])
    rel = jnp.concatenate([pieces[None], plane], axis=0)
    return jnp.roll(rel, f, axis=0).reshape(n_fsdp * rows, cols), vecs


def reduce_chain(grads, n_dp, n_fsdp, direct=False, direct_gather=None):
    d = lax.axis_index("dp")
    f = lax.axis_index("fsdp")
    bits = n_dp.bit_length() - 1
    leaves = [
        g.astype(jnp.bfloat16).reshape((n_fsdp,) + (2,) * bits + (2, g.shape[0] // (n_fsdp * 2 * n_dp), g.shape[1]))
        for g in grads
    ]
    held = list(range(bits - 1, -1, -1))
    if bits > 0:
        leaves, held = split_bit(leaves, held, 0, d, n_dp, 1)
    finals = []
    for h in range(2):
        order = chip_bits(n_dp)
        order = order[::-1] if h == 0 else order
        part = [lax.index_in_dim(a, h, 1 + len(held), keepdims=False) for a in leaves]
        hb = list(held)
        for bit in order:
            part, hb = split_bit(part, hb, bit, d, n_dp, 1)
        finals.append(part)
    acc = [jnp.stack([finals[0][i], finals[1][i]], axis=1) for i in range(len(grads))]
    if direct:
        total = [lax.dynamic_index_in_dim(a, f, 0, keepdims=False) for a in acc]
        for step in range(1, n_fsdp):
            out = [lax.dynamic_index_in_dim(a, (f + step) % n_fsdp, 0, keepdims=False).astype(jnp.bfloat16) for a in acc]
            got = lax.ppermute(out, "fsdp", [(i, (i + step) % n_fsdp) for i in range(n_fsdp)])
            total = [t + g.astype(jnp.float32) for t, g in zip(total, got)]
        send = [t.astype(jnp.bfloat16) for t in total]
    else:
        down = [(i, (i - 1) % n_fsdp) for i in range(n_fsdp)]
        if n_fsdp == 1:
            send = [a[0].astype(jnp.bfloat16) for a in acc]
        else:
            send = [lax.dynamic_index_in_dim(a, (f + 1) % n_fsdp, 0, keepdims=False).astype(jnp.bfloat16) for a in acc]
        for step in range(1, n_fsdp):
            got = lax.ppermute(send, "fsdp", down)
            chunk = (f + 1 + step) % n_fsdp
            send = [
                (g.astype(jnp.float32) + lax.dynamic_index_in_dim(a, chunk, 0, keepdims=False)).astype(jnp.bfloat16)
                for g, a in zip(got, acc)
            ]
    bits_chip = chip_bits(n_dp)
    if direct_gather is None:
        direct_gather = direct
    if direct_gather and len(bits_chip) == 2:
        masks = [2, 4, 6]
        got = []
        for mask in masks:
            got.append(lax.ppermute(send, "dp", xor_pairs(n_dp, mask)))
        both = []
        for i, own in enumerate(send):
            cand = jnp.stack([own] + [g[i] for g in got]).reshape((2, 2) + own.shape)
            high = ((d >> 2) & 1) == 1
            low_bit = ((d >> 1) & 1) == 1
            cand = jnp.where(high, cand[::-1], cand)
            cand = jnp.where(low_bit, cand[:, ::-1], cand)
            both.append(cand)
        hb = [2, 1]
    else:
        part, hb = send, []
        for bit in bits_chip:
            part, hb = exchange(part, hb, bit, d, n_dp)
        both = part
    if n_dp > 1:
        both, hb = exchange(both, hb, 0, d, n_dp)
    return [b.reshape(g.shape[0] // n_fsdp, g.shape[1]).astype(jnp.float32) for b, g in zip(both, grads)]


def gather_weights_native(shards):
    return [lax.all_gather(s, "fsdp", axis=0, tiled=True) for s in shards]


def reduce_weights_native(grads):
    return [
        lax.psum(lax.psum_scatter(g, "fsdp", scatter_dimension=0, tiled=True), "dp").astype(jnp.float32)
        for g in grads
    ]


def unpack_vectors(packed, sizes, n_fsdp):
    rows = packed.reshape(n_fsdp, -1)
    out = []
    offset = 0
    for size in sizes:
        width = size // n_fsdp
        out.append(rows[:, offset : offset + width].reshape(size))
        offset += width
    return out


def column_sums(values):
    return jnp.sum(values.astype(jnp.float32), axis=0)


def local_body(
    tokens,
    cotangent,
    crop_group,
    group_tokens,
    qkv_weight,
    query_bias,
    value_bias,
    out_weight,
    out_bias,
    attn_gain,
    attn_shift,
    mlp_gain,
    mlp_shift,
    up_weight,
    up_bias,
    down_weight,
    down_bias,
    n_dp,
    n_fsdp,
):
    small = n_dp * n_fsdp <= 64
    vectors = (query_bias, value_bias, out_bias, attn_gain, attn_shift, mlp_gain, mlp_shift, up_bias, down_bias)
    sizes = [v.shape[0] * n_fsdp for v in vectors]
    vec_local = jnp.concatenate([v.astype(jnp.bfloat16) for v in vectors])
    low = [w.astype(jnp.bfloat16) for w in (qkv_weight, out_weight, up_weight, down_weight)]
    if small:
        qkv_low, vec_rows = gather_chain(low[0], vec_local, n_dp, n_fsdp, True)
        out_low, _ = gather_chain(low[1], None, n_dp, n_fsdp)
        up_low, _ = gather_chain(low[2], None, n_dp, n_fsdp)
        down_low, _ = gather_chain(low[3], None, n_dp, n_fsdp)
    else:
        qkv_low, out_low, up_low, down_low = gather_weights_native(low)
        vec_rows = lax.all_gather(vec_local, "fsdp", axis=0, tiled=False)
    (
        query_add,
        value_add,
        out_add,
        gain_one,
        shift_one,
        gain_two,
        shift_two,
        up_add,
        down_add,
    ) = [v.astype(jnp.float32) for v in unpack_vectors(vec_rows, sizes, n_fsdp)]
    is_global = crop_group[0] == 1
    totals = (group_tokens[0] + group_tokens[1]).astype(jnp.float32)
    loss_share = jnp.where(is_global, group_tokens[1], group_tokens[0]).astype(jnp.float32) / totals
    inputs = tokens.astype(jnp.float32)
    scaled_one, inverse_one = normalize(inputs)
    normed_one = (scaled_one * gain_one + shift_one).astype(jnp.bfloat16)
    projected = jnp.dot(normed_one, qkv_low, preferred_element_type=jnp.float32)
    projected = projected + jnp.concatenate([query_add, jnp.zeros_like(query_add), value_add])
    projected_low = projected.astype(jnp.bfloat16)
    queries = projected_low[:, :D]
    key_rows = projected_low[:, D : 2 * D]
    value_rows = projected_low[:, 2 * D :]
    crop = jnp.where(is_global, GLEN, LLEN)
    context, logsum = attend_crops(queries, key_rows, value_rows, crop)
    context_low = context.astype(jnp.bfloat16)
    middle = inputs + (jnp.dot(context_low, out_low, preferred_element_type=jnp.float32) + out_add)
    scaled_two, inverse_two = normalize(middle)
    normed_two = (scaled_two * gain_two + shift_two).astype(jnp.bfloat16)
    preacts = jnp.dot(normed_two, up_low, preferred_element_type=jnp.float32) + up_add
    error_part = 1.0 + jax.scipy.special.erf(preacts * ROOT_HALF)
    activated = (0.5 * preacts * error_part).astype(jnp.bfloat16)
    mixed_out = (
        middle + (jnp.dot(activated, down_low, preferred_element_type=jnp.float32) + down_add)
    ).astype(jnp.bfloat16)
    upstream = cotangent.astype(jnp.float32) * loss_share
    upstream_low = upstream.astype(jnp.bfloat16)
    grad_down_weight = jnp.dot(activated.T, upstream_low, preferred_element_type=jnp.float32)
    grad_down_bias = column_sums(upstream_low)
    grad_activated = jnp.dot(upstream_low, down_low.T, preferred_element_type=jnp.float32)
    slope = 0.5 * error_part + preacts * jnp.exp(-0.5 * preacts * preacts) * INV_ROOT_TAU
    grad_preacts = (grad_activated * slope).astype(jnp.bfloat16)
    grad_up_weight = jnp.dot(normed_two.T, grad_preacts, preferred_element_type=jnp.float32)
    grad_up_bias = column_sums(grad_preacts)
    grad_normed_two = jnp.dot(grad_preacts, up_low.T, preferred_element_type=jnp.float32)
    grad_mlp_gain = jnp.sum(grad_normed_two * scaled_two, axis=0)
    grad_mlp_shift = jnp.sum(grad_normed_two, axis=0)
    grad_middle = upstream + norm_back(grad_normed_two, gain_two, scaled_two, inverse_two)
    grad_branch = grad_middle.astype(jnp.bfloat16)
    grad_out_weight = jnp.dot(context_low.T, grad_branch, preferred_element_type=jnp.float32)
    grad_out_bias = column_sums(grad_branch)
    grad_context = jnp.dot(grad_branch, out_low.T, preferred_element_type=jnp.float32).astype(
        jnp.bfloat16
    )
    grad_projected = attend_crops_back(queries, key_rows, value_rows, logsum, grad_context, crop)
    grad_qkv_weight = jnp.dot(normed_one.T, grad_projected, preferred_element_type=jnp.float32)
    grad_query_bias = column_sums(grad_projected[:, :D])
    grad_value_bias = column_sums(grad_projected[:, 2 * D :])
    grad_normed_one = jnp.dot(grad_projected, qkv_low.T, preferred_element_type=jnp.float32)
    grad_attn_gain = jnp.sum(grad_normed_one * scaled_one, axis=0)
    grad_attn_shift = jnp.sum(grad_normed_one, axis=0)
    grad_tokens = (
        grad_middle + norm_back(grad_normed_one, gain_one, scaled_one, inverse_one)
    ).astype(jnp.bfloat16)
    grad_vectors = (
        grad_query_bias,
        grad_value_bias,
        grad_out_bias,
        grad_attn_gain,
        grad_attn_shift,
        grad_mlp_gain,
        grad_mlp_shift,
        grad_up_bias,
        grad_down_bias,
    )
    vec_grads = jnp.concatenate(
        [g.astype(jnp.bfloat16).reshape(n_fsdp, -1) for g in grad_vectors], axis=1
    )
    if small:
        (grad_down_shard,) = reduce_chain([grad_down_weight], n_dp, n_fsdp)
        (grad_up_shard,) = reduce_chain([grad_up_weight], n_dp, n_fsdp, direct_gather=True)
        (grad_out_shard,) = reduce_chain([grad_out_weight], n_dp, n_fsdp)
        rows = grad_qkv_weight.shape[0] // (n_fsdp * 2 * n_dp)
        slot = vec_grads.shape[1] // (2 * n_dp)
        if slot % rows == 0:
            qkv_view = grad_qkv_weight.astype(jnp.bfloat16).reshape(n_fsdp, n_dp, 2, rows, -1)
            vec_view = vec_grads.reshape(n_fsdp, n_dp, 2, rows, slot // rows)
            pad = -(slot // rows) % 128
            vec_view = jnp.pad(vec_view, ((0, 0),) * 4 + ((0, pad),))
            joined = jnp.concatenate([qkv_view, vec_view], axis=-1)
            (both_shard,) = reduce_chain([joined.reshape(grad_qkv_weight.shape[0], -1)], n_dp, n_fsdp, True)
            cols = grad_qkv_weight.shape[1]
            grad_qkv_shard = both_shard[:, :cols]
            vec_flat = both_shard[:, cols : cols + slot // rows].reshape(-1)
        else:
            grad_qkv_shard, vec_flat = reduce_chain(
                [grad_qkv_weight, vec_grads.reshape(n_fsdp * 2 * n_dp, -1)], n_dp, n_fsdp
            )
    else:
        grad_qkv_shard, grad_out_shard, grad_up_shard, grad_down_shard = reduce_weights_native(
            [w.astype(jnp.bfloat16) for w in (grad_qkv_weight, grad_out_weight, grad_up_weight, grad_down_weight)],
        )
        (vec_flat,) = reduce_weights_native([vec_grads])
    vec_out = unpack_vectors(vec_flat.reshape(1, -1), [s // n_fsdp for s in sizes], 1)
    return (
        mixed_out,
        grad_tokens,
        grad_qkv_shard,
        vec_out[0],
        vec_out[1],
        grad_out_shard,
        vec_out[2],
        vec_out[3],
        vec_out[4],
        vec_out[5],
        vec_out[6],
        grad_up_shard,
        vec_out[7],
        grad_down_shard,
        vec_out[8],
    )


def solution(mesh):
    placed = (
        P(("dp", "fsdp"), None),
        P(("dp", "fsdp"), None),
        P("dp"),
        P(),
        P("fsdp", None),
        P("fsdp"),
        P("fsdp"),
        P("fsdp", None),
        P("fsdp"),
        P("fsdp"),
        P("fsdp"),
        P("fsdp"),
        P("fsdp"),
        P("fsdp", None),
        P("fsdp"),
        P("fsdp", None),
        P("fsdp"),
    )
    n_dp = mesh.shape["dp"]
    n_fsdp = mesh.shape["fsdp"]
    return jax.shard_map(
        functools.partial(local_body, n_dp=n_dp, n_fsdp=n_fsdp),
        mesh=mesh,
        in_specs=placed,
        out_specs=(
            P(("dp", "fsdp"), None),
            P(("dp", "fsdp"), None),
            P("fsdp", None),
            P("fsdp"),
            P("fsdp"),
            P("fsdp", None),
            P("fsdp"),
            P("fsdp"),
            P("fsdp"),
            P("fsdp"),
            P("fsdp"),
            P("fsdp", None),
            P("fsdp"),
            P("fsdp", None),
            P("fsdp"),
        ),
        check_vma=False,
    )
```

```python
import functools

import jax
import jax.numpy as jnp
from jax import lax
from jax.sharding import PartitionSpec as P


D = 1024
HEADS = 16
HEAD_DIM = 64
GLEN = 50
LLEN = 10


EPSILON = 1e-06
BIG_NEGATIVE = -1000000000.0
ROOT_HALF = 0.7071067811865476
INV_ROOT_TAU = 0.3989422804014327


def normalize(values):
    middle = jnp.mean(values, axis=-1, keepdims=True)
    centered = values - middle
    inverse = lax.rsqrt(jnp.mean(centered * centered, axis=-1, keepdims=True) + EPSILON)
    return (centered * inverse, inverse)


def norm_back(grad_out, gain, scaled, inverse):
    grad_scaled = grad_out * gain
    return inverse * (
        grad_scaled
        - jnp.mean(grad_scaled, axis=-1, keepdims=True)
        - scaled * jnp.mean(grad_scaled * scaled, axis=-1, keepdims=True)
    )


def by_crops(values, crop):
    return values.reshape(values.shape[0] // crop, crop, HEADS, HEAD_DIM)


def crop_scores(queries, key_rows):
    factor = HEAD_DIM ** (-0.5)
    return (
        jnp.einsum("cqhd,ckhd->chqk", queries, key_rows, preferred_element_type=jnp.float32)
        * factor
    )


def crop_mask(crop):
    segment = lax.iota(jnp.int32, GLEN) // crop
    return segment[:, None] == segment[None, :]


def attend_crops(queries, key_rows, value_rows, crop):
    length = queries.shape[0]
    crop_q, crop_k, crop_v = (
        by_crops(queries, GLEN),
        by_crops(key_rows, GLEN),
        by_crops(value_rows, GLEN),
    )
    scores = jnp.where(crop_mask(crop), crop_scores(crop_q, crop_k), BIG_NEGATIVE)
    highest = jnp.max(scores, axis=-1, keepdims=True)
    exponent = jnp.exp(scores - highest)
    summed = jnp.sum(exponent, axis=-1, keepdims=True)
    attention = (exponent / summed).astype(jnp.bfloat16)
    context = jnp.einsum("chqk,ckhd->cqhd", attention, crop_v, preferred_element_type=jnp.float32)
    logsum = (highest + jnp.log(summed))[..., 0]
    return (
        context.reshape(length, HEADS * HEAD_DIM),
        jnp.transpose(logsum, (0, 2, 1)).reshape(length, HEADS),
    )


def attend_crops_back(queries, key_rows, value_rows, logsum, grad_context, crop):
    length = queries.shape[0]
    factor = HEAD_DIM ** (-0.5)
    crop_q, crop_k, crop_v = (
        by_crops(queries, GLEN),
        by_crops(key_rows, GLEN),
        by_crops(value_rows, GLEN),
    )
    crop_g = by_crops(grad_context, GLEN)
    crop_l = jnp.transpose(logsum.reshape(length // GLEN, GLEN, HEADS), (0, 2, 1))
    scores = jnp.where(crop_mask(crop), crop_scores(crop_q, crop_k), BIG_NEGATIVE)
    probs = jnp.exp(scores - crop_l[..., None])
    probs_low = probs.astype(jnp.bfloat16)
    grad_values = jnp.einsum(
        "chqk,cqhd->ckhd", probs_low, crop_g, preferred_element_type=jnp.float32
    )
    grad_probs = jnp.einsum("cqhd,ckhd->chqk", crop_g, crop_v, preferred_element_type=jnp.float32)
    delta = jnp.sum(probs * grad_probs, axis=-1, keepdims=True)
    grad_scores = (probs * (grad_probs - delta)).astype(jnp.bfloat16)
    grad_queries = (
        jnp.einsum("chqk,ckhd->cqhd", grad_scores, crop_k, preferred_element_type=jnp.float32)
        * factor
    )
    grad_keys = (
        jnp.einsum("chqk,cqhd->ckhd", grad_scores, crop_q, preferred_element_type=jnp.float32)
        * factor
    )
    width = HEADS * HEAD_DIM
    return jnp.concatenate(
        [
            grad_queries.reshape(length, width),
            grad_keys.reshape(length, width),
            grad_values.reshape(length, width),
        ],
        axis=1,
    ).astype(jnp.bfloat16)


def xor_pairs(n, mask):
    return [(i, i ^ mask) for i in range(n)]


def exchange(leaves, held, bit, d, n_dp, lead=0):
    got = lax.ppermute(leaves, "dp", xor_pairs(n_dp, 1 << bit))
    pos = lead + sum(1 for b in held if b > bit)
    mine = ((d >> bit) & 1) == 0
    out = [
        jnp.where(mine, jnp.stack([a, g], axis=pos), jnp.stack([g, a], axis=pos))
        for a, g in zip(leaves, got)
    ]
    return out, sorted(held + [bit], reverse=True)


def split_bit(leaves, held, bit, d, n_dp, lead):
    axis = lead + held.index(bit)
    mine = (d >> bit) & 1
    send = [lax.dynamic_index_in_dim(a, 1 - mine, axis, keepdims=False) for a in leaves]
    keep = [lax.dynamic_index_in_dim(a, mine, axis, keepdims=False) for a in leaves]
    got = lax.ppermute([v.astype(jnp.bfloat16) for v in send], "dp", xor_pairs(n_dp, 1 << bit))
    return [k.astype(jnp.float32) + g.astype(jnp.float32) for k, g in zip(keep, got)], [b for b in held if b != bit]


def chip_bits(n_dp):
    return list(range(1, n_dp.bit_length() - 1))


def gather_chain(shard, vec, n_dp, n_fsdp, direct=False):
    d = lax.axis_index("dp")
    f = lax.axis_index("fsdp")
    rows, cols = shard.shape
    pieces = shard.reshape(n_dp, 2, rows // (2 * n_dp), cols)
    own = lax.dynamic_index_in_dim(pieces, d, 0, keepdims=False)
    down = [(i, (i - 1) % n_fsdp) for i in range(n_fsdp)]
    ring, vring = [], []
    buf = [own] + ([vec] if vec is not None else [])
    for step in range(1, n_fsdp):
        if direct:
            got = lax.ppermute(buf, "fsdp", [(i, (i - step) % n_fsdp) for i in range(n_fsdp)])
        else:
            got = buf = lax.ppermute(buf, "fsdp", down)
        ring.append(got[0])
        if vec is not None:
            vring.append(got[1])
    vecs = None
    if vec is not None:
        vecs = jnp.roll(jnp.stack([vec] + vring, axis=0), f, axis=0)
    if n_fsdp == 1:
        return shard, vecs
    zrel = jnp.stack(ring, axis=0)
    if direct and len(chip_bits(n_dp)) == 2:
        got = []
        for mask in [2, 4, 6]:
            got.append(lax.ppermute(zrel, "dp", xor_pairs(n_dp, mask)))
        cand = jnp.stack([zrel] + got, axis=1).reshape((n_fsdp - 1, 2, 2) + zrel.shape[1:])
        cand = jnp.where(((d >> 2) & 1) == 1, cand[:, ::-1], cand)
        both = jnp.where(((d >> 1) & 1) == 1, cand[:, :, ::-1], cand)
        (both,), _ = exchange([both], [2, 1], 0, d, n_dp, 1)
        plane = both.reshape((n_fsdp - 1, n_dp) + both.shape[-3:])
        rel = jnp.concatenate([pieces[None], plane], axis=0)
        return jnp.roll(rel, f, axis=0).reshape(n_fsdp * rows, cols), vecs
    halves = []
    for h in range(2):
        order = chip_bits(n_dp)
        order = order if h == 0 else order[::-1]
        leaves, held = [zrel[:, h]], []
        for bit in order:
            leaves, held = exchange(leaves, held, bit, d, n_dp, 1)
        halves.append(leaves[0])
    both = jnp.stack(halves, axis=-3)
    held = chip_bits(n_dp)[::-1]
    if n_dp > 1:
        (both,), held = exchange([both], held, 0, d, n_dp, 1)
    plane = both.reshape((n_fsdp - 1, n_dp) + both.shape[-3:])
    rel = jnp.concatenate([pieces[None], plane], axis=0)
    return jnp.roll(rel, f, axis=0).reshape(n_fsdp * rows, cols), vecs


def reduce_chain(grads, n_dp, n_fsdp, direct=False, direct_gather=None):
    d = lax.axis_index("dp")
    f = lax.axis_index("fsdp")
    bits = n_dp.bit_length() - 1
    leaves = [
        g.astype(jnp.bfloat16).reshape((n_fsdp,) + (2,) * bits + (2, g.shape[0] // (n_fsdp * 2 * n_dp), g.shape[1]))
        for g in grads
    ]
    held = list(range(bits - 1, -1, -1))
    if bits > 0:
        leaves, held = split_bit(leaves, held, 0, d, n_dp, 1)
    finals = []
    for h in range(2):
        order = chip_bits(n_dp)
        order = order[::-1] if h == 0 else order
        part = [lax.index_in_dim(a, h, 1 + len(held), keepdims=False) for a in leaves]
        hb = list(held)
        for bit in order:
            part, hb = split_bit(part, hb, bit, d, n_dp, 1)
        finals.append(part)
    acc = [jnp.stack([finals[0][i], finals[1][i]], axis=1) for i in range(len(grads))]
    if direct:
        total = [lax.dynamic_index_in_dim(a, f, 0, keepdims=False) for a in acc]
        for step in range(1, n_fsdp):
            out = [lax.dynamic_index_in_dim(a, (f + step) % n_fsdp, 0, keepdims=False).astype(jnp.bfloat16) for a in acc]
            got = lax.ppermute(out, "fsdp", [(i, (i + step) % n_fsdp) for i in range(n_fsdp)])
            total = [t + g.astype(jnp.float32) for t, g in zip(total, got)]
        send = [t.astype(jnp.bfloat16) for t in total]
    else:
        down = [(i, (i - 1) % n_fsdp) for i in range(n_fsdp)]
        if n_fsdp == 1:
            send = [a[0].astype(jnp.bfloat16) for a in acc]
        else:
            send = [lax.dynamic_index_in_dim(a, (f + 1) % n_fsdp, 0, keepdims=False).astype(jnp.bfloat16) for a in acc]
        for step in range(1, n_fsdp):
            got = lax.ppermute(send, "fsdp", down)
            chunk = (f + 1 + step) % n_fsdp
            send = [
                (g.astype(jnp.float32) + lax.dynamic_index_in_dim(a, chunk, 0, keepdims=False)).astype(jnp.bfloat16)
                for g, a in zip(got, acc)
            ]
    bits_chip = chip_bits(n_dp)
    if direct_gather is None:
        direct_gather = direct
    if direct_gather and len(bits_chip) == 2:
        masks = [2, 4, 6]
        got = []
        for mask in masks:
            got.append(lax.ppermute(send, "dp", xor_pairs(n_dp, mask)))
        both = []
        for i, own in enumerate(send):
            cand = jnp.stack([own] + [g[i] for g in got]).reshape((2, 2) + own.shape)
            high = ((d >> 2) & 1) == 1
            low_bit = ((d >> 1) & 1) == 1
            cand = jnp.where(high, cand[::-1], cand)
            cand = jnp.where(low_bit, cand[:, ::-1], cand)
            both.append(cand)
        hb = [2, 1]
    else:
        part, hb = send, []
        for bit in bits_chip:
            part, hb = exchange(part, hb, bit, d, n_dp)
        both = part
    if n_dp > 1:
        both, hb = exchange(both, hb, 0, d, n_dp)
    return [b.reshape(g.shape[0] // n_fsdp, g.shape[1]).astype(jnp.float32) for b, g in zip(both, grads)]


def gather_weights_native(shards):
    return [lax.all_gather(s, "fsdp", axis=0, tiled=True) for s in shards]


def reduce_weights_native(grads):
    return [
        lax.psum(lax.psum_scatter(g, "fsdp", scatter_dimension=0, tiled=True), "dp").astype(jnp.float32)
        for g in grads
    ]


def unpack_vectors(packed, sizes, n_fsdp):
    rows = packed.reshape(n_fsdp, -1)
    out = []
    offset = 0
    for size in sizes:
        width = size // n_fsdp
        out.append(rows[:, offset : offset + width].reshape(size))
        offset += width
    return out


def column_sums(values):
    return jnp.sum(values.astype(jnp.float32), axis=0)


def local_body(
    tokens,
    cotangent,
    crop_group,
    group_tokens,
    qkv_weight,
    query_bias,
    value_bias,
    out_weight,
    out_bias,
    attn_gain,
    attn_shift,
    mlp_gain,
    mlp_shift,
    up_weight,
    up_bias,
    down_weight,
    down_bias,
    n_dp,
    n_fsdp,
):
    small = n_dp * n_fsdp <= 64
    vectors = (query_bias, value_bias, out_bias, attn_gain, attn_shift, mlp_gain, mlp_shift, up_bias, down_bias)
    sizes = [v.shape[0] * n_fsdp for v in vectors]
    vec_local = jnp.concatenate([v.astype(jnp.bfloat16) for v in vectors])
    low = [w.astype(jnp.bfloat16) for w in (qkv_weight, out_weight, up_weight, down_weight)]
    if small:
        qkv_low, vec_rows = gather_chain(low[0], vec_local, n_dp, n_fsdp, True)
        out_low, _ = gather_chain(low[1], None, n_dp, n_fsdp)
        up_low, _ = gather_chain(low[2], None, n_dp, n_fsdp)
        down_low, _ = gather_chain(low[3], None, n_dp, n_fsdp)
    else:
        qkv_low, out_low, up_low, down_low = gather_weights_native(low)
        vec_rows = lax.all_gather(vec_local, "fsdp", axis=0, tiled=False)
    (
        query_add,
        value_add,
        out_add,
        gain_one,
        shift_one,
        gain_two,
        shift_two,
        up_add,
        down_add,
    ) = [v.astype(jnp.float32) for v in unpack_vectors(vec_rows, sizes, n_fsdp)]
    is_global = crop_group[0] == 1
    totals = (group_tokens[0] + group_tokens[1]).astype(jnp.float32)
    loss_share = jnp.where(is_global, group_tokens[1], group_tokens[0]).astype(jnp.float32) / totals
    inputs = tokens.astype(jnp.float32)
    scaled_one, inverse_one = normalize(inputs)
    normed_one = (scaled_one * gain_one + shift_one).astype(jnp.bfloat16)
    projected = jnp.dot(normed_one, qkv_low, preferred_element_type=jnp.float32)
    projected = projected + jnp.concatenate([query_add, jnp.zeros_like(query_add), value_add])
    projected_low = projected.astype(jnp.bfloat16)
    queries = projected_low[:, :D]
    key_rows = projected_low[:, D : 2 * D]
    value_rows = projected_low[:, 2 * D :]
    crop = jnp.where(is_global, GLEN, LLEN)
    context, logsum = attend_crops(queries, key_rows, value_rows, crop)
    context_low = context.astype(jnp.bfloat16)
    middle = inputs + (jnp.dot(context_low, out_low, preferred_element_type=jnp.float32) + out_add)
    scaled_two, inverse_two = normalize(middle)
    normed_two = (scaled_two * gain_two + shift_two).astype(jnp.bfloat16)
    preacts = jnp.dot(normed_two, up_low, preferred_element_type=jnp.float32) + up_add
    error_part = 1.0 + jax.scipy.special.erf(preacts * ROOT_HALF)
    activated = (0.5 * preacts * error_part).astype(jnp.bfloat16)
    mixed_out = (
        middle + (jnp.dot(activated, down_low, preferred_element_type=jnp.float32) + down_add)
    ).astype(jnp.bfloat16)
    upstream = cotangent.astype(jnp.float32) * loss_share
    upstream_low = upstream.astype(jnp.bfloat16)
    grad_down_weight = jnp.dot(activated.T, upstream_low, preferred_element_type=jnp.float32)
    grad_down_bias = column_sums(upstream_low)
    grad_activated = jnp.dot(upstream_low, down_low.T, preferred_element_type=jnp.float32)
    slope = 0.5 * error_part + preacts * jnp.exp(-0.5 * preacts * preacts) * INV_ROOT_TAU
    grad_preacts = (grad_activated * slope).astype(jnp.bfloat16)
    grad_up_weight = jnp.dot(normed_two.T, grad_preacts, preferred_element_type=jnp.float32)
    grad_up_bias = column_sums(grad_preacts)
    grad_normed_two = jnp.dot(grad_preacts, up_low.T, preferred_element_type=jnp.float32)
    grad_mlp_gain = jnp.sum(grad_normed_two * scaled_two, axis=0)
    grad_mlp_shift = jnp.sum(grad_normed_two, axis=0)
    grad_middle = upstream + norm_back(grad_normed_two, gain_two, scaled_two, inverse_two)
    grad_branch = grad_middle.astype(jnp.bfloat16)
    grad_out_weight = jnp.dot(context_low.T, grad_branch, preferred_element_type=jnp.float32)
    grad_out_bias = column_sums(grad_branch)
    grad_context = jnp.dot(grad_branch, out_low.T, preferred_element_type=jnp.float32).astype(
        jnp.bfloat16
    )
    grad_projected = attend_crops_back(queries, key_rows, value_rows, logsum, grad_context, crop)
    grad_qkv_weight = jnp.dot(normed_one.T, grad_projected, preferred_element_type=jnp.float32)
    grad_query_bias = column_sums(grad_projected[:, :D])
    grad_value_bias = column_sums(grad_projected[:, 2 * D :])
    grad_normed_one = jnp.dot(grad_projected, qkv_low.T, preferred_element_type=jnp.float32)
    grad_attn_gain = jnp.sum(grad_normed_one * scaled_one, axis=0)
    grad_attn_shift = jnp.sum(grad_normed_one, axis=0)
    grad_tokens = (
        grad_middle + norm_back(grad_normed_one, gain_one, scaled_one, inverse_one)
    ).astype(jnp.bfloat16)
    grad_vectors = (
        grad_query_bias,
        grad_value_bias,
        grad_out_bias,
        grad_attn_gain,
        grad_attn_shift,
        grad_mlp_gain,
        grad_mlp_shift,
        grad_up_bias,
        grad_down_bias,
    )
    vec_grads = jnp.concatenate(
        [g.astype(jnp.bfloat16).reshape(n_fsdp, -1) for g in grad_vectors], axis=1
    )
    if small:
        (grad_down_shard,) = reduce_chain([grad_down_weight], n_dp, n_fsdp)
        (grad_up_shard,) = reduce_chain([grad_up_weight], n_dp, n_fsdp, direct_gather=True)
        (grad_out_shard,) = reduce_chain([grad_out_weight], n_dp, n_fsdp, direct_gather=True)
        rows = grad_qkv_weight.shape[0] // (n_fsdp * 2 * n_dp)
        slot = vec_grads.shape[1] // (2 * n_dp)
        if slot % rows == 0:
            qkv_view = grad_qkv_weight.astype(jnp.bfloat16).reshape(n_fsdp, n_dp, 2, rows, -1)
            vec_view = vec_grads.reshape(n_fsdp, n_dp, 2, rows, slot // rows)
            pad = -(slot // rows) % 128
            vec_view = jnp.pad(vec_view, ((0, 0),) * 4 + ((0, pad),))
            joined = jnp.concatenate([qkv_view, vec_view], axis=-1)
            (both_shard,) = reduce_chain([joined.reshape(grad_qkv_weight.shape[0], -1)], n_dp, n_fsdp, True)
            cols = grad_qkv_weight.shape[1]
            grad_qkv_shard = both_shard[:, :cols]
            vec_flat = both_shard[:, cols : cols + slot // rows].reshape(-1)
        else:
            grad_qkv_shard, vec_flat = reduce_chain(
                [grad_qkv_weight, vec_grads.reshape(n_fsdp * 2 * n_dp, -1)], n_dp, n_fsdp
            )
    else:
        grad_qkv_shard, grad_out_shard, grad_up_shard, grad_down_shard = reduce_weights_native(
            [w.astype(jnp.bfloat16) for w in (grad_qkv_weight, grad_out_weight, grad_up_weight, grad_down_weight)],
        )
        (vec_flat,) = reduce_weights_native([vec_grads])
    vec_out = unpack_vectors(vec_flat.reshape(1, -1), [s // n_fsdp for s in sizes], 1)
    return (
        mixed_out,
        grad_tokens,
        grad_qkv_shard,
        vec_out[0],
        vec_out[1],
        grad_out_shard,
        vec_out[2],
        vec_out[3],
        vec_out[4],
        vec_out[5],
        vec_out[6],
        grad_up_shard,
        vec_out[7],
        grad_down_shard,
        vec_out[8],
    )


def solution(mesh):
    placed = (
        P(("dp", "fsdp"), None),
        P(("dp", "fsdp"), None),
        P("dp"),
        P(),
        P("fsdp", None),
        P("fsdp"),
        P("fsdp"),
        P("fsdp", None),
        P("fsdp"),
        P("fsdp"),
        P("fsdp"),
        P("fsdp"),
        P("fsdp"),
        P("fsdp", None),
        P("fsdp"),
        P("fsdp", None),
        P("fsdp"),
    )
    n_dp = mesh.shape["dp"]
    n_fsdp = mesh.shape["fsdp"]
    return jax.shard_map(
        functools.partial(local_body, n_dp=n_dp, n_fsdp=n_fsdp),
        mesh=mesh,
        in_specs=placed,
        out_specs=(
            P(("dp", "fsdp"), None),
            P(("dp", "fsdp"), None),
            P("fsdp", None),
            P("fsdp"),
            P("fsdp"),
            P("fsdp", None),
            P("fsdp"),
            P("fsdp"),
            P("fsdp"),
            P("fsdp"),
            P("fsdp"),
            P("fsdp", None),
            P("fsdp"),
            P("fsdp", None),
            P("fsdp"),
        ),
        check_vma=False,
    )
```
